16 devices in a mesh: dp: 2 (over y, z), ep: 8 (over x, core).
Axes of the slice: x: 4, y: 2, z: 1, core: 2. Of those that a mesh axis runs over, the one named last changes fastest.
The devices are a block of a 4x4x8 slice.
Arguments:
- tokens: bfloat16 [2048, 1536], P(('dp', 'ep')), parts along dimension 0
- expert_ids: int32 [2048, 8], P(('dp', 'ep')), parts along dimension 0
- gate_vals: float32 [2048, 8], P(('dp', 'ep')), parts along dimension 0
- w_gate: bfloat16 [40, 1536, 512], P('ep')
- w_up: bfloat16 [40, 1536, 512], P('ep')
- w_down: bfloat16 [40, 512, 1536], P('ep')
- grad_out: bfloat16 [2048, 1536], P(('dp', 'ep')), parts along dimension 0
Outputs:
- output 1: bfloat16 [2048, 1536], P(('dp', 'ep')), parts along dimension 0
- output 2: bfloat16 [2048, 1536], P(('dp', 'ep')), parts along dimension 0
- output 3: bfloat16 [80, 1536, 512], P(('dp', 'ep')), parts along dimension 0
- output 4: bfloat16 [80, 1536, 512], P(('dp', 'ep')), parts along dimension 0
- output 5: bfloat16 [80, 512, 1536], P(('dp', 'ep')), parts along dimension 0
There are 2 independent parts. The reference program is written for one: setup_inputs(seed, part) draws one part's arguments, and reference() takes and returns one part's arrays. A program takes and returns all parts, laid end to end along the dimension named above; an argument that names none is the same for every part.
All inputs are finite; a program needn't handle non-finite values.
Results may differ from the reference program's by a relative error of at most 0.00147.
Values are sent between devices in bfloat16 or wider.
A program may use at most 768 MiB of HBM per device.

```python
import jax
import jax.numpy as jnp
from jax import lax

EP = 8
TOK = 128
D = 1536
FF = 512
EXPERTS = 40
TOP = 8

CAP = ((2 * TOK * TOP + 8 * EXPERTS - 1) // (8 * EXPERTS)) * 8
HOT = EXPERTS // 2


def chip_routing(chip_key, hot_count):
    sub_keys = jax.random.split(chip_key, 3)
    cold_order = jax.random.permutation(sub_keys[0], EXPERTS - 1)
    cold_ids = jnp.where(cold_order >= HOT, cold_order + 1, cold_order).astype(jnp.int32)
    rest_count = TOK * TOP - hot_count - CAP
    base_count = rest_count // (EXPERTS - 2)
    extra_count = rest_count % (EXPERTS - 2)
    cold_rank = jnp.arange(EXPERTS - 1)
    cold_count = jnp.where(cold_rank == 0, CAP, base_count + (cold_rank - 1 < extra_count).astype(jnp.int32))
    counts = jnp.concatenate([jnp.reshape(hot_count, (1,)), cold_count]).astype(jnp.int32)
    listed_ids = jnp.concatenate([jnp.full((1,), HOT, jnp.int32), cold_ids])
    count_ends = jnp.cumsum(counts)
    list_slot = jnp.searchsorted(count_ends, jnp.arange(TOK * TOP), side="right")
    id_grid = listed_ids[list_slot].reshape(TOP, TOK).T
    id_grid = id_grid[jax.random.permutation(sub_keys[1], TOK)]
    row_shift = jax.random.randint(sub_keys[2], (TOK, 1), 0, TOP)
    col_index = (jnp.arange(TOP)[None, :] + row_shift) % TOP
    return jnp.take_along_axis(id_grid, col_index, axis=1)


def draw_routing(route_key):
    sub_keys = jax.random.split(route_key, 3)
    full_chip = jax.random.randint(sub_keys[0], (), 0, EP)
    hot_count = jax.random.randint(sub_keys[1], (EP,), TOK // 4, TOK + 1)
    hot_count = jnp.where(jnp.arange(EP) == full_chip, TOK, hot_count).astype(jnp.int32)
    chip_ids = jax.vmap(chip_routing)(jax.random.split(sub_keys[2], EP), hot_count)
    return chip_ids.reshape(EP * TOK, TOP).astype(jnp.int32)


def setup_inputs(seed: int = 0, part: int = 0) -> dict:
    part_keys = jax.random.split(jax.random.fold_in(jax.random.key(seed), part), 4)
    weight_keys = jax.random.split(jax.random.key(seed + 1), 3)
    tokens = jax.random.normal(part_keys[0], (EP * TOK, D), jnp.float32).astype(jnp.bfloat16)
    expert_ids = draw_routing(part_keys[1])
    gate_vals = jax.random.uniform(part_keys[2], (EP * TOK, TOP), jnp.float32, 0.5, 1.5) * TOP ** -0.5
    w_gate = (jax.random.normal(weight_keys[0], (EXPERTS, D, FF), jnp.float32) * D ** -0.5).astype(jnp.bfloat16)
    w_up = (jax.random.normal(weight_keys[1], (EXPERTS, D, FF), jnp.float32) * D ** -0.5).astype(jnp.bfloat16)
    w_down = (jax.random.normal(weight_keys[2], (EXPERTS, FF, D), jnp.float32) * FF ** -0.5).astype(jnp.bfloat16)
    grad_out = jax.random.normal(part_keys[3], (EP * TOK, D), jnp.float32).astype(jnp.bfloat16)
    return {"tokens": tokens, "expert_ids": expert_ids, "gate_vals": gate_vals, "w_gate": w_gate, "w_up": w_up, "w_down": w_down, "grad_out": grad_out}


def expert_step(in_rows, d_rows_out, gate_w, up_w, down_w):
    act_a = jnp.dot(in_rows, gate_w, preferred_element_type=jnp.float32)
    act_b = jnp.dot(in_rows, up_w, preferred_element_type=jnp.float32)
    sig_a = jax.nn.sigmoid(act_a)
    hidden = (act_a * sig_a * act_b).astype(jnp.bfloat16)
    expert_out = jnp.dot(hidden, down_w, preferred_element_type=jnp.float32).astype(jnp.bfloat16)
    d_hidden = jnp.dot(d_rows_out, down_w.T, preferred_element_type=jnp.float32)
    d_act_a = (d_hidden * act_b * sig_a * (1.0 + act_a * (1.0 - sig_a))).astype(jnp.bfloat16)
    d_act_b = (d_hidden * act_a * sig_a).astype(jnp.bfloat16)
    d_rows = (jnp.dot(d_act_a, gate_w.T, preferred_element_type=jnp.float32) + jnp.dot(d_act_b, up_w.T, preferred_element_type=jnp.float32)).astype(jnp.bfloat16)
    grad_gate = jnp.dot(in_rows.T, d_act_a, preferred_element_type=jnp.float32)
    grad_up = jnp.dot(in_rows.T, d_act_b, preferred_element_type=jnp.float32)
    grad_down = jnp.dot(hidden.T, d_rows_out, preferred_element_type=jnp.float32)
    return expert_out, d_rows, grad_gate, grad_up, grad_down


def reference(tokens, expert_ids, gate_vals, w_gate, w_up, w_down, grad_out):
    num_rows = EP * TOK * TOP
    cold_cap = EP * CAP
    cold_total = EXPERTS * cold_cap
    flat_ids = expert_ids.reshape(num_rows)
    sort_order = jnp.argsort(flat_ids, stable=True)
    sorted_ids = flat_ids[sort_order]
    group_start = jnp.searchsorted(sorted_ids, jnp.arange(EXPERTS), side="left")
    sorted_rank = (jnp.arange(num_rows) - group_start[sorted_ids]).astype(jnp.int32)
    slot_rank = jnp.zeros((num_rows,), jnp.int32).at[sort_order].set(sorted_rank)
    buf_pos = jnp.where(flat_ids == HOT, cold_total + slot_rank, flat_ids * cold_cap + slot_rank)
    tok_rep = jnp.broadcast_to(tokens[:, None, :], (EP * TOK, TOP, D)).reshape(num_rows, D)
    d_rep = (gate_vals[:, :, None] * grad_out[:, None, :].astype(jnp.float32)).astype(jnp.bfloat16).reshape(num_rows, D)
    buf_rows = cold_total + EP * TOK
    x_buf = jnp.zeros((buf_rows, D), jnp.bfloat16).at[buf_pos].set(tok_rep)
    d_buf = jnp.zeros((buf_rows, D), jnp.bfloat16).at[buf_pos].set(d_rep)

    def cold_body(expert_in):
        return expert_step(expert_in[0], expert_in[1], expert_in[2], expert_in[3], expert_in[4])

    cold_res = lax.map(cold_body, (x_buf[:cold_total].reshape(EXPERTS, cold_cap, D), d_buf[:cold_total].reshape(EXPERTS, cold_cap, D), w_gate, w_up, w_down))
    hot_res = expert_step(x_buf[cold_total:], d_buf[cold_total:], w_gate[HOT], w_up[HOT], w_down[HOT])
    out_buf = jnp.concatenate([cold_res[0].reshape(cold_total, D), hot_res[0]], axis=0)
    dx_buf = jnp.concatenate([cold_res[1].reshape(cold_total, D), hot_res[1]], axis=0)
    y_rows = out_buf[buf_pos].reshape(EP * TOK, TOP, D).astype(jnp.float32)
    moe_out = jnp.sum(gate_vals[:, :, None] * y_rows, axis=1).astype(jnp.bfloat16)
    dx_rows = dx_buf[buf_pos].reshape(EP * TOK, TOP, D).astype(jnp.float32)
    grad_tokens = jnp.sum(dx_rows, axis=1).astype(jnp.bfloat16)
    grad_list = [cold_g.at[HOT].add(hot_g).astype(jnp.bfloat16) for cold_g, hot_g in zip(cold_res[2:], hot_res[2:])]
    return (moe_out, grad_tokens, grad_list[0], grad_list[1], grad_list[2])
```

```python
import functools

import jax
import jax.numpy as jnp
from jax import lax
from jax.experimental import pallas as pl
from jax.experimental.pallas import tpu as pltpu
from jax.sharding import PartitionSpec as P

MESH = pl.DeviceIdType.MESH
F32 = jnp.float32
BF16 = jnp.bfloat16


def dot_nn(a, b):
    return lax.dot_general(a, b, (((1,), (0,)), ((), ())), preferred_element_type=F32)


def dot_nt(a, b):
    return lax.dot_general(a, b, (((1,), (1,)), ((), ())), preferred_element_type=F32)


def dot_tn(a, b):
    return lax.dot_general(a, b, (((0,), (0,)), ((), ())), preferred_element_type=F32)


def layer_kernel(cfg, x_hbm, dy_hbm, meta_ref, w1_hbm, w3_hbm, w2_hbm,
                 y_hbm, dx_hbm, xr_hbm, dr_hbm, ur_hbm, da_hbm, db_hbm, xe_hbm, de_hbm, ue_hbm, dae_hbm, dbe_hbm,
                 x_all, dy_all, meta_all, rt, gt, mc, ypart, dxpart, ybuf, dxbuf, yra, yrb, yfl, yfr, dxra, dxrb, dxfl, dxfr,
                 rows, urow, darow, dbrow, act1, act2, orow, w1, w3, w2, outb,
                 m_send, m_recv, ag_send, ag_recv, rs_send, rs_recv, w_sem, st_sem, io_sem):
    chips, tok, width, hid, n_loc, cap, owner = cfg
    group = 2 * chips
    cp = 2 * cap
    n_rows = chips * cp
    hot_rows = chips * 2 * tok
    hb_rows = hot_rows // 2
    half = tok // 2
    me = lax.axis_index("ep")
    c = me // 2
    k = lax.rem(me, 2)
    c_r = lax.rem(c + 1, chips)
    c_l = lax.rem(c + chips - 1, chips)
    c_o = lax.rem(c + 2, chips)
    right = 2 * c_r + k
    left = 2 * c_l + k
    partner = 2 * c + 1 - k
    is_owner = me == owner

    own_x = pltpu.make_async_copy(x_hbm, x_all.at[c, pl.ds(k * tok, tok)], io_sem.at[0])
    own_dy = pltpu.make_async_copy(dy_hbm, dy_all.at[c, pl.ds(k * tok, tok)], io_sem.at[1])
    own_x.start()
    own_dy.start()

    def w_copies(i):
        e = lax.rem(i, n_loc)
        s = lax.rem(i, 2)
        return (pltpu.make_async_copy(w1_hbm.at[e], w1.at[s], w_sem.at[0, s]),
                pltpu.make_async_copy(w3_hbm.at[e], w3.at[s], w_sem.at[1, s]),
                pltpu.make_async_copy(w2_hbm.at[e], w2.at[s], w_sem.at[2, s]))

    for cpy in w_copies(0):
        cpy.start()
    meta_all[me] = meta_ref[...]

    barrier = pltpu.get_barrier_semaphore()
    for d in range(1, group):
        pl.semaphore_signal(barrier, inc=1, device_id={"ep": lax.rem(me + d, group)}, device_id_type=MESH)
    pl.semaphore_wait(barrier, group - 1)

    def meta_copy(d):
        return pltpu.make_async_remote_copy(
            src_ref=meta_ref, dst_ref=meta_all.at[me], send_sem=m_send.at[d], recv_sem=m_recv.at[d],
            device_id={"ep": lax.rem(me + d, group)}, device_id_type=MESH)

    def ag(ref, t, i):
        chip, core, r0, n, dev = (
            (c, k, 0, half, right), (c, k, half, half, right), (c, k, half, half, left), (c, k, 0, half, left),
            (c, k, 0, tok, partner),
            (c_l, k, 0, half, right), (c_r, k, half, half, left),
            (c_l, k, 0, tok, partner), (c_r, k, 0, tok, partner),
            (c_o, k, 0, half, partner), (c_o, k, half, half, partner))[i]
        blk = ref.at[chip, pl.ds(core * tok + r0, n)]
        return pltpu.make_async_remote_copy(
            src_ref=blk, dst_ref=blk, send_sem=ag_send.at[t, i], recv_sem=ag_recv.at[t, i],
            device_id={"ep": dev}, device_id_type=MESH)

    own_x.wait()
    for d in range(1, group):
        meta_copy(d).start()
    for i in (0, 2, 1, 3, 4):
        ag(x_all, 0, i).start()
    own_dy.wait()

    @pl.loop(0, chips * 2 * tok // 64)
    def _(r):
        q = r // (2 * tok // 64)
        o = pl.multiple_of(lax.rem(r, 2 * tok // 64) * 64, 64)
        ypart[q, pl.ds(o, 64)] = jnp.zeros((64, width), F32)
        dxpart[q, pl.ds(o, 64)] = jnp.zeros((64, width), F32)

    for d in range(1, group):
        meta_copy(d).wait_recv()

    upper = (lax.broadcasted_iota(jnp.int32, (tok, tok), 0) < lax.broadcasted_iota(jnp.int32, (tok, tok), 1)).astype(F32).astype(BF16)
    row_id = lax.broadcasted_iota(jnp.int32, (8, tok), 0)
    for s in range(group):
        q, core = s // 2, s % 2
        ids = meta_all[s, 0:8, :]
        gates = meta_all[s, 8:16, :]
        mask_m = jnp.zeros((8, tok), F32)
        gate_m = jnp.zeros((8, tok), F32)
        for le in range(n_loc):
            eq = ids == (me * n_loc + le).astype(F32)
            hit = jnp.sum(jnp.where(eq, 1.0, 0.0), axis=0, keepdims=True)
            gv = jnp.sum(jnp.where(eq, gates, 0.0), axis=0, keepdims=True)
            mask_m = jnp.where(row_id == le, hit, mask_m)
            gate_m = jnp.where(row_id == le, gv, gate_m)
        rank = dot_nn(mask_m.astype(BF16), upper)
        pos = jnp.where(mask_m > 0.0, rank + float(cap * core), -1.0)
        rt[q, :, core * tok:(core + 1) * tok] = pos
        gt[q, :, core * tok:(core + 1) * tok] = gate_m
        both = jnp.concatenate([pos, gate_m, jnp.zeros((tok - 16, tok), F32)], axis=0)
        mc[q, core * tok:(core + 1) * tok, :] = jnp.transpose(both)

    ag(x_all, 0, 0).wait_recv()
    ag(x_all, 0, 5).start()
    ag(x_all, 0, 2).wait_recv()
    ag(x_all, 0, 6).start()
    for i in (0, 2, 1, 3, 4):
        ag(dy_all, 1, i).start()
    ag(x_all, 0, 1).wait_recv()
    ag(x_all, 0, 7).start()
    ag(x_all, 0, 3).wait_recv()
    ag(x_all, 0, 8).start()
    ag(x_all, 0, 4).wait_recv()
    ag(x_all, 0, 5).wait_recv()
    ag(x_all, 0, 9).start()
    ag(x_all, 0, 6).wait_recv()
    ag(x_all, 0, 10).start()
    for i in (7, 8, 9, 10):
        ag(x_all, 0, i).wait_recv()

    def pick_rows(q, e):
        hit = rt[q, pl.ds(e, 1), :] == lax.broadcasted_iota(jnp.int32, (cp, 2 * tok), 0).astype(F32)
        return hit

    def column(q, lane):
        m = mc[q]
        return jnp.sum(jnp.where(lax.broadcasted_iota(jnp.int32, (2 * tok, 128), 1) == lane, m, 0.0), axis=1, keepdims=True)

    def put_rows(q, e):
        hit = column(q, e) == lax.broadcasted_iota(jnp.int32, (2 * tok, cp), 1).astype(F32)
        return jnp.where(hit, 1.0, 0.0).astype(BF16)

    def forward(m, s, aoff):
        for j in range(hid // 256):
            cs = slice(j * 256, (j + 1) * 256)
            act1[pl.ds(aoff, m), cs] = dot_nn(rows[s, 0:m, :], w1[s, :, cs])
            act2[pl.ds(aoff, m), cs] = dot_nn(rows[s, 0:m, :], w3[s, :, cs])

        @pl.loop(0, m // 32)
        def _(r):
            o = pl.multiple_of(aoff + r * 32, 32)
            a = act1[pl.ds(o, 32), :]
            b = act2[pl.ds(o, 32), :]
            sg = jax.nn.sigmoid(a)
            ga = a * sg
            act1[pl.ds(o, 32), :] = b * (sg * (1.0 + a * (1.0 - sg)))
            act2[pl.ds(o, 32), :] = ga
            urow[s, pl.ds(pl.multiple_of(r * 32, 32), 32), :] = (ga * b).astype(BF16)

        for j in range(width // 256):
            cs = slice(j * 256, (j + 1) * 256)
            orow[0:m, cs] = dot_nn(urow[s, 0:m, :], w2[s, :, cs]).astype(BF16)

    def backward(m, s, aoff):
        for j in range(hid // 256):
            cs = slice(j * 256, (j + 1) * 256)
            du = dot_nt(rows[s, 0:m, :], w2[s, cs, :])
            darow[s, 0:m, cs] = (du * act1[pl.ds(aoff, m), cs]).astype(BF16)
            dbrow[s, 0:m, cs] = (du * act2[pl.ds(aoff, m), cs]).astype(BF16)
        for j in range(width // 256):
            cs = slice(j * 256, (j + 1) * 256)
            orow[0:m, cs] = (dot_nt(darow[s, 0:m, :], w1[s, cs, :]) + dot_nt(dbrow[s, 0:m, :], w3[s, cs, :])).astype(BF16)

    def act_off(e):
        return pl.multiple_of(jnp.where(e == 0, 0, hot_rows + (e - 1) * n_rows), 64)

    def st_fwd(e, s):
        return (pltpu.make_async_copy(rows.at[s, 0:n_rows], xr_hbm.at[e], st_sem.at[0, s]),
                pltpu.make_async_copy(urow.at[s, 0:n_rows], ur_hbm.at[e], st_sem.at[1, s]))

    def st_bwd(e, s):
        return (pltpu.make_async_copy(rows.at[s, 0:n_rows], dr_hbm.at[e], st_sem.at[0, s]),
                pltpu.make_async_copy(darow.at[s, 0:n_rows], da_hbm.at[e], st_sem.at[1, s]),
                pltpu.make_async_copy(dbrow.at[s, 0:n_rows], db_hbm.at[e], st_sem.at[2, s]))

    def hot_store(hb, pairs):
        rest = hb_rows - n_rows

        @pl.when(hb == 0)
        def _():
            cps = []
            for t, (src, main, extra) in enumerate(pairs):
                cps.append(pltpu.make_async_copy(src.at[0:n_rows], main.at[0], io_sem.at[2 + 2 * t]))
                cps.append(pltpu.make_async_copy(src.at[n_rows:hb_rows], extra.at[0:rest], io_sem.at[3 + 2 * t]))
            for cpy in cps:
                cpy.start()
            for cpy in cps:
                cpy.wait()

        @pl.when(hb == 1)
        def _():
            cps = [pltpu.make_async_copy(src.at[0:hb_rows], extra.at[rest:rest + hb_rows], io_sem.at[2 + 2 * t])
                   for t, (src, main, extra) in enumerate(pairs)]
            for cpy in cps:
                cpy.start()
            for cpy in cps:
                cpy.wait()

    @pl.loop(0, n_loc)
    def _(e):
        s = lax.rem(e, 2)
        hot = jnp.logical_and(is_owner, e == 0)
        for cpy in w_copies(e + 1):
            cpy.start()
        for cpy in w_copies(e):
            cpy.wait()

        @pl.when(e == 1)
        def _():
            ag(dy_all, 1, 0).wait_recv()
            ag(dy_all, 1, 5).start()
            ag(dy_all, 1, 2).wait_recv()
            ag(dy_all, 1, 6).start()

        @pl.when(e == 3)
        def _():
            ag(dy_all, 1, 1).wait_recv()
            ag(dy_all, 1, 7).start()
            ag(dy_all, 1, 3).wait_recv()
            ag(dy_all, 1, 8).start()

        @pl.when(jnp.logical_not(hot))
        def _():
            for q in range(chips):
                hit = jnp.where(pick_rows(q, e), 1.0, 0.0).astype(BF16)
                rows[s, q * cp:(q + 1) * cp, :] = dot_nn(hit, x_all[q]).astype(BF16)
            forward(n_rows, s, act_off(e))
            for q in range(chips):
                gate = column(q, e + 8)
                ypart[q] += gate * dot_nn(put_rows(q, e), orow[q * cp:(q + 1) * cp, :])

        @pl.when(hot)
        def _():
            @pl.loop(0, 2)
            def _(hb):
                for qq in range(chips // 2):
                    q = hb * (chips // 2) + qq
                    on = column(q, 0) >= 0.0
                    rows[0, qq * 2 * tok:(qq + 1) * 2 * tok, :] = jnp.where(on, x_all[q].astype(F32), 0.0).astype(BF16)
                forward(hb_rows, 0, pl.multiple_of(hb * hb_rows, 64))
                for qq in range(chips // 2):
                    q = hb * (chips // 2) + qq
                    ypart[q] += column(q, 8) * orow[qq * 2 * tok:(qq + 1) * 2 * tok, :].astype(F32)
                hot_store(hb, ((rows.at[0], xr_hbm, xe_hbm), (urow.at[0], ur_hbm, ue_hbm)))

        @pl.when(jnp.logical_and(e >= 1, jnp.logical_not(jnp.logical_and(is_owner, e == 1))))
        def _():
            for cpy in st_fwd(e - 1, 1 - s):
                cpy.wait()

        @pl.when(jnp.logical_not(hot))
        def _():
            for cpy in st_fwd(e, s):
                cpy.start()

    def rs(t, j):
        part, buf, ra, rb, fl, fr = ((ypart, ybuf, yra, yrb, yfl, yfr), (dxpart, dxbuf, dxra, dxrb, dxfl, dxfr))[t]
        o = k * tok
        if j < 4:
            q = (c_o, c_r, c_l, c)[j]
            src, dst, dev = part.at[q, pl.ds((1 - k) * tok, tok)], buf.at[q], partner
        else:
            src, dst, dev = (
                (part.at[c_o, pl.ds(o, half)], ra, right),
                (part.at[c_o, pl.ds(o + half, half)], rb, left),
                (part.at[c_r, pl.ds(o + half, half)], fl.at[half:tok], right),
                (part.at[c_l, pl.ds(o, half)], fr.at[0:half], left),
                (part.at[c_r, pl.ds(o, half)], fl.at[0:half], right),
                (part.at[c_l, pl.ds(o + half, half)], fr.at[half:tok], left))[j - 4]
        return pltpu.make_async_remote_copy(
            src_ref=src, dst_ref=dst, send_sem=rs_send.at[t, j], recv_sem=rs_recv.at[t, j],
            device_id={"ep": dev}, device_id_type=MESH)

    def add_rows(part, q, off, src, n):
        @pl.loop(0, n // 32)
        def _(r):
            o = pl.multiple_of(r * 32, 32)
            part[q, pl.ds(pl.multiple_of(off + r * 32, 32), 32)] += src[pl.ds(o, 32)]

    def rs_begin(t):
        part, buf = ((ypart, ybuf), (dxpart, dxbuf))[t]
        for j in range(4):
            rs(t, j).start()
        for j, q in enumerate((c_o, c_r, c_l, c)):
            rs(t, j).wait_recv()
            add_rows(part, q, k * tok, buf.at[q], tok)
            if j == 0:
                rs(t, 4).start()
                rs(t, 5).start()
            if j == 1:
                rs(t, 6).start()
            if j == 2:
                rs(t, 7).start()

    def rs_relay(t):
        part, ra, rb = ((ypart, yra, yrb), (dxpart, dxra, dxrb))[t]
        rs(t, 4).wait_recv()
        add_rows(part, c_r, k * tok, ra, half)
        rs(t, 8).start()
        rs(t, 5).wait_recv()
        add_rows(part, c_l, k * tok + half, rb, half)
        rs(t, 9).start()

    def rs_end(t):
        part, fl, fr, out = ((ypart, yfl, yfr, y_hbm), (dxpart, dxfl, dxfr, dx_hbm))[t]
        for j in (6, 7, 8, 9):
            rs(t, j).wait_recv()

        @pl.loop(0, tok // 32)
        def _(r):
            o = pl.multiple_of(r * 32, 32)
            total = part[c, pl.ds(pl.multiple_of(k * tok + r * 32, 32), 32)] + fl[pl.ds(o, 32)] + fr[pl.ds(o, 32)]
            outb[t, pl.ds(o, 32)] = total.astype(BF16)

        return pltpu.make_async_copy(outb.at[t], out, io_sem.at[t])

    rs_begin(0)
    ag(dy_all, 1, 4).wait_recv()
    ag(dy_all, 1, 5).wait_recv()
    ag(dy_all, 1, 9).start()
    ag(dy_all, 1, 6).wait_recv()
    ag(dy_all, 1, 10).start()
    for i in (7, 8, 9, 10):
        ag(dy_all, 1, i).wait_recv()
    for cpy in st_fwd(n_loc - 1, (n_loc - 1) % 2):
        cpy.wait()

    @pl.loop(0, n_loc)
    def _(e):
        s = lax.rem(e + n_loc, 2)
        hot = jnp.logical_and(is_owner, e == 0)

        @pl.when(e + 1 < n_loc)
        def _():
            for cpy in w_copies(e + n_loc + 1):
                cpy.start()

        for cpy in w_copies(e + n_loc):
            cpy.wait()

        @pl.when(e == 2)
        def _():
            rs_relay(0)

        @pl.when(jnp.logical_not(hot))
        def _():
            for q in range(chips):
                hit = pick_rows(q, e)
                gate = jnp.sum(jnp.where(hit, gt[q, pl.ds(e, 1), :], 0.0), axis=1, keepdims=True)
                got = dot_nn(jnp.where(hit, 1.0, 0.0).astype(BF16), dy_all[q])
                rows[s, q * cp:(q + 1) * cp, :] = (gate * got).astype(BF16)
            backward(n_rows, s, act_off(e))
            for q in range(chips):
                dxpart[q] += dot_nn(put_rows(q, e), orow[q * cp:(q + 1) * cp, :])

        @pl.when(hot)
        def _():
            @pl.loop(0, 2)
            def _(hb):
                for qq in range(chips // 2):
                    q = hb * (chips // 2) + qq
                    rows[s, qq * 2 * tok:(qq + 1) * 2 * tok, :] = (column(q, 8) * dy_all[q].astype(F32)).astype(BF16)
                backward(hb_rows, s, pl.multiple_of(hb * hb_rows, 64))
                for qq in range(chips // 2):
                    q = hb * (chips // 2) + qq
                    dxpart[q] += orow[qq * 2 * tok:(qq + 1) * 2 * tok, :].astype(F32)
                hot_store(hb, ((rows.at[s], dr_hbm, de_hbm), (darow.at[s], da_hbm, dae_hbm), (dbrow.at[s], db_hbm, dbe_hbm)))

        @pl.when(jnp.logical_and(e >= 1, jnp.logical_not(jnp.logical_and(is_owner, e == 1))))
        def _():
            for cpy in st_bwd(e - 1, 1 - s):
                cpy.wait()

        @pl.when(jnp.logical_not(hot))
        def _():
            for cpy in st_bwd(e, s):
                cpy.start()

    rs_begin(1)
    y_out = rs_end(0)
    y_out.start()
    rs_relay(1)
    dx_out = rs_end(1)
    dx_out.start()

    for cpy in st_bwd(n_loc - 1, (2 * n_loc - 1) % 2):
        cpy.wait()
    for d in range(1, group):
        meta_copy(d).wait_send()
    for i in range(11):
        ag(x_all, 0, i).wait_send()
        ag(dy_all, 1, i).wait_send()
    for j in range(10):
        rs(0, j).wait_send()
        rs(1, j).wait_send()
    y_out.wait()
    dx_out.wait()


def grad_kernel(owner, x_ref, d_ref, u_ref, da_ref, db_ref, xe, de, ue, dae, dbe, g1, g3, g2, xb, db_, ub, dab, dbb, sem):
    e = pl.program_id(0)
    hot = jnp.logical_and(lax.axis_index("ep") == owner, e == 0)

    @pl.when(jnp.logical_not(hot))
    def _():
        g1[0] = dot_tn(x_ref[0], da_ref[0]).astype(BF16)
        g3[0] = dot_tn(x_ref[0], db_ref[0]).astype(BF16)
        g2[0] = dot_tn(u_ref[0], d_ref[0]).astype(BF16)

    @pl.when(hot)
    def _():
        cps = [pltpu.make_async_copy(src, dst, sem.at[i]) for i, (src, dst) in enumerate(((xe, xb), (de, db_), (ue, ub), (dae, dab), (dbe, dbb)))]
        for cpy in cps:
            cpy.start()
        for cpy in cps:
            cpy.wait()
        g1[0] = (dot_tn(x_ref[0], da_ref[0]) + dot_tn(xb[...], dab[...])).astype(BF16)
        g3[0] = (dot_tn(x_ref[0], db_ref[0]) + dot_tn(xb[...], dbb[...])).astype(BF16)
        g2[0] = (dot_tn(u_ref[0], d_ref[0]) + dot_tn(ub[...], db_[...])).astype(BF16)


def solution(mesh):
    group = mesh.shape["ep"]
    num_dev = mesh.shape["dp"] * group
    tok_spec = P(("dp", "ep"), None)
    w_spec = P("ep", None, None)
    grad_spec = P(("dp", "ep"), None, None)

    def layer_fn(tokens, expert_ids, gate_vals, w_gate, w_up, w_down, grad_out):
        n_exp, width, hid = w_gate.shape
        tok = tokens.shape[0] // num_dev
        top_k = expert_ids.shape[1]
        cap = ((2 * tok * top_k + 8 * n_exp - 1) // (8 * n_exp)) * 8
        n_loc = n_exp // group
        hot = n_exp // 2
        owner = hot // n_loc
        chips = group // 2
        n_rows = chips * 2 * cap
        hot_rows = group * tok
        extra = hot_rows - n_rows
        cfg = (chips, tok, width, hid, n_loc, cap, owner)

        def device_fn(x, ids, gates, w1, w3, w2, dy):
            meta = jnp.concatenate([ids.T.astype(F32), gates.T], axis=0)
            any_spec = pl.BlockSpec(memory_space=pl.ANY)
            sds = jax.ShapeDtypeStruct
            hb = hot_rows // 2
            outs = pl.pallas_call(
                functools.partial(layer_kernel, cfg),
                out_shape=(
                    sds((tok, width), BF16), sds((tok, width), BF16),
                    sds((n_loc, n_rows, width), BF16), sds((n_loc, n_rows, width), BF16),
                    sds((n_loc, n_rows, hid), BF16), sds((n_loc, n_rows, hid), BF16), sds((n_loc, n_rows, hid), BF16),
                    sds((extra, width), BF16), sds((extra, width), BF16),
                    sds((extra, hid), BF16), sds((extra, hid), BF16), sds((extra, hid), BF16)),
                in_specs=[any_spec, any_spec, pl.BlockSpec(memory_space=pltpu.VMEM), any_spec, any_spec, any_spec],
                out_specs=[any_spec] * 12,
                scratch_shapes=[
                    pltpu.VMEM((chips, 2 * tok, width), BF16), pltpu.VMEM((chips, 2 * tok, width), BF16),
                    pltpu.VMEM((group, 16, tok), F32),
                    pltpu.VMEM((chips, 8, 2 * tok), F32), pltpu.VMEM((chips, 8, 2 * tok), F32),
                    pltpu.VMEM((chips, 2 * tok, 128), F32),
                    pltpu.VMEM((chips, 2 * tok, width), F32), pltpu.VMEM((chips, 2 * tok, width), F32),
                    pltpu.VMEM((chips, tok, width), F32), pltpu.VMEM((chips, tok, width), F32),
                    pltpu.VMEM((tok // 2, width), F32), pltpu.VMEM((tok // 2, width), F32),
                    pltpu.VMEM((tok, width), F32), pltpu.VMEM((tok, width), F32),
                    pltpu.VMEM((tok // 2, width), F32), pltpu.VMEM((tok // 2, width), F32),
                    pltpu.VMEM((tok, width), F32), pltpu.VMEM((tok, width), F32),
                    pltpu.VMEM((2, hb, width), BF16), pltpu.VMEM((2, hb, hid), BF16),
                    pltpu.VMEM((2, hb, hid), BF16), pltpu.VMEM((2, hb, hid), BF16),
                    pltpu.VMEM((hot_rows + (n_loc - 1) * n_rows, hid), F32), pltpu.VMEM((hot_rows + (n_loc - 1) * n_rows, hid), F32),
                    pltpu.VMEM((hb, width), BF16),
                    pltpu.VMEM((2, width, hid), BF16), pltpu.VMEM((2, width, hid), BF16), pltpu.VMEM((2, hid, width), BF16),
                    pltpu.VMEM((2, tok, width), BF16),
                    pltpu.SemaphoreType.DMA((group,)), pltpu.SemaphoreType.DMA((group,)),
                    pltpu.SemaphoreType.DMA((2, 11)), pltpu.SemaphoreType.DMA((2, 11)),
                    pltpu.SemaphoreType.DMA((2, 10)), pltpu.SemaphoreType.DMA((2, 10)),
                    pltpu.SemaphoreType.DMA((3, 2)), pltpu.SemaphoreType.DMA((3, 2)), pltpu.SemaphoreType.DMA((8,)),
                ],
                compiler_params=pltpu.CompilerParams(collective_id=0, has_side_effects=True, vmem_limit_bytes=67043328),
                name="moe_layer",
            )(x, dy, meta, w1, w3, w2)
            y, dx, xr, dr, ur, dar, dbr, xe, de, ue, dae, dbe = outs

            def blk(r, n):
                return pl.BlockSpec((1, r, n), lambda e: (e, 0, 0))

            g1, g3, g2 = pl.pallas_call(
                functools.partial(grad_kernel, owner),
                grid=(n_loc,),
                out_shape=(sds((n_loc, width, hid), BF16), sds((n_loc, width, hid), BF16), sds((n_loc, hid, width), BF16)),
                in_specs=[blk(n_rows, width), blk(n_rows, width), blk(n_rows, hid), blk(n_rows, hid), blk(n_rows, hid)] + [any_spec] * 5,
                out_specs=[blk(width, hid), blk(width, hid), blk(hid, width)],
                scratch_shapes=[pltpu.VMEM((extra, width), BF16), pltpu.VMEM((extra, width), BF16), pltpu.VMEM((extra, hid), BF16),
                                pltpu.VMEM((extra, hid), BF16), pltpu.VMEM((extra, hid), BF16), pltpu.SemaphoreType.DMA((5,))],
                compiler_params=pltpu.CompilerParams(vmem_limit_bytes=60 << 20),
                name="weight_grads",
            )(xr, dr, ur, dar, dbr, xe, de, ue, dae, dbe)
            return y, dx, g1, g3, g2

        return jax.shard_map(device_fn, mesh=mesh, in_specs=(tok_spec, tok_spec, tok_spec, w_spec, w_spec, w_spec, tok_spec),
                             out_specs=(tok_spec, tok_spec, grad_spec, grad_spec, grad_spec), check_vma=False)(
            tokens, expert_ids, gate_vals, w_gate, w_up, w_down, grad_out)

    return layer_fn
```

```python
import functools

import jax
import jax.numpy as jnp
from jax import lax
from jax.experimental import pallas as pl
from jax.experimental.pallas import tpu as pltpu
from jax.sharding import PartitionSpec as P

MESH = pl.DeviceIdType.MESH
F32 = jnp.float32
BF16 = jnp.bfloat16


def dot_nn(a, b):
    return lax.dot_general(a, b, (((1,), (0,)), ((), ())), preferred_element_type=F32)


def dot_nt(a, b):
    return lax.dot_general(a, b, (((1,), (1,)), ((), ())), preferred_element_type=F32)


def dot_tn(a, b):
    return lax.dot_general(a, b, (((0,), (0,)), ((), ())), preferred_element_type=F32)


def layer_kernel(cfg, x_hbm, dy_hbm, ids_ref, gates_ref, w1_hbm, w3_hbm, w2_hbm,
                 y_hbm, soa_hbm, sob_hbm, sra_hbm, srb_hbm, sla_hbm, slb_hbm, sc_hbm, xr_hbm, dr_hbm, ur_hbm, da_hbm, db_hbm, xe_hbm, de_hbm, ue_hbm, dae_hbm, dbe_hbm,
                 x_all, dy_all, ids_all, gates_all, rt, gt, mc, ypart, dxpart, ybuf, dxbuf, yra, yrb, yfl, yfr,
                 rows, urow, darow, dbrow, act1, act2, orow, w1, w3, w2, outb,
                 m_send, m_recv, ag_send, ag_recv, rs_send, rs_recv, w_sem, st_sem, io_sem, so_sem):
    chips, tok, width, hid, n_loc, cap, owner = cfg
    group = 2 * chips
    cp = 2 * cap
    n_rows = chips * cp
    hot_rows = chips * 2 * tok
    hb_rows = hot_rows // 2
    half = tok // 2
    me = lax.axis_index("ep")
    c = me // 2
    k = lax.rem(me, 2)
    c_r = lax.rem(c + 1, chips)
    c_l = lax.rem(c + chips - 1, chips)
    c_o = lax.rem(c + 2, chips)
    right = 2 * c_r + k
    left = 2 * c_l + k
    partner = 2 * c + 1 - k
    is_owner = me == owner

    own_x = pltpu.make_async_copy(x_hbm, x_all.at[c, pl.ds(k * tok, tok)], io_sem.at[0])
    own_dy = pltpu.make_async_copy(dy_hbm, dy_all.at[c, pl.ds(k * tok, tok)], io_sem.at[1])
    own_x.start()
    own_dy.start()

    def w_copies(i):
        e = lax.rem(i, n_loc)
        s = lax.rem(i, 2)
        return (pltpu.make_async_copy(w1_hbm.at[e], w1.at[s], w_sem.at[0, s]),
                pltpu.make_async_copy(w3_hbm.at[e], w3.at[s], w_sem.at[1, s]),
                pltpu.make_async_copy(w2_hbm.at[e], w2.at[s], w_sem.at[2, s]))

    for cpy in w_copies(0):
        cpy.start()
    ids_all[me] = ids_ref[...]
    gates_all[me] = gates_ref[...]

    barrier = pltpu.get_barrier_semaphore()
    for d in range(1, group):
        pl.semaphore_signal(barrier, inc=1, device_id={"ep": lax.rem(me + d, group)}, device_id_type=MESH)
    pl.semaphore_wait(barrier, group - 1)

    def meta_copies(d):
        return tuple(pltpu.make_async_remote_copy(
            src_ref=src, dst_ref=dst.at[me], send_sem=m_send.at[i, d], recv_sem=m_recv.at[i, d],
            device_id={"ep": lax.rem(me + d, group)}, device_id_type=MESH)
            for i, (src, dst) in enumerate(((ids_ref, ids_all), (gates_ref, gates_all))))

    def ag(ref, t, i):
        chip, core, r0, n, dev = (
            (c, k, 0, half, right), (c, k, half, half, right), (c, k, half, half, left), (c, k, 0, half, left),
            (c, k, 0, tok, partner),
            (c_l, k, 0, half, right), (c_r, k, half, half, left),
            (c_l, k, 0, tok, partner), (c_r, k, 0, tok, partner),
            (c_o, k, 0, half, partner), (c_o, k, half, half, partner))[i]
        blk = ref.at[chip, pl.ds(core * tok + r0, n)]
        return pltpu.make_async_remote_copy(
            src_ref=blk, dst_ref=blk, send_sem=ag_send.at[t, i], recv_sem=ag_recv.at[t, i],
            device_id={"ep": dev}, device_id_type=MESH)

    own_x.wait()
    for d in range(1, group):
        for cpy in meta_copies(d):
            cpy.start()
    for i in (0, 2, 1, 3, 4):
        ag(x_all, 0, i).start()
    own_dy.wait()

    @pl.loop(0, chips * 2 * tok // 64)
    def _(r):
        q = r // (2 * tok // 64)
        o = pl.multiple_of(lax.rem(r, 2 * tok // 64) * 64, 64)
        ypart[q, pl.ds(o, 64)] = jnp.zeros((64, width), F32)
        dxpart[q, pl.ds(o, 64)] = jnp.zeros((64, width), F32)

    for d in range(1, group):
        for cpy in meta_copies(d):
            cpy.wait_recv()

    upper = (lax.broadcasted_iota(jnp.int32, (tok, tok), 0) < lax.broadcasted_iota(jnp.int32, (tok, tok), 1)).astype(F32).astype(BF16)
    row_id = lax.broadcasted_iota(jnp.int32, (8, tok), 0)
    for s in range(group):
        q, core = s // 2, s % 2
        ids = ids_all[s]
        gates = gates_all[s]
        mask_m = jnp.zeros((8, tok), F32)
        gate_m = jnp.zeros((8, tok), F32)
        for le in range(n_loc):
            eq = ids == me * n_loc + le
            hit = jnp.sum(jnp.where(eq, 1.0, 0.0), axis=0, keepdims=True)
            gv = jnp.sum(jnp.where(eq, gates, 0.0), axis=0, keepdims=True)
            mask_m = jnp.where(row_id == le, hit, mask_m)
            gate_m = jnp.where(row_id == le, gv, gate_m)
        rank = dot_nn(mask_m.astype(BF16), upper)
        pos = jnp.where(mask_m > 0.0, rank + float(cap * core), -1.0)
        rt[q, :, core * tok:(core + 1) * tok] = pos
        gt[q, :, core * tok:(core + 1) * tok] = gate_m
        both = jnp.concatenate([pos, gate_m, jnp.zeros((tok - 16, tok), F32)], axis=0)
        mc[q, core * tok:(core + 1) * tok, :] = jnp.transpose(both)

    ag(x_all, 0, 0).wait_recv()
    ag(x_all, 0, 5).start()
    ag(x_all, 0, 2).wait_recv()
    ag(x_all, 0, 6).start()
    for i in (0, 2, 1, 3, 4):
        ag(dy_all, 1, i).start()
    ag(x_all, 0, 1).wait_recv()
    ag(x_all, 0, 7).start()
    ag(x_all, 0, 3).wait_recv()
    ag(x_all, 0, 8).start()
    ag(x_all, 0, 4).wait_recv()
    ag(x_all, 0, 5).wait_recv()
    ag(x_all, 0, 9).start()
    ag(x_all, 0, 6).wait_recv()
    ag(x_all, 0, 10).start()
    for i in (7, 8, 9, 10):
        ag(x_all, 0, i).wait_recv()

    def pick_rows(q, e):
        hit = rt[q, pl.ds(e, 1), :] == lax.broadcasted_iota(jnp.int32, (cp, 2 * tok), 0).astype(F32)
        return hit

    def column(q, lane):
        m = mc[q]
        return jnp.sum(jnp.where(lax.broadcasted_iota(jnp.int32, (2 * tok, 128), 1) == lane, m, 0.0), axis=1, keepdims=True)

    def put_rows(q, e):
        hit = column(q, e) == lax.broadcasted_iota(jnp.int32, (2 * tok, cp), 1).astype(F32)
        return jnp.where(hit, 1.0, 0.0).astype(BF16)

    def forward(m, s, aoff):
        for j in range(hid // 256):
            cs = slice(j * 256, (j + 1) * 256)
            act1[pl.ds(aoff, m), cs] = dot_nn(rows[s, 0:m, :], w1[s, :, cs])
            act2[pl.ds(aoff, m), cs] = dot_nn(rows[s, 0:m, :], w3[s, :, cs])

        @pl.loop(0, m // 32)
        def _(r):
            o = pl.multiple_of(aoff + r * 32, 32)
            a = act1[pl.ds(o, 32), :]
            b = act2[pl.ds(o, 32), :]
            sg = jax.nn.sigmoid(a)
            ga = a * sg
            act1[pl.ds(o, 32), :] = b * (sg * (1.0 + a * (1.0 - sg)))
            act2[pl.ds(o, 32), :] = ga
            urow[s, pl.ds(pl.multiple_of(r * 32, 32), 32), :] = (ga * b).astype(BF16)

        for j in range(width // 256):
            cs = slice(j * 256, (j + 1) * 256)
            orow[0:m, cs] = dot_nn(urow[s, 0:m, :], w2[s, :, cs]).astype(BF16)

    def backward(m, s, aoff):
        for j in range(hid // 256):
            cs = slice(j * 256, (j + 1) * 256)
            du = dot_nt(rows[s, 0:m, :], w2[s, cs, :])
            darow[s, 0:m, cs] = (du * act1[pl.ds(aoff, m), cs]).astype(BF16)
            dbrow[s, 0:m, cs] = (du * act2[pl.ds(aoff, m), cs]).astype(BF16)
        for j in range(width // 256):
            cs = slice(j * 256, (j + 1) * 256)
            orow[0:m, cs] = (dot_nt(darow[s, 0:m, :], w1[s, cs, :]) + dot_nt(dbrow[s, 0:m, :], w3[s, cs, :])).astype(BF16)

    def act_off(e):
        return pl.multiple_of(jnp.where(e == 0, 0, hot_rows + (e - 1) * n_rows), 64)

    def st_fwd(e, s):
        return (pltpu.make_async_copy(rows.at[s, 0:n_rows], xr_hbm.at[e], st_sem.at[0, s]),
                pltpu.make_async_copy(urow.at[s, 0:n_rows], ur_hbm.at[e], st_sem.at[1, s]))

    def st_bwd(e, s):
        return (pltpu.make_async_copy(rows.at[s, 0:n_rows], dr_hbm.at[e], st_sem.at[0, s]),
                pltpu.make_async_copy(darow.at[s, 0:n_rows], da_hbm.at[e], st_sem.at[1, s]),
                pltpu.make_async_copy(dbrow.at[s, 0:n_rows], db_hbm.at[e], st_sem.at[2, s]))

    def hot_store(hb, pairs):
        rest = hb_rows - n_rows

        @pl.when(hb == 0)
        def _():
            cps = []
            for t, (src, main, extra) in enumerate(pairs):
                cps.append(pltpu.make_async_copy(src.at[0:n_rows], main.at[0], io_sem.at[2 + 2 * t]))
                cps.append(pltpu.make_async_copy(src.at[n_rows:hb_rows], extra.at[0:rest], io_sem.at[3 + 2 * t]))
            for cpy in cps:
                cpy.start()
            for cpy in cps:
                cpy.wait()

        @pl.when(hb == 1)
        def _():
            cps = [pltpu.make_async_copy(src.at[0:hb_rows], extra.at[rest:rest + hb_rows], io_sem.at[2 + 2 * t])
                   for t, (src, main, extra) in enumerate(pairs)]
            for cpy in cps:
                cpy.start()
            for cpy in cps:
                cpy.wait()

    @pl.loop(0, n_loc)
    def _(e):
        s = lax.rem(e, 2)
        hot = jnp.logical_and(is_owner, e == 0)
        for cpy in w_copies(e + 1):
            cpy.start()
        for cpy in w_copies(e):
            cpy.wait()

        @pl.when(e == 1)
        def _():
            ag(dy_all, 1, 0).wait_recv()
            ag(dy_all, 1, 5).start()
            ag(dy_all, 1, 2).wait_recv()
            ag(dy_all, 1, 6).start()

        @pl.when(e == 3)
        def _():
            ag(dy_all, 1, 1).wait_recv()
            ag(dy_all, 1, 7).start()
            ag(dy_all, 1, 3).wait_recv()
            ag(dy_all, 1, 8).start()

        @pl.when(jnp.logical_not(hot))
        def _():
            for q in range(chips):
                hit = jnp.where(pick_rows(q, e), 1.0, 0.0).astype(BF16)
                rows[s, q * cp:(q + 1) * cp, :] = dot_nn(hit, x_all[q]).astype(BF16)
            forward(n_rows, s, act_off(e))
            for q in range(chips):
                gate = column(q, e + 8)
                ypart[q] += gate * dot_nn(put_rows(q, e), orow[q * cp:(q + 1) * cp, :])

        @pl.when(hot)
        def _():
            @pl.loop(0, 2)
            def _(hb):
                for qq in range(chips // 2):
                    q = hb * (chips // 2) + qq
                    on = column(q, 0) >= 0.0
                    rows[0, qq * 2 * tok:(qq + 1) * 2 * tok, :] = jnp.where(on, x_all[q].astype(F32), 0.0).astype(BF16)
                forward(hb_rows, 0, pl.multiple_of(hb * hb_rows, 64))
                for qq in range(chips // 2):
                    q = hb * (chips // 2) + qq
                    ypart[q] += column(q, 8) * orow[qq * 2 * tok:(qq + 1) * 2 * tok, :].astype(F32)
                hot_store(hb, ((rows.at[0], xr_hbm, xe_hbm), (urow.at[0], ur_hbm, ue_hbm)))

        @pl.when(jnp.logical_and(e >= 1, jnp.logical_not(jnp.logical_and(is_owner, e == 1))))
        def _():
            for cpy in st_fwd(e - 1, 1 - s):
                cpy.wait()

        @pl.when(jnp.logical_not(hot))
        def _():
            for cpy in st_fwd(e, s):
                cpy.start()

    def rs(t, j):
        part, buf = ((ypart, ybuf), (dxpart, dxbuf))[t]
        o = k * tok
        if j < 4:
            q = (c_o, c_r, c_l, c)[j]
            src, dst, dev = part.at[q, pl.ds((1 - k) * tok, tok)], buf.at[q], partner
        else:
            src, dst, dev = (
                (part.at[c_o, pl.ds(o, half)], yra, right),
                (part.at[c_o, pl.ds(o + half, half)], yrb, left),
                (part.at[c_r, pl.ds(o + half, half)], yfl.at[half:tok], right),
                (part.at[c_l, pl.ds(o, half)], yfr.at[0:half], left),
                (part.at[c_r, pl.ds(o, half)], yfl.at[0:half], right),
                (part.at[c_l, pl.ds(o + half, half)], yfr.at[half:tok], left))[j - 4]
        return pltpu.make_async_remote_copy(
            src_ref=src, dst_ref=dst, send_sem=rs_send.at[t, j], recv_sem=rs_recv.at[t, j],
            device_id={"ep": dev}, device_id_type=MESH)

    def add_rows(part, q, off, src, n):
        @pl.loop(0, n // 32)
        def _(r):
            o = pl.multiple_of(r * 32, 32)
            part[q, pl.ds(pl.multiple_of(off + r * 32, 32), 32)] += src[pl.ds(o, 32)]

    def rs_begin_y():
        for j in range(4):
            rs(0, j).start()
        for j, q in enumerate((c_o, c_r, c_l, c)):
            rs(0, j).wait_recv()
            add_rows(ypart, q, k * tok, ybuf.at[q], tok)
            if j == 0:
                rs(0, 4).start()
                rs(0, 5).start()
            if j == 1:
                rs(0, 6).start()
            if j == 2:
                rs(0, 7).start()

    def rs_relay_y():
        rs(0, 4).wait_recv()
        add_rows(ypart, c_r, k * tok, yra, half)
        rs(0, 8).start()
        rs(0, 5).wait_recv()
        add_rows(ypart, c_l, k * tok + half, yrb, half)
        rs(0, 9).start()

    def rs_end_y():
        for j in (6, 7, 8, 9):
            rs(0, j).wait_recv()

        @pl.loop(0, tok // 32)
        def _(r):
            o = pl.multiple_of(r * 32, 32)
            total = ypart[c, pl.ds(pl.multiple_of(k * tok + r * 32, 32), 32)] + yfl[pl.ds(o, 32)] + yfr[pl.ds(o, 32)]
            outb[pl.ds(o, 32)] = total.astype(BF16)

        return pltpu.make_async_copy(outb, y_hbm, io_sem.at[0])

    def chip_sums_out(j):
        q = (c_o, c_r, c_l, c)[j]
        if j == 3:
            return (pltpu.make_async_copy(dxpart.at[q, pl.ds(k * tok, tok)], sc_hbm, so_sem.at[6]),)
        lo, hi = ((soa_hbm, sob_hbm), (sra_hbm, srb_hbm), (sla_hbm, slb_hbm))[j]
        return (pltpu.make_async_copy(dxpart.at[q, pl.ds(k * tok, half)], lo, so_sem.at[2 * j]),
                pltpu.make_async_copy(dxpart.at[q, pl.ds(k * tok + half, half)], hi, so_sem.at[2 * j + 1]))

    rs_begin_y()
    ag(dy_all, 1, 4).wait_recv()
    ag(dy_all, 1, 5).wait_recv()
    ag(dy_all, 1, 9).start()
    ag(dy_all, 1, 6).wait_recv()
    ag(dy_all, 1, 10).start()
    for i in (7, 8, 9, 10):
        ag(dy_all, 1, i).wait_recv()
    for cpy in st_fwd(n_loc - 1, (n_loc - 1) % 2):
        cpy.wait()

    @pl.loop(0, n_loc)
    def _(e):
        s = lax.rem(e + n_loc, 2)
        hot = jnp.logical_and(is_owner, e == 0)

        @pl.when(e + 1 < n_loc)
        def _():
            for cpy in w_copies(e + n_loc + 1):
                cpy.start()

        for cpy in w_copies(e + n_loc):
            cpy.wait()

        @pl.when(e == n_loc - 1)
        def _():
            rs_relay_y()

        @pl.when(jnp.logical_not(hot))
        def _():
            for q in range(chips):
                hit = pick_rows(q, e)
                gate = jnp.sum(jnp.where(hit, gt[q, pl.ds(e, 1), :], 0.0), axis=1, keepdims=True)
                got = dot_nn(jnp.where(hit, 1.0, 0.0).astype(BF16), dy_all[q])
                rows[s, q * cp:(q + 1) * cp, :] = (gate * got).astype(BF16)
            backward(n_rows, s, act_off(e))
            for q in range(chips):
                dxpart[q] += dot_nn(put_rows(q, e), orow[q * cp:(q + 1) * cp, :])

        @pl.when(hot)
        def _():
            @pl.loop(0, 2)
            def _(hb):
                for qq in range(chips // 2):
                    q = hb * (chips // 2) + qq
                    rows[s, qq * 2 * tok:(qq + 1) * 2 * tok, :] = (column(q, 8) * dy_all[q].astype(F32)).astype(BF16)
                backward(hb_rows, s, pl.multiple_of(hb * hb_rows, 64))
                for qq in range(chips // 2):
                    q = hb * (chips // 2) + qq
                    dxpart[q] += orow[qq * 2 * tok:(qq + 1) * 2 * tok, :].astype(F32)
                hot_store(hb, ((rows.at[s], dr_hbm, de_hbm), (darow.at[s], da_hbm, dae_hbm), (dbrow.at[s], db_hbm, dbe_hbm)))

        @pl.when(jnp.logical_and(e >= 1, jnp.logical_not(jnp.logical_and(is_owner, e == 1))))
        def _():
            for cpy in st_bwd(e - 1, 1 - s):
                cpy.wait()

        @pl.when(jnp.logical_not(hot))
        def _():
            for cpy in st_bwd(e, s):
                cpy.start()

    for j in range(4):
        rs(1, j).start()
    for j, q in enumerate((c_o, c_r, c_l, c)):
        rs(1, j).wait_recv()
        add_rows(dxpart, q, k * tok, dxbuf.at[q], tok)
        for cpy in chip_sums_out(j):
            cpy.start()
    y_out = rs_end_y()
    y_out.start()

    for cpy in st_bwd(n_loc - 1, (2 * n_loc - 1) % 2):
        cpy.wait()
    for d in range(1, group):
        for cpy in meta_copies(d):
            cpy.wait_send()
    for i in range(11):
        ag(x_all, 0, i).wait_send()
        ag(dy_all, 1, i).wait_send()
    for j in range(10):
        rs(0, j).wait_send()
    for j in range(4):
        rs(1, j).wait_send()
        for cpy in chip_sums_out(j):
            cpy.wait()
    y_out.wait()


def expert_grads(x_ref, d_ref, u_ref, da_ref, db_ref, g1, g3, g2):
    g1[0] = dot_tn(x_ref[0], da_ref[0]).astype(BF16)
    g3[0] = dot_tn(x_ref[0], db_ref[0]).astype(BF16)
    g2[0] = dot_tn(u_ref[0], d_ref[0]).astype(BF16)


def first_grads_kernel(owner, x_ref, d_ref, u_ref, da_ref, db_ref, xe, de, ue, dae, dbe, g1, g3, g2, xb, db_, ub, dab, dbb, sem):
    e = pl.program_id(0)
    hot = jnp.logical_and(lax.axis_index("ep") == owner, e == 0)

    @pl.when(jnp.logical_not(hot))
    def _():
        expert_grads(x_ref, d_ref, u_ref, da_ref, db_ref, g1, g3, g2)

    @pl.when(hot)
    def _():
        cps = [pltpu.make_async_copy(src, dst, sem.at[i]) for i, (src, dst) in enumerate(((xe, xb), (de, db_), (ue, ub), (dae, dab), (dbe, dbb)))]
        for cpy in cps:
            cpy.start()
        for cpy in cps:
            cpy.wait()
        g1[0] = (dot_tn(x_ref[0], da_ref[0]) + dot_tn(xb[...], dab[...])).astype(BF16)
        g3[0] = (dot_tn(x_ref[0], db_ref[0]) + dot_tn(xb[...], dbb[...])).astype(BF16)
        g2[0] = (dot_tn(u_ref[0], d_ref[0]) + dot_tn(ub[...], db_[...])).astype(BF16)


def later_grads_kernel(x_ref, d_ref, u_ref, da_ref, db_ref, g1_in, g3_in, g2_in, g1, g3, g2):
    del g1_in, g3_in, g2_in
    expert_grads(x_ref, d_ref, u_ref, da_ref, db_ref, g1, g3, g2)


def solution(mesh):
    group = mesh.shape["ep"]
    num_dev = mesh.shape["dp"] * group
    tok_spec = P(("dp", "ep"), None)
    w_spec = P("ep", None, None)
    grad_spec = P(("dp", "ep"), None, None)

    def layer_fn(tokens, expert_ids, gate_vals, w_gate, w_up, w_down, grad_out):
        n_exp, width, hid = w_gate.shape
        tok = tokens.shape[0] // num_dev
        top_k = expert_ids.shape[1]
        cap = ((2 * tok * top_k + 8 * n_exp - 1) // (8 * n_exp)) * 8
        n_loc = n_exp // group
        hot = n_exp // 2
        owner = hot // n_loc
        chips = group // 2
        n_rows = chips * 2 * cap
        hot_rows = group * tok
        extra = hot_rows - n_rows
        cfg = (chips, tok, width, hid, n_loc, cap, owner)

        def device_fn(x, ids, gates, w1, w3, w2, dy):
            any_spec = pl.BlockSpec(memory_space=pl.ANY)
            vmem_spec = pl.BlockSpec(memory_space=pltpu.VMEM)
            sds = jax.ShapeDtypeStruct
            hb = hot_rows // 2
            half = tok // 2
            act_rows = hot_rows + (n_loc - 1) * n_rows
            outs = pl.pallas_call(
                functools.partial(layer_kernel, cfg),
                out_shape=(
                    sds((tok, width), BF16), *[sds((half, width), F32)] * 6, sds((tok, width), F32),
                    sds((n_loc, n_rows, width), BF16), sds((n_loc, n_rows, width), BF16),
                    sds((n_loc, n_rows, hid), BF16), sds((n_loc, n_rows, hid), BF16), sds((n_loc, n_rows, hid), BF16),
                    sds((extra, width), BF16), sds((extra, width), BF16),
                    sds((extra, hid), BF16), sds((extra, hid), BF16), sds((extra, hid), BF16)),
                in_specs=[any_spec, any_spec, vmem_spec, vmem_spec, any_spec, any_spec, any_spec],
                out_specs=[any_spec] * 18,
                scratch_shapes=[
                    pltpu.VMEM((chips, 2 * tok, width), BF16), pltpu.VMEM((chips, 2 * tok, width), BF16),
                    pltpu.VMEM((group, top_k, tok), jnp.int32), pltpu.VMEM((group, top_k, tok), F32),
                    pltpu.VMEM((chips, 8, 2 * tok), F32), pltpu.VMEM((chips, 8, 2 * tok), F32),
                    pltpu.VMEM((chips, 2 * tok, 128), F32),
                    pltpu.VMEM((chips, 2 * tok, width), F32), pltpu.VMEM((chips, 2 * tok, width), F32),
                    pltpu.VMEM((chips, tok, width), F32), pltpu.VMEM((chips, tok, width), F32),
                    pltpu.VMEM((half, width), F32), pltpu.VMEM((half, width), F32),
                    pltpu.VMEM((tok, width), F32), pltpu.VMEM((tok, width), F32),
                    pltpu.VMEM((2, hb, width), BF16), pltpu.VMEM((2, hb, hid), BF16),
                    pltpu.VMEM((2, hb, hid), BF16), pltpu.VMEM((2, hb, hid), BF16),
                    pltpu.VMEM((act_rows, hid), F32), pltpu.VMEM((act_rows, hid), F32),
                    pltpu.VMEM((hb, width), BF16),
                    pltpu.VMEM((2, width, hid), BF16), pltpu.VMEM((2, width, hid), BF16), pltpu.VMEM((2, hid, width), BF16),
                    pltpu.VMEM((tok, width), BF16),
                    pltpu.SemaphoreType.DMA((2, group)), pltpu.SemaphoreType.DMA((2, group)),
                    pltpu.SemaphoreType.DMA((2, 11)), pltpu.SemaphoreType.DMA((2, 11)),
                    pltpu.SemaphoreType.DMA((2, 10)), pltpu.SemaphoreType.DMA((2, 10)),
                    pltpu.SemaphoreType.DMA((3, 2)), pltpu.SemaphoreType.DMA((3, 2)), pltpu.SemaphoreType.DMA((8,)),
                    pltpu.SemaphoreType.DMA((7,)),
                ],
                compiler_params=pltpu.CompilerParams(collective_id=0, has_side_effects=True, vmem_limit_bytes=67043328),
                name="moe_layer",
            )(x, dy, ids.T, gates.T, w1, w3, w2)
            y, soa, sob, sra, srb, sla, slb, sc, xr, dr, ur, dar, dbr, xe, de, ue, dae, dbe = outs

            to_right = [(i, (i + 2) % group) for i in range(group)]
            to_left = [(i, (i + group - 2) % group) for i in range(group)]
            ra = lax.ppermute(soa, "ep", to_right)
            rb = lax.ppermute(sob, "ep", to_left)
            fl_hi = lax.ppermute(srb, "ep", to_right)
            fr_lo = lax.ppermute(sla, "ep", to_left)

            n_first = (n_loc + 1) // 2
            g_shapes = (sds((n_loc, width, hid), BF16), sds((n_loc, width, hid), BF16), sds((n_loc, hid, width), BF16))

            def blk(r, n, first):
                return pl.BlockSpec((1, r, n), lambda e: (e + first, 0, 0))

            def row_specs(first):
                return [blk(n_rows, width, first), blk(n_rows, width, first), blk(n_rows, hid, first), blk(n_rows, hid, first), blk(n_rows, hid, first)]

            def out_blks(first):
                return [blk(width, hid, first), blk(width, hid, first), blk(hid, width, first)]

            def cost(n):
                return pl.CostEstimate(flops=n * 6 * n_rows * width * hid, transcendentals=0,
                                       bytes_accessed=n * 2 * (2 * n_rows * width + 3 * n_rows * hid + 3 * width * hid))

            grads = pl.pallas_call(
                functools.partial(first_grads_kernel, owner),
                grid=(n_first,), out_shape=g_shapes,
                in_specs=row_specs(0) + [any_spec] * 5, out_specs=out_blks(0),
                scratch_shapes=[pltpu.VMEM((extra, width), BF16), pltpu.VMEM((extra, width), BF16), pltpu.VMEM((extra, hid), BF16),
                                pltpu.VMEM((extra, hid), BF16), pltpu.VMEM((extra, hid), BF16), pltpu.SemaphoreType.DMA((5,))],
                compiler_params=pltpu.CompilerParams(vmem_limit_bytes=60 << 20),
                cost_estimate=cost(n_first), name="first_grads",
            )(xr, dr, ur, dar, dbr, xe, de, ue, dae, dbe)

            fl_lo = lax.ppermute(sra + ra, "ep", to_right)
            fr_hi = lax.ppermute(slb + rb, "ep", to_left)
            g1, g3, g2 = pl.pallas_call(
                later_grads_kernel,
                grid=(n_loc - n_first,), out_shape=g_shapes,
                in_specs=row_specs(n_first) + [any_spec] * 3, out_specs=out_blks(n_first),
                input_output_aliases={5: 0, 6: 1, 7: 2},
                compiler_params=pltpu.CompilerParams(vmem_limit_bytes=60 << 20),
                cost_estimate=cost(n_loc - n_first), name="later_grads",
            )(xr, dr, ur, dar, dbr, *grads)
            fl = jnp.concatenate([fl_lo, fl_hi], axis=0)
            fr = jnp.concatenate([fr_lo, fr_hi], axis=0)
            dx = (sc + fl + fr).astype(BF16)
            return y, dx, g1, g3, g2

        return jax.shard_map(device_fn, mesh=mesh, in_specs=(tok_spec, tok_spec, tok_spec, w_spec, w_spec, w_spec, tok_spec),
                             out_specs=(tok_spec, tok_spec, grad_spec, grad_spec, grad_spec), check_vma=False)(
            tokens, expert_ids, gate_vals, w_gate, w_up, w_down, grad_out)

    return layer_fn
```

```python
import functools

import jax
import jax.numpy as jnp
from jax import lax
from jax.experimental import pallas as pl
from jax.experimental.pallas import tpu as pltpu
from jax.sharding import PartitionSpec as P

MESH = pl.DeviceIdType.MESH
F32 = jnp.float32
BF16 = jnp.bfloat16


def dot_nn(a, b):
    return lax.dot_general(a, b, (((1,), (0,)), ((), ())), preferred_element_type=F32)


def dot_nt(a, b):
    return lax.dot_general(a, b, (((1,), (1,)), ((), ())), preferred_element_type=F32)


def dot_tn(a, b):
    return lax.dot_general(a, b, (((0,), (0,)), ((), ())), preferred_element_type=F32)


def layer_kernel(cfg, x_hbm, dy_hbm, ids_ref, gates_ref, w1_hbm, w3_hbm, w2_hbm,
                 y_hbm, soa_hbm, sob_hbm, sra_hbm, srb_hbm, sla_hbm, slb_hbm, sc_hbm, xr_hbm, dr_hbm, ur_hbm, da_hbm, db_hbm, xh_hbm, dh_hbm, uh_hbm, dah_hbm, dbh_hbm,
                 x_all, dy_all, ids_all, gates_all, rt, gt, mc, ypart, dxpart, cbuf, yra, yrb, yfl, yfr,
                 erows, hrows, urow, uhot, darow, dbrow, act1, act2, orow, pbuf, w1, w3, w2, outb,
                 m_send, m_recv, ag_send, ag_recv, rs_send, rs_recv, w_sem, st_sem, hst_sem, io_sem, so_sem, free_sem):
    chips, tok, width, hid, n_loc, cap, owner = cfg
    group = 2 * chips
    two = 2 * tok
    cp = 2 * cap
    n_rows = chips * cp
    hot_rows = chips * two
    half = tok // 2
    last = n_loc - 1
    me = lax.axis_index("ep")
    c = me // 2
    k = lax.rem(me, 2)
    c_r = lax.rem(c + 1, chips)
    c_l = lax.rem(c + chips - 1, chips)
    c_o = lax.rem(c + 2, chips)
    near = (c, c_l, c_r, c_o)
    right = 2 * c_r + k
    left = 2 * c_l + k
    partner = 2 * c + 1 - k
    is_owner = me == owner

    own_x = pltpu.make_async_copy(x_hbm, x_all.at[c, pl.ds(k * tok, tok)], io_sem.at[0])
    own_dy = pltpu.make_async_copy(dy_hbm, dy_all.at[c, pl.ds(k * tok, tok)], io_sem.at[1])
    own_x.start()
    own_dy.start()

    def w_copies(i):
        e = lax.rem(i, n_loc)
        s = lax.rem(i, 2)
        return (pltpu.make_async_copy(w1_hbm.at[e], w1.at[s], w_sem.at[0, s]),
                pltpu.make_async_copy(w3_hbm.at[e], w3.at[s], w_sem.at[1, s]),
                pltpu.make_async_copy(w2_hbm.at[e], w2.at[s], w_sem.at[2, s]))

    for cpy in w_copies(0):
        cpy.start()
    ids_all[me] = ids_ref[...]
    gates_all[me] = gates_ref[...]

    barrier = pltpu.get_barrier_semaphore()
    for d in range(1, group):
        pl.semaphore_signal(barrier, inc=1, device_id={"ep": lax.rem(me + d, group)}, device_id_type=MESH)
    pl.semaphore_wait(barrier, group - 1)

    def meta_copies(d):
        return tuple(pltpu.make_async_remote_copy(
            src_ref=src, dst_ref=dst.at[me], send_sem=m_send.at[i, d], recv_sem=m_recv.at[i, d],
            device_id={"ep": lax.rem(me + d, group)}, device_id_type=MESH)
            for i, (src, dst) in enumerate(((ids_ref, ids_all), (gates_ref, gates_all))))

    def ag(ref, t, i):
        chip, core, r0, n, dev = (
            (c, k, 0, half, right), (c, k, half, half, right), (c, k, half, half, left), (c, k, 0, half, left),
            (c, k, 0, tok, partner),
            (c_l, k, 0, half, right), (c_r, k, half, half, left),
            (c_l, k, 0, tok, partner), (c_r, k, 0, tok, partner),
            (c_o, k, 0, half, partner), (c_o, k, half, half, partner))[i]
        blk = ref.at[chip, pl.ds(core * tok + r0, n)]
        return pltpu.make_async_remote_copy(
            src_ref=blk, dst_ref=blk, send_sem=ag_send.at[t, i], recv_sem=ag_recv.at[t, i],
            device_id={"ep": dev}, device_id_type=MESH)

    own_x.wait()
    for d in range(1, group):
        for cpy in meta_copies(d):
            cpy.start()
    for i in (4, 0, 2, 1, 3):
        ag(x_all, 0, i).start()
    own_dy.wait()

    @pl.loop(0, chips * two // 64)
    def _(r):
        q = r // (two // 64)
        o = pl.multiple_of(lax.rem(r, two // 64) * 64, 64)
        ypart[q, pl.ds(o, 64)] = jnp.zeros((64, width), F32)
        dxpart[q, pl.ds(o, 64)] = jnp.zeros((64, width), F32)

    for d in range(1, group):
        for cpy in meta_copies(d):
            cpy.wait_recv()

    upper = (lax.broadcasted_iota(jnp.int32, (tok, tok), 0) < lax.broadcasted_iota(jnp.int32, (tok, tok), 1)).astype(F32).astype(BF16)
    row_id = lax.broadcasted_iota(jnp.int32, (8, tok), 0)
    for s in range(group):
        q, core = s // 2, s % 2
        ids = ids_all[s]
        gates = gates_all[s]
        mask_m = jnp.zeros((8, tok), F32)
        gate_m = jnp.zeros((8, tok), F32)
        for le in range(n_loc):
            eq = ids == me * n_loc + le
            hit = jnp.sum(jnp.where(eq, 1.0, 0.0), axis=0, keepdims=True)
            gv = jnp.sum(jnp.where(eq, gates, 0.0), axis=0, keepdims=True)
            mask_m = jnp.where(row_id == le, hit, mask_m)
            gate_m = jnp.where(row_id == le, gv, gate_m)
        rank = dot_nn(mask_m.astype(BF16), upper)
        pos = jnp.where(mask_m > 0.0, rank + float(cap * core), -1.0)
        rt[q, :, core * tok:(core + 1) * tok] = pos
        gt[q, :, core * tok:(core + 1) * tok] = gate_m
        both = jnp.concatenate([pos, gate_m, jnp.zeros((tok - 16, tok), F32)], axis=0)
        mc[q, core * tok:(core + 1) * tok, :] = jnp.transpose(both)

    def pick(p, q, src, scaled):
        for e in range(n_loc):
            hit = rt[q, e:e + 1, :] == lax.broadcasted_iota(jnp.int32, (cp, two), 0).astype(F32)
            pbuf[e * cp:(e + 1) * cp, :] = jnp.where(hit, 1.0, 0.0).astype(BF16)
        gates = [None] * n_loc
        if scaled:
            for e in range(n_loc):
                hit = rt[q, e:e + 1, :] == lax.broadcasted_iota(jnp.int32, (cp, two), 0).astype(F32)
                gates[e] = jnp.sum(jnp.where(hit, gt[q, e:e + 1, :], 0.0), axis=1, keepdims=True)
        for j in range(width // 256):
            cs = slice(j * 256, (j + 1) * 256)
            got = dot_nn(pbuf[...], src[q, :, cs])
            for e in range(n_loc):
                part = got[e * cp:(e + 1) * cp]
                erows[e, pl.ds(p * cp, cp), cs] = (gates[e] * part if scaled else part).astype(BF16)

    def column(q, lane):
        return jnp.sum(jnp.where(lax.broadcasted_iota(jnp.int32, (two, 128), 1) == lane, mc[q], 0.0), axis=1, keepdims=True)

    def put_rows(q, e):
        hit = column(q, e) == lax.broadcasted_iota(jnp.int32, (two, cp), 1).astype(F32)
        return jnp.where(hit, 1.0, 0.0).astype(BF16)

    def forward(m, src, dst, s, aoff):
        for j in range(hid // 256):
            cs = slice(j * 256, (j + 1) * 256)
            act1[pl.ds(aoff, m), cs] = dot_nn(src[...], w1[s, :, cs])
            act2[pl.ds(aoff, m), cs] = dot_nn(src[...], w3[s, :, cs])

        @pl.loop(0, m // 16)
        def _(r):
            o = pl.multiple_of(aoff + r * 16, 16)
            a = act1[pl.ds(o, 16), :]
            b = act2[pl.ds(o, 16), :]
            sg = jax.nn.sigmoid(a)
            ga = a * sg
            act1[pl.ds(o, 16), :] = b * (sg * (1.0 + a * (1.0 - sg)))
            act2[pl.ds(o, 16), :] = ga
            dst[pl.ds(pl.multiple_of(r * 16, 16), 16), :] = (ga * b).astype(BF16)

        for j in range(width // 256):
            cs = slice(j * 256, (j + 1) * 256)
            orow[0:m, cs] = dot_nn(dst[...], w2[s, :, cs]).astype(BF16)

    def backward(m, src, s, aoff):
        for j in range(hid // 256):
            cs = slice(j * 256, (j + 1) * 256)
            du = dot_nt(src[...], w2[s, cs, :])
            darow[s, 0:m, cs] = (du * act1[pl.ds(aoff, m), cs]).astype(BF16)
            dbrow[s, 0:m, cs] = (du * act2[pl.ds(aoff, m), cs]).astype(BF16)
        for j in range(width // 256):
            cs = slice(j * 256, (j + 1) * 256)
            orow[0:m, cs] = (dot_nt(darow[s, 0:m, :], w1[s, cs, :]) + dot_nt(dbrow[s, 0:m, :], w3[s, cs, :])).astype(BF16)

    def act_off(e):
        return pl.multiple_of(jnp.where(e == 0, 0, hot_rows + (e - 1) * n_rows), 64)

    def add_out(q, e, first):
        ypart[q] += column(q, e + 8) * dot_nn(put_rows(q, e), orow[first:first + cp, :])

    def hot_forward(p, q, s):
        on = column(q, 0) >= 0.0
        hrows[0:two, :] = jnp.where(on, x_all[q].astype(F32), 0.0).astype(BF16)
        xs = pltpu.make_async_copy(hrows.at[0:two], xh_hbm.at[pl.ds(p * two, two)], hst_sem.at[0])
        xs.start()
        o = pl.multiple_of(p * two, 64)
        forward(two, hrows.at[0:two], uhot.at[pl.ds(o, two)], s, o)
        ypart[q] += column(q, 8) * orow[0:two, :].astype(F32)
        xs.wait()

    def turn(i):
        for cpy in w_copies(i + 1):
            cpy.start()
        for cpy in w_copies(i):
            cpy.wait()

    ag(x_all, 0, 4).wait_recv()
    pick(0, c, x_all, False)

    @pl.loop(0, n_loc)
    def _(e):
        s = lax.rem(e, 2)
        hot = jnp.logical_and(is_owner, e == 0)
        turn(e)

        @pl.when(e == 3)
        def _():
            ag(x_all, 0, 0).wait_recv()
            ag(x_all, 0, 5).start()
            ag(x_all, 0, 2).wait_recv()
            ag(x_all, 0, 6).start()
            for i in (4, 0, 2, 1, 3):
                ag(dy_all, 1, i).start()

        @pl.when(jnp.logical_not(hot))
        def _():
            forward(cp, erows.at[e, 0:cp], urow.at[e, 0:cp], s, act_off(e))
            add_out(c, e, 0)

        @pl.when(hot)
        def _():
            hot_forward(0, c, s)

    def rs(t, j):
        part = (ypart, dxpart)[t]
        o = k * tok
        if j < 4:
            q = (c_o, c_r, c_l, c)[j]
            src, dst, dev = part.at[q, pl.ds((1 - k) * tok, tok)], cbuf.at[q], partner
        else:
            src, dst, dev = (
                (part.at[c_o, pl.ds(o, half)], yra, right),
                (part.at[c_o, pl.ds(o + half, half)], yrb, left),
                (part.at[c_r, pl.ds(o + half, half)], yfl.at[half:tok], right),
                (part.at[c_l, pl.ds(o, half)], yfr.at[0:half], left),
                (part.at[c_r, pl.ds(o, half)], yfl.at[0:half], right),
                (part.at[c_l, pl.ds(o + half, half)], yfr.at[half:tok], left))[j - 4]
        return pltpu.make_async_remote_copy(
            src_ref=src, dst_ref=dst, send_sem=rs_send.at[t, j], recv_sem=rs_recv.at[t, j],
            device_id={"ep": dev}, device_id_type=MESH)

    def add_rows(part, q, off, src, n):
        @pl.loop(0, n // 32)
        def _(r):
            o = pl.multiple_of(r * 32, 32)
            part[q, pl.ds(pl.multiple_of(off + r * 32, 32), 32)] += src[pl.ds(o, 32)]

    ag(x_all, 0, 1).wait_recv()
    ag(x_all, 0, 7).start()
    ag(x_all, 0, 3).wait_recv()
    ag(x_all, 0, 8).start()
    rs(0, 3).start()
    ag(x_all, 0, 7).wait_recv()
    pick(1, c_l, x_all, False)
    ag(x_all, 0, 8).wait_recv()
    pick(2, c_r, x_all, False)
    ag(x_all, 0, 5).wait_recv()
    ag(x_all, 0, 9).start()
    ag(x_all, 0, 6).wait_recv()
    ag(x_all, 0, 10).start()
    rs(0, 3).wait_recv()
    add_rows(ypart, c, k * tok, cbuf.at[c], tok)
    ag(x_all, 0, 9).wait_recv()
    ag(x_all, 0, 10).wait_recv()
    pick(3, c_o, x_all, False)

    def st_fwd(e):
        return (pltpu.make_async_copy(erows.at[e], xr_hbm.at[e], st_sem.at[0, e]),
                pltpu.make_async_copy(urow.at[e], ur_hbm.at[e], st_sem.at[1, e]))

    @pl.loop(0, n_loc)
    def _(e):
        s = lax.rem(e + n_loc, 2)
        hot = jnp.logical_and(is_owner, e == 0)
        turn(e + n_loc)

        @pl.when(e == 2)
        def _():
            ag(dy_all, 1, 0).wait_recv()
            ag(dy_all, 1, 5).start()
            ag(dy_all, 1, 2).wait_recv()
            ag(dy_all, 1, 6).start()

        @pl.when(jnp.logical_not(hot))
        def _():
            forward(n_rows - cp, erows.at[e, cp:n_rows], urow.at[e, cp:n_rows], s, pl.multiple_of(act_off(e) + cp, 16))
            for j, p in enumerate((3, 2, 1)):
                add_out(near[p], e, (p - 1) * cp)

                @pl.when(e == last)
                def _():
                    rs(0, j).start()

            for cpy in st_fwd(e):
                cpy.start()

        @pl.when(hot)
        def _():
            @pl.loop(1, chips)
            def _(p):
                q = jnp.where(p == 1, c_l, jnp.where(p == 2, c_r, c_o))
                hot_forward(p, q, s)

    for j, q in enumerate((c_o, c_r, c_l)):
        rs(0, j).wait_recv()
        add_rows(ypart, q, k * tok, cbuf.at[q], tok)
        if j == 0:
            rs(0, 4).start()
            rs(0, 5).start()
        else:
            rs(0, 5 + j).start()
    pl.semaphore_signal(free_sem, inc=1, device_id={"ep": partner}, device_id_type=MESH)

    ag(dy_all, 1, 4).wait_recv()
    ag(dy_all, 1, 1).wait_recv()
    ag(dy_all, 1, 7).start()
    ag(dy_all, 1, 3).wait_recv()
    ag(dy_all, 1, 8).start()
    ag(dy_all, 1, 5).wait_recv()
    ag(dy_all, 1, 9).start()
    ag(dy_all, 1, 6).wait_recv()
    ag(dy_all, 1, 10).start()
    for i in (7, 8, 9, 10):
        ag(dy_all, 1, i).wait_recv()

    @pl.loop(0, n_loc)
    def _(e):
        @pl.when(jnp.logical_not(jnp.logical_and(is_owner, e == 0)))
        def _():
            for cpy in st_fwd(e):
                cpy.wait()

    @pl.when(is_owner)
    def _():
        us = pltpu.make_async_copy(uhot, uh_hbm, hst_sem.at[0])
        us.start()
        us.wait()

    @pl.loop(0, chips)
    def _(p):
        q = jnp.where(p == 0, c, jnp.where(p == 1, c_l, jnp.where(p == 2, c_r, c_o)))
        pick(p, q, dy_all, True)

    def st_d(e):
        return pltpu.make_async_copy(erows.at[e], dr_hbm.at[e], st_sem.at[0, e])

    def st_ab(e, s):
        return (pltpu.make_async_copy(darow.at[s, 0:n_rows], da_hbm.at[e], st_sem.at[1, s]),
                pltpu.make_async_copy(dbrow.at[s, 0:n_rows], db_hbm.at[e], st_sem.at[1, 2 + s]))

    for e in range(n_loc):
        st_d(e).start()

    def rs_relay_y():
        rs(0, 4).wait_recv()
        add_rows(ypart, c_r, k * tok, yra, half)
        rs(0, 8).start()
        rs(0, 5).wait_recv()
        add_rows(ypart, c_l, k * tok + half, yrb, half)
        rs(0, 9).start()

    @pl.loop(0, n_loc)
    def _(e):
        s = lax.rem(e, 2)
        hot = jnp.logical_and(is_owner, e == 0)

        @pl.when(e < last)
        def _():
            for cpy in w_copies(e + 2 * n_loc + 1):
                cpy.start()

        for cpy in w_copies(e + 2 * n_loc):
            cpy.wait()

        @pl.when(e == last)
        def _():
            rs_relay_y()

        @pl.when(jnp.logical_not(hot))
        def _():
            backward(n_rows, erows.at[e], s, act_off(e))
            for p in range(chips):
                dxpart[near[p]] += dot_nn(put_rows(near[p], e), orow[p * cp:(p + 1) * cp, :])

        @pl.when(hot)
        def _():
            @pl.loop(0, chips // 2)
            def _(h):
                pair = (jnp.where(h == 0, c, c_r), jnp.where(h == 0, c_l, c_o))
                for i, q in enumerate(pair):
                    hrows[i * two:(i + 1) * two, :] = (column(q, 8) * dy_all[q].astype(F32)).astype(BF16)
                o = pl.multiple_of(h * 2 * two, 64)
                ds_ = pltpu.make_async_copy(hrows, dh_hbm.at[pl.ds(o, 2 * two)], hst_sem.at[0])
                ds_.start()
                backward(2 * two, hrows, s, o)
                sa = pltpu.make_async_copy(darow.at[s], dah_hbm.at[pl.ds(o, 2 * two)], hst_sem.at[1])
                sb = pltpu.make_async_copy(dbrow.at[s], dbh_hbm.at[pl.ds(o, 2 * two)], hst_sem.at[2])
                sa.start()
                sb.start()
                for i, q in enumerate(pair):
                    dxpart[q] += orow[i * two:(i + 1) * two, :].astype(F32)
                ds_.wait()
                sa.wait()
                sb.wait()

        @pl.when(jnp.logical_and(e >= 1, jnp.logical_not(jnp.logical_and(is_owner, e == 1))))
        def _():
            for cpy in st_ab(e - 1, 1 - s):
                cpy.wait()

        @pl.when(jnp.logical_not(hot))
        def _():
            for cpy in st_ab(e, s):
                cpy.start()

    def rs_end_y():
        for j in (6, 7, 8, 9):
            rs(0, j).wait_recv()

        @pl.loop(0, tok // 32)
        def _(r):
            o = pl.multiple_of(r * 32, 32)
            total = ypart[c, pl.ds(pl.multiple_of(k * tok + r * 32, 32), 32)] + yfl[pl.ds(o, 32)] + yfr[pl.ds(o, 32)]
            outb[pl.ds(o, 32)] = total.astype(BF16)

        return pltpu.make_async_copy(outb, y_hbm, io_sem.at[0])

    def chip_sums_out(j):
        q = (c_o, c_r, c_l, c)[j]
        if j == 3:
            return (pltpu.make_async_copy(dxpart.at[q, pl.ds(k * tok, tok)], sc_hbm, so_sem.at[6]),)
        lo, hi = ((soa_hbm, sob_hbm), (sra_hbm, srb_hbm), (sla_hbm, slb_hbm))[j]
        return (pltpu.make_async_copy(dxpart.at[q, pl.ds(k * tok, half)], lo, so_sem.at[2 * j]),
                pltpu.make_async_copy(dxpart.at[q, pl.ds(k * tok + half, half)], hi, so_sem.at[2 * j + 1]))

    pl.semaphore_wait(free_sem, 1)
    for j in range(4):
        rs(1, j).start()
    for j, q in enumerate((c_o, c_r, c_l, c)):
        rs(1, j).wait_recv()
        add_rows(dxpart, q, k * tok, cbuf.at[q], tok)
        for cpy in chip_sums_out(j):
            cpy.start()
    y_out = rs_end_y()
    y_out.start()

    for e in range(n_loc):
        st_d(e).wait()
    for cpy in st_ab(last, last % 2):
        cpy.wait()
    for d in range(1, group):
        for cpy in meta_copies(d):
            cpy.wait_send()
    for i in range(11):
        ag(x_all, 0, i).wait_send()
        ag(dy_all, 1, i).wait_send()
    for j in range(10):
        rs(0, j).wait_send()
    for j in range(4):
        rs(1, j).wait_send()
        for cpy in chip_sums_out(j):
            cpy.wait()
    y_out.wait()


def expert_grads(x_ref, d_ref, u_ref, da_ref, db_ref, g1, g3, g2):
    g1[0] = dot_tn(x_ref[0], da_ref[0]).astype(BF16)
    g3[0] = dot_tn(x_ref[0], db_ref[0]).astype(BF16)
    g2[0] = dot_tn(u_ref[0], d_ref[0]).astype(BF16)


def first_grads_kernel(owner, x_ref, d_ref, u_ref, da_ref, db_ref, xh, dh, uh, dah, dbh, g1, g3, g2, xb, dbuf, ub, dab, dbb, sem):
    i = pl.program_id(0)
    is_owner = lax.axis_index("ep") == owner
    hot = jnp.logical_and(is_owner, i == pl.num_programs(0) - 1)

    def copies():
        return [pltpu.make_async_copy(src, dst, sem.at[j]) for j, (src, dst) in enumerate(((xh, xb), (dah, dab), (dbh, dbb), (uh, ub), (dh, dbuf)))]

    @pl.when(jnp.logical_and(is_owner, i == 0))
    def _():
        for cpy in copies():
            cpy.start()

    @pl.when(jnp.logical_not(hot))
    def _():
        expert_grads(x_ref, d_ref, u_ref, da_ref, db_ref, g1, g3, g2)

    @pl.when(hot)
    def _():
        for cpy in copies():
            cpy.wait()
        g1[0] = dot_tn(xb[...], dab[...]).astype(BF16)
        g3[0] = dot_tn(xb[...], dbb[...]).astype(BF16)
        g2[0] = dot_tn(ub[...], dbuf[...]).astype(BF16)


def later_grads_kernel(x_ref, d_ref, u_ref, da_ref, db_ref, g1_in, g3_in, g2_in, g1, g3, g2):
    del g1_in, g3_in, g2_in
    expert_grads(x_ref, d_ref, u_ref, da_ref, db_ref, g1, g3, g2)


def solution(mesh):
    group = mesh.shape["ep"]
    num_dev = mesh.shape["dp"] * group
    tok_spec = P(("dp", "ep"), None)
    w_spec = P("ep", None, None)
    grad_spec = P(("dp", "ep"), None, None)

    def layer_fn(tokens, expert_ids, gate_vals, w_gate, w_up, w_down, grad_out):
        n_exp, width, hid = w_gate.shape
        tok = tokens.shape[0] // num_dev
        top_k = expert_ids.shape[1]
        cap = ((2 * tok * top_k + 8 * n_exp - 1) // (8 * n_exp)) * 8
        n_loc = n_exp // group
        hot = n_exp // 2
        owner = hot // n_loc
        chips = group // 2
        n_rows = chips * 2 * cap
        hot_rows = group * tok
        cfg = (chips, tok, width, hid, n_loc, cap, owner)

        def device_fn(x, ids, gates, w1, w3, w2, dy):
            any_spec = pl.BlockSpec(memory_space=pl.ANY)
            vmem_spec = pl.BlockSpec(memory_space=pltpu.VMEM)
            sds = jax.ShapeDtypeStruct
            hb = hot_rows // 2
            half = tok // 2
            act_rows = hot_rows + (n_loc - 1) * n_rows
            outs = pl.pallas_call(
                functools.partial(layer_kernel, cfg),
                out_shape=(
                    sds((tok, width), BF16), *[sds((half, width), F32)] * 6, sds((tok, width), F32),
                    sds((n_loc, n_rows, width), BF16), sds((n_loc, n_rows, width), BF16),
                    sds((n_loc, n_rows, hid), BF16), sds((n_loc, n_rows, hid), BF16), sds((n_loc, n_rows, hid), BF16),
                    sds((hot_rows, width), BF16), sds((hot_rows, width), BF16),
                    sds((hot_rows, hid), BF16), sds((hot_rows, hid), BF16), sds((hot_rows, hid), BF16)),
                in_specs=[any_spec, any_spec, vmem_spec, vmem_spec, any_spec, any_spec, any_spec],
                out_specs=[any_spec] * 18,
                scratch_shapes=[
                    pltpu.VMEM((chips, 2 * tok, width), BF16), pltpu.VMEM((chips, 2 * tok, width), BF16),
                    pltpu.VMEM((group, top_k, tok), jnp.int32), pltpu.VMEM((group, top_k, tok), F32),
                    pltpu.VMEM((chips, 8, 2 * tok), F32), pltpu.VMEM((chips, 8, 2 * tok), F32),
                    pltpu.VMEM((chips, 2 * tok, 128), F32),
                    pltpu.VMEM((chips, 2 * tok, width), F32), pltpu.VMEM((chips, 2 * tok, width), F32),
                    pltpu.VMEM((chips, tok, width), F32),
                    pltpu.VMEM((half, width), F32), pltpu.VMEM((half, width), F32),
                    pltpu.VMEM((tok, width), F32), pltpu.VMEM((tok, width), F32),
                    pltpu.VMEM((n_loc, n_rows, width), BF16), pltpu.VMEM((hb, width), BF16),
                    pltpu.VMEM((n_loc, n_rows, hid), BF16), pltpu.VMEM((hot_rows, hid), BF16),
                    pltpu.VMEM((2, hb, hid), BF16), pltpu.VMEM((2, hb, hid), BF16),
                    pltpu.VMEM((act_rows, hid), F32), pltpu.VMEM((act_rows, hid), F32),
                    pltpu.VMEM((hb, width), BF16), pltpu.VMEM((n_loc * 2 * cap, 2 * tok), BF16),
                    pltpu.VMEM((2, width, hid), BF16), pltpu.VMEM((2, width, hid), BF16), pltpu.VMEM((2, hid, width), BF16),
                    pltpu.VMEM((tok, width), BF16),
                    pltpu.SemaphoreType.DMA((2, group)), pltpu.SemaphoreType.DMA((2, group)),
                    pltpu.SemaphoreType.DMA((2, 11)), pltpu.SemaphoreType.DMA((2, 11)),
                    pltpu.SemaphoreType.DMA((2, 10)), pltpu.SemaphoreType.DMA((2, 10)),
                    pltpu.SemaphoreType.DMA((3, 2)), pltpu.SemaphoreType.DMA((2, n_loc)), pltpu.SemaphoreType.DMA((3,)),
                    pltpu.SemaphoreType.DMA((2,)), pltpu.SemaphoreType.DMA((7,)), pltpu.SemaphoreType.REGULAR,
                ],
                compiler_params=pltpu.CompilerParams(collective_id=0, has_side_effects=True, vmem_limit_bytes=67043328),
                name="moe_layer",
            )(x, dy, ids.T, gates.T, w1, w3, w2)
            y, soa, sob, sra, srb, sla, slb, sc, xr, dr, ur, dar, dbr, xh, dh, uh, dah, dbh = outs

            to_right = [(i, (i + 2) % group) for i in range(group)]
            to_left = [(i, (i + group - 2) % group) for i in range(group)]
            ra = lax.ppermute(soa, "ep", to_right)
            rb = lax.ppermute(sob, "ep", to_left)
            fl_hi = lax.ppermute(srb, "ep", to_right)
            fr_lo = lax.ppermute(sla, "ep", to_left)

            n_first = (n_loc + 1) // 2
            g_shapes = (sds((n_loc, width, hid), BF16), sds((n_loc, width, hid), BF16), sds((n_loc, hid, width), BF16))

            def blk(r, n, at):
                return pl.BlockSpec((1, r, n), lambda i: (at(i), 0, 0))

            def row_specs(at):
                return [blk(n_rows, width, at), blk(n_rows, width, at), blk(n_rows, hid, at), blk(n_rows, hid, at), blk(n_rows, hid, at)]

            def out_blks(at):
                return [blk(width, hid, at), blk(width, hid, at), blk(hid, width, at)]

            def cost(n):
                return pl.CostEstimate(flops=n * 6 * n_rows * width * hid, transcendentals=0,
                                       bytes_accessed=n * 2 * (2 * n_rows * width + 3 * n_rows * hid + 3 * width * hid))

            def first_at(i):
                return lax.rem(i + 1, n_first)

            def later_at(i):
                return i + n_first

            grads = pl.pallas_call(
                functools.partial(first_grads_kernel, owner),
                grid=(n_first,), out_shape=g_shapes,
                in_specs=row_specs(first_at) + [any_spec] * 5, out_specs=out_blks(first_at),
                scratch_shapes=[pltpu.VMEM((hot_rows, width), BF16), pltpu.VMEM((hot_rows, width), BF16), pltpu.VMEM((hot_rows, hid), BF16),
                                pltpu.VMEM((hot_rows, hid), BF16), pltpu.VMEM((hot_rows, hid), BF16), pltpu.SemaphoreType.DMA((5,))],
                compiler_params=pltpu.CompilerParams(vmem_limit_bytes=60 << 20),
                cost_estimate=cost(n_first), name="first_grads",
            )(xr, dr, ur, dar, dbr, xh, dh, uh, dah, dbh)

            fl_lo = lax.ppermute(sra + ra, "ep", to_right)
            fr_hi = lax.ppermute(slb + rb, "ep", to_left)
            g1, g3, g2 = pl.pallas_call(
                later_grads_kernel,
                grid=(n_loc - n_first,), out_shape=g_shapes,
                in_specs=row_specs(later_at) + [any_spec] * 3, out_specs=out_blks(later_at),
                input_output_aliases={5: 0, 6: 1, 7: 2},
                compiler_params=pltpu.CompilerParams(vmem_limit_bytes=60 << 20),
                cost_estimate=cost(n_loc - n_first), name="later_grads",
            )(xr, dr, ur, dar, dbr, *grads)
            fl = jnp.concatenate([fl_lo, fl_hi], axis=0)
            fr = jnp.concatenate([fr_lo, fr_hi], axis=0)
            dx = (sc + fl + fr).astype(BF16)
            return y, dx, g1, g3, g2

        return jax.shard_map(device_fn, mesh=mesh, in_specs=(tok_spec, tok_spec, tok_spec, w_spec, w_spec, w_spec, tok_spec),
                             out_specs=(tok_spec, tok_spec, grad_spec, grad_spec, grad_spec), check_vma=False)(
            tokens, expert_ids, gate_vals, w_gate, w_up, w_down, grad_out)

    return layer_fn
```

```python
import functools

import jax
import jax.numpy as jnp
from jax import lax
from jax.experimental import pallas as pl
from jax.experimental.pallas import tpu as pltpu
from jax.sharding import PartitionSpec as P

MESH = pl.DeviceIdType.MESH
F32 = jnp.float32
BF16 = jnp.bfloat16


def dot_nn(a, b):
    return lax.dot_general(a, b, (((1,), (0,)), ((), ())), preferred_element_type=F32)


def dot_nt(a, b):
    return lax.dot_general(a, b, (((1,), (1,)), ((), ())), preferred_element_type=F32)


def dot_tn(a, b):
    return lax.dot_general(a, b, (((0,), (0,)), ((), ())), preferred_element_type=F32)


def layer_kernel(cfg, x_hbm, dy_hbm, ids_ref, gates_ref, w1_hbm, w3_hbm, w2_hbm,
                 y_hbm, go_r, go_l, sr_hbm, sl_hbm, sc_hbm, xr_hbm, dr_hbm, ur_hbm, da_hbm, db_hbm, xh_hbm, dh_hbm, uh_hbm, dah_hbm, dbh_hbm,
                 x_all, dy_all, ids_all, gates_all, rt, gt, mc, ypart, dxpart, cbuf, yra, yrb, yfl, yfr,
                 erows, hrows, urow, uhot, darow, dbrow, act1, act2, orow, pbuf, w1, w3, w2, outb,
                 m_send, m_recv, ag_send, ag_recv, rs_send, rs_recv, w_sem, st_sem, hst_sem, io_sem, so_sem, free_sem):
    chips, tok, width, hid, n_loc, cap, owner = cfg
    group = 2 * chips
    two = 2 * tok
    cp = 2 * cap
    n_rows = chips * cp
    hot_rows = chips * two
    half = tok // 2
    last = n_loc - 1
    me = lax.axis_index("ep")
    c = me // 2
    k = lax.rem(me, 2)
    c_r = lax.rem(c + 1, chips)
    c_l = lax.rem(c + chips - 1, chips)
    c_o = lax.rem(c + 2, chips)
    near = (c, c_l, c_r, c_o)
    right = 2 * c_r + k
    left = 2 * c_l + k
    partner = 2 * c + 1 - k
    is_owner = me == owner

    own_x = pltpu.make_async_copy(x_hbm, x_all.at[c, pl.ds(k * tok, tok)], io_sem.at[0])
    own_dy = pltpu.make_async_copy(dy_hbm, dy_all.at[c, pl.ds(k * tok, tok)], io_sem.at[1])
    own_x.start()
    own_dy.start()

    def w_copies(i):
        e = lax.rem(i, n_loc)
        s = lax.rem(i, 2)
        return (pltpu.make_async_copy(w1_hbm.at[e], w1.at[s], w_sem.at[0, s]),
                pltpu.make_async_copy(w3_hbm.at[e], w3.at[s], w_sem.at[1, s]),
                pltpu.make_async_copy(w2_hbm.at[e], w2.at[s], w_sem.at[2, s]))

    for cpy in w_copies(0):
        cpy.start()
    ids_all[me] = ids_ref[...]
    gates_all[me] = gates_ref[...]

    barrier = pltpu.get_barrier_semaphore()
    for d in range(1, group):
        pl.semaphore_signal(barrier, inc=1, device_id={"ep": lax.rem(me + d, group)}, device_id_type=MESH)
    pl.semaphore_wait(barrier, group - 1)

    def meta_copies(d):
        return tuple(pltpu.make_async_remote_copy(
            src_ref=src, dst_ref=dst.at[me], send_sem=m_send.at[i, d], recv_sem=m_recv.at[i, d],
            device_id={"ep": lax.rem(me + d, group)}, device_id_type=MESH)
            for i, (src, dst) in enumerate(((ids_ref, ids_all), (gates_ref, gates_all))))

    def ag(ref, t, i):
        chip, core, r0, n, dev = (
            (c, k, 0, half, right), (c, k, half, half, right), (c, k, half, half, left), (c, k, 0, half, left),
            (c, k, 0, tok, partner),
            (c_l, k, 0, half, right), (c_r, k, half, half, left),
            (c_l, k, 0, tok, partner), (c_r, k, 0, tok, partner),
            (c_o, k, 0, half, partner), (c_o, k, half, half, partner))[i]
        blk = ref.at[chip, pl.ds(core * tok + r0, n)]
        return pltpu.make_async_remote_copy(
            src_ref=blk, dst_ref=blk, send_sem=ag_send.at[t, i], recv_sem=ag_recv.at[t, i],
            device_id={"ep": dev}, device_id_type=MESH)

    own_x.wait()
    for d in range(1, group):
        for cpy in meta_copies(d):
            cpy.start()
    for i in (4, 0, 2, 1, 3):
        ag(x_all, 0, i).start()
    own_dy.wait()

    @pl.loop(0, chips * two // 64)
    def _(r):
        q = r // (two // 64)
        o = pl.multiple_of(lax.rem(r, two // 64) * 64, 64)
        ypart[q, pl.ds(o, 64)] = jnp.zeros((64, width), F32)
        dxpart[q, pl.ds(o, 64)] = jnp.zeros((64, width), F32)

    for d in range(1, group):
        for cpy in meta_copies(d):
            cpy.wait_recv()

    upper = (lax.broadcasted_iota(jnp.int32, (tok, tok), 0) < lax.broadcasted_iota(jnp.int32, (tok, tok), 1)).astype(F32).astype(BF16)
    row_id = lax.broadcasted_iota(jnp.int32, (8, tok), 0)
    for s in range(group):
        q, core = s // 2, s % 2
        ids = ids_all[s]
        gates = gates_all[s]
        mask_m = jnp.zeros((8, tok), F32)
        gate_m = jnp.zeros((8, tok), F32)
        for le in range(n_loc):
            eq = ids == me * n_loc + le
            hit = jnp.sum(jnp.where(eq, 1.0, 0.0), axis=0, keepdims=True)
            gv = jnp.sum(jnp.where(eq, gates, 0.0), axis=0, keepdims=True)
            mask_m = jnp.where(row_id == le, hit, mask_m)
            gate_m = jnp.where(row_id == le, gv, gate_m)
        rank = dot_nn(mask_m.astype(BF16), upper)
        pos = jnp.where(mask_m > 0.0, rank + float(cap * core), -1.0)
        rt[q, :, core * tok:(core + 1) * tok] = pos
        gt[q, :, core * tok:(core + 1) * tok] = gate_m
        both = jnp.concatenate([pos, gate_m, jnp.zeros((tok - 16, tok), F32)], axis=0)
        mc[q, core * tok:(core + 1) * tok, :] = jnp.transpose(both)

    def pick(p, q, src, scaled):
        for e in range(n_loc):
            hit = rt[q, e:e + 1, :] == lax.broadcasted_iota(jnp.int32, (cp, two), 0).astype(F32)
            pbuf[e * cp:(e + 1) * cp, :] = jnp.where(hit, 1.0, 0.0).astype(BF16)
        gates = [None] * n_loc
        if scaled:
            for e in range(n_loc):
                hit = rt[q, e:e + 1, :] == lax.broadcasted_iota(jnp.int32, (cp, two), 0).astype(F32)
                gates[e] = jnp.sum(jnp.where(hit, gt[q, e:e + 1, :], 0.0), axis=1, keepdims=True)
        for j in range(width // 256):
            cs = slice(j * 256, (j + 1) * 256)
            got = dot_nn(pbuf[...], src[q, :, cs])
            for e in range(n_loc):
                part = got[e * cp:(e + 1) * cp]
                erows[e, pl.ds(p * cp, cp), cs] = (gates[e] * part if scaled else part).astype(BF16)

    def column(q, lane):
        return jnp.sum(jnp.where(lax.broadcasted_iota(jnp.int32, (two, 128), 1) == lane, mc[q], 0.0), axis=1, keepdims=True)

    def put_rows(q, e):
        hit = column(q, e) == lax.broadcasted_iota(jnp.int32, (two, cp), 1).astype(F32)
        return jnp.where(hit, 1.0, 0.0).astype(BF16)

    def forward(m, src, dst, s, aoff):
        for j in range(hid // 256):
            cs = slice(j * 256, (j + 1) * 256)
            a = dot_nn(src[...], w1[s, :, cs])
            b = dot_nn(src[...], w3[s, :, cs])
            sg = jax.nn.sigmoid(a)
            ga = a * sg
            act1[pl.ds(aoff, m), cs] = b * (sg * (1.0 + a * (1.0 - sg)))
            act2[pl.ds(aoff, m), cs] = ga
            dst[:, cs] = (ga * b).astype(BF16)

        for j in range(width // 256):
            cs = slice(j * 256, (j + 1) * 256)
            orow[0:m, cs] = dot_nn(dst[...], w2[s, :, cs]).astype(BF16)

    def backward(m, src, s, aoff, ooff):
        for j in range(hid // 256):
            cs = slice(j * 256, (j + 1) * 256)
            du = dot_nt(src[...], w2[s, cs, :])
            darow[s, 0:m, cs] = (du * act1[pl.ds(aoff, m), cs]).astype(BF16)
            dbrow[s, 0:m, cs] = (du * act2[pl.ds(aoff, m), cs]).astype(BF16)
        for j in range(width // 256):
            cs = slice(j * 256, (j + 1) * 256)
            orow[pl.ds(ooff, m), cs] = (dot_nt(darow[s, 0:m, :], w1[s, cs, :]) + dot_nt(dbrow[s, 0:m, :], w3[s, cs, :])).astype(BF16)

    def act_off(e):
        return pl.multiple_of(jnp.where(e == 0, 0, hot_rows + (e - 1) * n_rows), 64)

    def add_out(q, e, first):
        gate = column(q, e + 8)
        put = put_rows(q, e)
        for j in range(width // 256):
            cs = slice(j * 256, (j + 1) * 256)
            ypart[q, :, cs] += gate * dot_nn(put, orow[first:first + cp, cs])

    def add_dx_one(q, p, e):
        put = put_rows(q, e)
        for j in range(width // 256):
            cs = slice(j * 256, (j + 1) * 256)
            dxpart[q, :, cs] += dot_nn(put, orow[p * cp:(p + 1) * cp, cs])

    def add_dx_two(q, p, e):
        now, before = column(q, e), column(q, e - 1)
        now = jnp.where(now >= 0.0, now + float(cp), -1.0)
        lane = lax.broadcasted_iota(jnp.int32, (two, 2 * cp), 1).astype(F32)
        put = jnp.where(jnp.logical_or(before == lane, now == lane), 1.0, 0.0).astype(BF16)
        for j in range(width // 256):
            cs = slice(j * 256, (j + 1) * 256)
            both = jnp.concatenate([orow[2 * two + p * cp:2 * two + (p + 1) * cp, cs], orow[p * cp:(p + 1) * cp, cs]], axis=0)
            dxpart[q, :, cs] += dot_nn(put, both)

    def lane_of(q, r, n, lane):
        m = mc[q, pl.ds(r, n), :]
        return jnp.sum(jnp.where(lax.broadcasted_iota(jnp.int32, (n, 128), 1) == lane, m, 0.0), axis=1, keepdims=True)

    def hot_forward(p, q, s):
        @pl.loop(0, two // 32)
        def _(r):
            o = pl.multiple_of(r * 32, 32)
            on = lane_of(q, o, 32, 0) >= 0.0
            hrows[pl.ds(o, 32), :] = jnp.where(on, x_all[q, pl.ds(o, 32), :].astype(F32), 0.0).astype(BF16)

        xs = pltpu.make_async_copy(hrows.at[0:two], xh_hbm.at[pl.ds(p * two, two)], hst_sem.at[0])
        xs.start()
        o = pl.multiple_of(p * two, 64)
        forward(two, hrows.at[0:two], uhot.at[pl.ds(o, two)], s, o)

        @pl.loop(0, two // 32)
        def _(r):
            i = pl.multiple_of(r * 32, 32)
            ypart[q, pl.ds(i, 32), :] += lane_of(q, i, 32, 8) * orow[pl.ds(i, 32), :].astype(F32)

        xs.wait()

    def turn(i):
        for cpy in w_copies(i + 1):
            cpy.start()
        for cpy in w_copies(i):
            cpy.wait()

    ag(x_all, 0, 4).wait_recv()
    pick(0, c, x_all, False)

    @pl.loop(0, n_loc)
    def _(e):
        s = lax.rem(e, 2)
        hot = jnp.logical_and(is_owner, e == 0)
        turn(e)

        @pl.when(e == 3)
        def _():
            ag(x_all, 0, 0).wait_recv()
            ag(x_all, 0, 5).start()
            ag(x_all, 0, 2).wait_recv()
            ag(x_all, 0, 6).start()
            for i in (4, 0, 2, 1, 3):
                ag(dy_all, 1, i).start()

        @pl.when(jnp.logical_not(hot))
        def _():
            forward(cp, erows.at[e, 0:cp], urow.at[e, 0:cp], s, act_off(e))
            add_out(c, e, 0)

        @pl.when(hot)
        def _():
            hot_forward(0, c, s)

    def rs(t, j):
        part = (ypart, dxpart)[t]
        o = k * tok
        if j < 4:
            q = (c_o, c_r, c_l, c)[j]
            src, dst, dev = part.at[q, pl.ds((1 - k) * tok, tok)], cbuf.at[q], partner
        else:
            src, dst, dev = (
                (part.at[c_o, pl.ds(o, half)], yra, right),
                (part.at[c_o, pl.ds(o + half, half)], yrb, left),
                (part.at[c_r, pl.ds(o + half, half)], yfl.at[half:tok], right),
                (part.at[c_l, pl.ds(o, half)], yfr.at[0:half], left),
                (part.at[c_r, pl.ds(o, half)], yfl.at[0:half], right),
                (part.at[c_l, pl.ds(o + half, half)], yfr.at[half:tok], left))[j - 4]
        return pltpu.make_async_remote_copy(
            src_ref=src, dst_ref=dst, send_sem=rs_send.at[t, j], recv_sem=rs_recv.at[t, j],
            device_id={"ep": dev}, device_id_type=MESH)

    def add_rows(part, q, off, src, n):
        @pl.loop(0, n // 32)
        def _(r):
            o = pl.multiple_of(r * 32, 32)
            part[q, pl.ds(pl.multiple_of(off + r * 32, 32), 32)] += src[pl.ds(o, 32)]

    ag(x_all, 0, 1).wait_recv()
    ag(x_all, 0, 7).start()
    ag(x_all, 0, 3).wait_recv()
    ag(x_all, 0, 8).start()
    rs(0, 3).start()
    ag(x_all, 0, 7).wait_recv()
    pick(1, c_l, x_all, False)
    ag(x_all, 0, 8).wait_recv()
    pick(2, c_r, x_all, False)
    ag(x_all, 0, 5).wait_recv()
    ag(x_all, 0, 9).start()
    ag(x_all, 0, 6).wait_recv()
    ag(x_all, 0, 10).start()
    rs(0, 3).wait_recv()
    add_rows(ypart, c, k * tok, cbuf.at[c], tok)
    ag(x_all, 0, 9).wait_recv()
    ag(x_all, 0, 10).wait_recv()
    pick(3, c_o, x_all, False)

    def st_fwd(e):
        return (pltpu.make_async_copy(erows.at[e], xr_hbm.at[e], st_sem.at[0, e]),
                pltpu.make_async_copy(urow.at[e], ur_hbm.at[e], st_sem.at[1, e]))

    @pl.loop(0, n_loc)
    def _(e):
        s = lax.rem(e + n_loc, 2)
        hot = jnp.logical_and(is_owner, e == 0)
        turn(e + n_loc)

        @pl.when(e == 1)
        def _():
            ag(dy_all, 1, 0).wait_recv()
            ag(dy_all, 1, 5).start()
            ag(dy_all, 1, 2).wait_recv()
            ag(dy_all, 1, 6).start()

        @pl.when(e == 3)
        def _():
            ag(dy_all, 1, 4).wait_recv()
            ag(dy_all, 1, 1).wait_recv()
            ag(dy_all, 1, 7).start()
            ag(dy_all, 1, 3).wait_recv()
            ag(dy_all, 1, 8).start()

        @pl.when(jnp.logical_not(hot))
        def _():
            forward(n_rows - cp, erows.at[e, cp:n_rows], urow.at[e, cp:n_rows], s, pl.multiple_of(act_off(e) + cp, 16))
            for j, p in enumerate((3, 2, 1)):
                add_out(near[p], e, (p - 1) * cp)

                @pl.when(e == last)
                def _():
                    rs(0, j).start()

            for cpy in st_fwd(e):
                cpy.start()

        @pl.when(hot)
        def _():
            @pl.loop(1, chips)
            def _(p):
                q = jnp.where(p == 1, c_l, jnp.where(p == 2, c_r, c_o))
                hot_forward(p, q, s)

    @pl.loop(0, n_loc)
    def _(e):
        @pl.when(jnp.logical_not(jnp.logical_and(is_owner, e == 0)))
        def _():
            for cpy in st_fwd(e):
                cpy.wait()

    for j, q in enumerate((c_o, c_r, c_l)):
        rs(0, j).wait_recv()
        add_rows(ypart, q, k * tok, cbuf.at[q], tok)
        if j == 0:
            rs(0, 4).start()
            rs(0, 5).start()
            ag(dy_all, 1, 5).wait_recv()
            ag(dy_all, 1, 9).start()
            ag(dy_all, 1, 6).wait_recv()
            ag(dy_all, 1, 10).start()
        else:
            rs(0, 5 + j).start()
    pl.semaphore_signal(free_sem, inc=1, device_id={"ep": partner}, device_id_type=MESH)

    @pl.when(is_owner)
    def _():
        us = pltpu.make_async_copy(uhot, uh_hbm, hst_sem.at[0])
        us.start()
        us.wait()

    for i in (7, 8, 9, 10):
        ag(dy_all, 1, i).wait_recv()

    @pl.loop(0, chips)
    def _(p):
        q = jnp.where(p == 0, c, jnp.where(p == 1, c_l, jnp.where(p == 2, c_r, c_o)))
        pick(p, q, dy_all, True)

    def st_d(e):
        return pltpu.make_async_copy(erows.at[e], dr_hbm.at[e], st_sem.at[0, e])

    def st_ab(e, s):
        return (pltpu.make_async_copy(darow.at[s, 0:n_rows], da_hbm.at[e], st_sem.at[1, s]),
                pltpu.make_async_copy(dbrow.at[s, 0:n_rows], db_hbm.at[e], st_sem.at[1, 2 + s]))

    for e in range(n_loc):
        st_d(e).start()

    def rs_relay_y():
        rs(0, 4).wait_recv()
        add_rows(ypart, c_r, k * tok, yra, half)
        rs(0, 8).start()
        rs(0, 5).wait_recv()
        add_rows(ypart, c_l, k * tok + half, yrb, half)
        rs(0, 9).start()

    @pl.loop(0, n_loc)
    def _(e):
        s = lax.rem(e, 2)
        hot = jnp.logical_and(is_owner, e == 0)

        @pl.when(e < last)
        def _():
            for cpy in w_copies(e + 2 * n_loc + 1):
                cpy.start()

        for cpy in w_copies(e + 2 * n_loc):
            cpy.wait()

        @pl.when(e == last - 1)
        def _():
            rs_relay_y()

        @pl.when(jnp.logical_not(hot))
        def _():
            backward(n_rows, erows.at[e], s, act_off(e), pl.multiple_of(s * 2 * two, 64))

            @pl.when(e == 0)
            def _():
                for p in range(chips):
                    add_dx_one(near[p], p, e)

            @pl.when(e == last)
            def _():
                pl.semaphore_wait(free_sem, 1)

            @pl.when(jnp.logical_and(e > 0, s == 0))
            def _():
                for j, p in enumerate((3, 2, 1, 0)):
                    add_dx_two(near[p], p, e)

                    @pl.when(e == last)
                    def _():
                        rs(1, j).start()

        @pl.when(hot)
        def _():
            @pl.loop(0, chips // 2)
            def _(h):
                pair = (jnp.where(h == 0, c, c_r), jnp.where(h == 0, c_l, c_o))
                for i, q in enumerate(pair):
                    @pl.loop(0, two // 32)
                    def _(r):
                        at = pl.multiple_of(r * 32, 32)
                        got = dy_all[q, pl.ds(at, 32), :].astype(F32)
                        hrows[pl.ds(pl.multiple_of(i * two + r * 32, 32), 32), :] = (lane_of(q, at, 32, 8) * got).astype(BF16)

                o = pl.multiple_of(h * 2 * two, 64)
                ds_ = pltpu.make_async_copy(hrows, dh_hbm.at[pl.ds(o, 2 * two)], hst_sem.at[0])
                ds_.start()
                backward(2 * two, hrows, s, o, 0)
                sa = pltpu.make_async_copy(darow.at[s], dah_hbm.at[pl.ds(o, 2 * two)], hst_sem.at[1])
                sb = pltpu.make_async_copy(dbrow.at[s], dbh_hbm.at[pl.ds(o, 2 * two)], hst_sem.at[2])
                sa.start()
                sb.start()
                for i, q in enumerate(pair):
                    @pl.loop(0, two // 32)
                    def _(r):
                        at = pl.multiple_of(r * 32, 32)
                        dxpart[q, pl.ds(at, 32), :] += orow[pl.ds(pl.multiple_of(i * two + r * 32, 32), 32), :].astype(F32)

                ds_.wait()
                sa.wait()
                sb.wait()

        @pl.when(jnp.logical_and(e >= 1, jnp.logical_not(jnp.logical_and(is_owner, e == 1))))
        def _():
            for cpy in st_ab(e - 1, 1 - s):
                cpy.wait()

        @pl.when(jnp.logical_not(hot))
        def _():
            for cpy in st_ab(e, s):
                cpy.start()

    def rs_end_y():
        for j in (6, 7, 8, 9):
            rs(0, j).wait_recv()

        @pl.loop(0, tok // 32)
        def _(r):
            o = pl.multiple_of(r * 32, 32)
            total = ypart[c, pl.ds(pl.multiple_of(k * tok + r * 32, 32), 32)] + yfl[pl.ds(o, 32)] + yfr[pl.ds(o, 32)]
            outb[pl.ds(o, 32)] = total.astype(BF16)

        return pltpu.make_async_copy(outb, y_hbm, io_sem.at[0])

    def chip_sums_out(j):
        q = (c_o, c_r, c_l, c)[j]
        lo = dxpart.at[q, pl.ds(k * tok, half)]
        hi = dxpart.at[q, pl.ds(k * tok + half, half)]
        if j == 3:
            return (pltpu.make_async_copy(dxpart.at[q, pl.ds(k * tok, tok)], sc_hbm, so_sem.at[6]),)
        to_lo, to_hi = ((go_r.at[0:half], go_l.at[0:half]), (sr_hbm, go_r.at[half:tok]), (go_l.at[half:tok], sl_hbm))[j]
        return (pltpu.make_async_copy(lo, to_lo, so_sem.at[2 * j]), pltpu.make_async_copy(hi, to_hi, so_sem.at[2 * j + 1]))

    for j, q in enumerate((c_o, c_r, c_l, c)):
        rs(1, j).wait_recv()
        add_rows(dxpart, q, k * tok, cbuf.at[q], tok)
        for cpy in chip_sums_out(j):
            cpy.start()
    y_out = rs_end_y()
    y_out.start()

    for e in range(n_loc):
        st_d(e).wait()
    for cpy in st_ab(last, last % 2):
        cpy.wait()
    for d in range(1, group):
        for cpy in meta_copies(d):
            cpy.wait_send()
    for i in range(11):
        ag(x_all, 0, i).wait_send()
        ag(dy_all, 1, i).wait_send()
    for j in range(10):
        rs(0, j).wait_send()
    for j in range(4):
        rs(1, j).wait_send()
        for cpy in chip_sums_out(j):
            cpy.wait()
    y_out.wait()


def expert_grads(x_ref, d_ref, u_ref, da_ref, db_ref, g1, g3, g2):
    g1[0] = dot_tn(x_ref[0], da_ref[0]).astype(BF16)
    g3[0] = dot_tn(x_ref[0], db_ref[0]).astype(BF16)
    g2[0] = dot_tn(u_ref[0], d_ref[0]).astype(BF16)


def first_grads_kernel(owner, x_ref, d_ref, u_ref, da_ref, db_ref, xh, dh, uh, dah, dbh, y_ref, g1, g3, g2, y_out, xb, dbuf, ub, dab, dbb, sem):
    i = pl.program_id(0)
    y_out[...] = y_ref[...]
    is_owner = lax.axis_index("ep") == owner
    hot = jnp.logical_and(is_owner, i == pl.num_programs(0) - 1)

    def copies():
        return [pltpu.make_async_copy(src, dst, sem.at[j]) for j, (src, dst) in enumerate(((xh, xb), (dah, dab), (dbh, dbb), (uh, ub), (dh, dbuf)))]

    @pl.when(jnp.logical_and(is_owner, i == 0))
    def _():
        for cpy in copies():
            cpy.start()

    @pl.when(jnp.logical_not(hot))
    def _():
        expert_grads(x_ref, d_ref, u_ref, da_ref, db_ref, g1, g3, g2)

    @pl.when(hot)
    def _():
        for cpy in copies():
            cpy.wait()
        g1[0] = dot_tn(xb[...], dab[...]).astype(BF16)
        g3[0] = dot_tn(xb[...], dbb[...]).astype(BF16)
        g2[0] = dot_tn(ub[...], dbuf[...]).astype(BF16)


def later_grads_kernel(x_ref, d_ref, u_ref, da_ref, db_ref, g1_in, g3_in, g2_in, g1, g3, g2):
    del g1_in, g3_in, g2_in
    expert_grads(x_ref, d_ref, u_ref, da_ref, db_ref, g1, g3, g2)


def solution(mesh):
    group = mesh.shape["ep"]
    num_dev = mesh.shape["dp"] * group
    tok_spec = P(("dp", "ep"), None)
    w_spec = P("ep", None, None)
    grad_spec = P(("dp", "ep"), None, None)

    def layer_fn(tokens, expert_ids, gate_vals, w_gate, w_up, w_down, grad_out):
        n_exp, width, hid = w_gate.shape
        tok = tokens.shape[0] // num_dev
        top_k = expert_ids.shape[1]
        cap = ((2 * tok * top_k + 8 * n_exp - 1) // (8 * n_exp)) * 8
        n_loc = n_exp // group
        hot = n_exp // 2
        owner = hot // n_loc
        chips = group // 2
        n_rows = chips * 2 * cap
        hot_rows = group * tok
        cfg = (chips, tok, width, hid, n_loc, cap, owner)

        def device_fn(x, ids, gates, w1, w3, w2, dy):
            any_spec = pl.BlockSpec(memory_space=pl.ANY)
            vmem_spec = pl.BlockSpec(memory_space=pltpu.VMEM)
            sds = jax.ShapeDtypeStruct
            hb = hot_rows // 2
            half = tok // 2
            act_rows = hot_rows + (n_loc - 1) * n_rows
            outs = pl.pallas_call(
                functools.partial(layer_kernel, cfg),
                out_shape=(
                    sds((tok, width), BF16), *[sds((tok, width), F32)] * 2, *[sds((half, width), F32)] * 2, sds((tok, width), F32),
                    sds((n_loc, n_rows, width), BF16), sds((n_loc, n_rows, width), BF16),
                    sds((n_loc, n_rows, hid), BF16), sds((n_loc, n_rows, hid), BF16), sds((n_loc, n_rows, hid), BF16),
                    sds((hot_rows, width), BF16), sds((hot_rows, width), BF16),
                    sds((hot_rows, hid), BF16), sds((hot_rows, hid), BF16), sds((hot_rows, hid), BF16)),
                in_specs=[any_spec, any_spec, vmem_spec, vmem_spec, any_spec, any_spec, any_spec],
                out_specs=[any_spec] * 16,
                scratch_shapes=[
                    pltpu.VMEM((chips, 2 * tok, width), BF16), pltpu.VMEM((chips, 2 * tok, width), BF16),
                    pltpu.VMEM((group, top_k, tok), jnp.int32), pltpu.VMEM((group, top_k, tok), F32),
                    pltpu.VMEM((chips, 8, 2 * tok), F32), pltpu.VMEM((chips, 8, 2 * tok), F32),
                    pltpu.VMEM((chips, 2 * tok, 128), F32),
                    pltpu.VMEM((chips, 2 * tok, width), F32), pltpu.VMEM((chips, 2 * tok, width), F32),
                    pltpu.VMEM((chips, tok, width), F32),
                    pltpu.VMEM((half, width), F32), pltpu.VMEM((half, width), F32),
                    pltpu.VMEM((tok, width), F32), pltpu.VMEM((tok, width), F32),
                    pltpu.VMEM((n_loc, n_rows, width), BF16), pltpu.VMEM((hb, width), BF16),
                    pltpu.VMEM((n_loc, n_rows, hid), BF16), pltpu.VMEM((hot_rows, hid), BF16),
                    pltpu.VMEM((2, hb, hid), BF16), pltpu.VMEM((2, hb, hid), BF16),
                    pltpu.VMEM((act_rows, hid), F32), pltpu.VMEM((act_rows, hid), F32),
                    pltpu.VMEM((hb + n_rows, width), BF16), pltpu.VMEM((n_loc * 2 * cap, 2 * tok), BF16),
                    pltpu.VMEM((2, width, hid), BF16), pltpu.VMEM((2, width, hid), BF16), pltpu.VMEM((2, hid, width), BF16),
                    pltpu.VMEM((tok, width), BF16),
                    pltpu.SemaphoreType.DMA((2, group)), pltpu.SemaphoreType.DMA((2, group)),
                    pltpu.SemaphoreType.DMA((2, 11)), pltpu.SemaphoreType.DMA((2, 11)),
                    pltpu.SemaphoreType.DMA((2, 10)), pltpu.SemaphoreType.DMA((2, 10)),
                    pltpu.SemaphoreType.DMA((3, 2)), pltpu.SemaphoreType.DMA((2, n_loc)), pltpu.SemaphoreType.DMA((3,)),
                    pltpu.SemaphoreType.DMA((2,)), pltpu.SemaphoreType.DMA((7,)), pltpu.SemaphoreType.REGULAR,
                ],
                compiler_params=pltpu.CompilerParams(collective_id=0, has_side_effects=True, vmem_limit_bytes=67043328),
                name="moe_layer",
            )(x, dy, ids.T, gates.T, w1, w3, w2)
            y, go_r, go_l, sr, sl, sc, xr, dr, ur, dar, dbr, xh, dh, uh, dah, dbh = outs

            to_right = [(i, (i + 2) % group) for i in range(group)]
            to_left = [(i, (i + group - 2) % group) for i in range(group)]
            from_l = lax.ppermute(go_r, "ep", to_right)
            from_r = lax.ppermute(go_l, "ep", to_left)

            n_first = (n_loc + 1) // 2
            g_shapes = (sds((n_loc, width, hid), BF16), sds((n_loc, width, hid), BF16), sds((n_loc, hid, width), BF16))

            def blk(r, n, at):
                return pl.BlockSpec((1, r, n), lambda i: (at(i), 0, 0))

            def row_specs(at):
                return [blk(n_rows, width, at), blk(n_rows, width, at), blk(n_rows, hid, at), blk(n_rows, hid, at), blk(n_rows, hid, at)]

            def out_blks(at):
                return [blk(width, hid, at), blk(width, hid, at), blk(hid, width, at)]

            def cost(n):
                return pl.CostEstimate(flops=n * 6 * n_rows * width * hid, transcendentals=0,
                                       bytes_accessed=n * 2 * (2 * n_rows * width + 3 * n_rows * hid + 3 * width * hid))

            def first_at(i):
                return lax.rem(i + 1, n_first)

            def later_at(i):
                return i + n_first

            y_spec = pl.BlockSpec((tok, width), lambda i: (0, 0))
            *grads, y = pl.pallas_call(
                functools.partial(first_grads_kernel, owner),
                grid=(n_first,), out_shape=g_shapes + (sds((tok, width), BF16),),
                in_specs=row_specs(first_at) + [any_spec] * 5 + [y_spec], out_specs=out_blks(first_at) + [y_spec],
                scratch_shapes=[pltpu.VMEM((hot_rows, width), BF16), pltpu.VMEM((hot_rows, width), BF16), pltpu.VMEM((hot_rows, hid), BF16),
                                pltpu.VMEM((hot_rows, hid), BF16), pltpu.VMEM((hot_rows, hid), BF16), pltpu.SemaphoreType.DMA((5,))],
                compiler_params=pltpu.CompilerParams(vmem_limit_bytes=60 << 20),
                cost_estimate=cost(n_first), name="first_grads",
            )(xr, dr, ur, dar, dbr, xh, dh, uh, dah, dbh, y)

            fl_lo = lax.ppermute(sr + from_l[:half], "ep", to_right)
            fr_hi = lax.ppermute(sl + from_r[:half], "ep", to_left)
            g1, g3, g2 = pl.pallas_call(
                later_grads_kernel,
                grid=(n_loc - n_first,), out_shape=g_shapes,
                in_specs=row_specs(later_at) + [any_spec] * 3, out_specs=out_blks(later_at),
                input_output_aliases={5: 0, 6: 1, 7: 2},
                compiler_params=pltpu.CompilerParams(vmem_limit_bytes=60 << 20),
                cost_estimate=cost(n_loc - n_first), name="later_grads",
            )(xr, dr, ur, dar, dbr, *grads)
            fl = jnp.concatenate([fl_lo, from_l[half:]], axis=0)
            fr = jnp.concatenate([from_r[half:], fr_hi], axis=0)
            dx = (sc + fl + fr).astype(BF16)
            return y, dx, g1, g3, g2

        return jax.shard_map(device_fn, mesh=mesh, in_specs=(tok_spec, tok_spec, tok_spec, w_spec, w_spec, w_spec, tok_spec),
                             out_specs=(tok_spec, tok_spec, grad_spec, grad_spec, grad_spec), check_vma=False)(
            tokens, expert_ids, gate_vals, w_gate, w_up, w_down, grad_out)

    return layer_fn
```

```python
import functools

import jax
import jax.numpy as jnp
from jax import lax
from jax.experimental import pallas as pl
from jax.experimental.pallas import tpu as pltpu
from jax.sharding import PartitionSpec as P

MESH = pl.DeviceIdType.MESH
F32 = jnp.float32
BF16 = jnp.bfloat16


def dot_nn(a, b):
    return lax.dot_general(a, b, (((1,), (0,)), ((), ())), preferred_element_type=F32)


def dot_nt(a, b):
    return lax.dot_general(a, b, (((1,), (1,)), ((), ())), preferred_element_type=F32)


def dot_tn(a, b):
    return lax.dot_general(a, b, (((0,), (0,)), ((), ())), preferred_element_type=F32)


def layer_kernel(cfg, x_hbm, dy_hbm, ids_ref, gates_ref, w1_hbm, w3_hbm, w2_hbm,
                 y_hbm, go_r, go_l, sr_hbm, sl_hbm, sc_hbm, xr_hbm, dr_hbm, ur_hbm, da_hbm, db_hbm, xh_hbm, dh_hbm, uh_hbm, dah_hbm, dbh_hbm,
                 x_all, dy_all, ids_all, gates_all, rt, gt, mc, ypart, dxpart, cbuf, yra, yrb, yfl, yfr,
                 erows, hrows, urow, uhot, darow, dbrow, act1, act2, orow, pbuf, w1, w3, w2, outb,
                 m_send, m_recv, ag_send, ag_recv, rs_send, rs_recv, w_sem, st_sem, hst_sem, io_sem, so_sem, free_sem):
    chips, tok, width, hid, n_loc, cap, owner = cfg
    group = 2 * chips
    two = 2 * tok
    cp = 2 * cap
    n_rows = chips * cp
    hot_rows = chips * two
    half = tok // 2
    last = n_loc - 1
    me = lax.axis_index("ep")
    c = me // 2
    k = lax.rem(me, 2)
    c_r = lax.rem(c + 1, chips)
    c_l = lax.rem(c + chips - 1, chips)
    c_o = lax.rem(c + 2, chips)
    near = (c, c_l, c_r, c_o)
    right = 2 * c_r + k
    left = 2 * c_l + k
    partner = 2 * c + 1 - k
    is_owner = me == owner

    own_x = pltpu.make_async_copy(x_hbm, x_all.at[c, pl.ds(k * tok, tok)], io_sem.at[0])
    own_dy = pltpu.make_async_copy(dy_hbm, dy_all.at[c, pl.ds(k * tok, tok)], io_sem.at[1])
    own_x.start()
    own_dy.start()

    def w_copies(e):
        s = lax.rem(e, 2)
        return (pltpu.make_async_copy(w1_hbm.at[e], w1.at[s], w_sem.at[0, s]),
                pltpu.make_async_copy(w3_hbm.at[e], w3.at[s], w_sem.at[1, s]),
                pltpu.make_async_copy(w2_hbm.at[e], w2.at[s], w_sem.at[2, s]))

    for e in (last, last - 1):
        for cpy in w_copies(e):
            cpy.start()
    ids_all[me] = ids_ref[...]
    gates_all[me] = gates_ref[...]

    barrier = pltpu.get_barrier_semaphore()
    for d in range(1, group):
        pl.semaphore_signal(barrier, inc=1, device_id={"ep": lax.rem(me + d, group)}, device_id_type=MESH)
    pl.semaphore_wait(barrier, group - 1)

    def meta_copies(d):
        return tuple(pltpu.make_async_remote_copy(
            src_ref=src, dst_ref=dst.at[me], send_sem=m_send.at[i, d], recv_sem=m_recv.at[i, d],
            device_id={"ep": lax.rem(me + d, group)}, device_id_type=MESH)
            for i, (src, dst) in enumerate(((ids_ref, ids_all), (gates_ref, gates_all))))

    def ag(ref, t, i):
        chip, core, r0, n, dev = (
            (c, k, 0, half, right), (c, k, half, half, right), (c, k, half, half, left), (c, k, 0, half, left),
            (c, k, 0, tok, partner),
            (c_l, k, 0, half, right), (c_r, k, half, half, left),
            (c_l, k, 0, tok, partner), (c_r, k, 0, tok, partner),
            (c_o, k, 0, half, partner), (c_o, k, half, half, partner))[i]
        blk = ref.at[chip, pl.ds(core * tok + r0, n)]
        return pltpu.make_async_remote_copy(
            src_ref=blk, dst_ref=blk, send_sem=ag_send.at[t, i], recv_sem=ag_recv.at[t, i],
            device_id={"ep": dev}, device_id_type=MESH)

    own_x.wait()
    for d in range(1, group):
        for cpy in meta_copies(d):
            cpy.start()
    for i in (4, 0, 2, 1, 3):
        ag(x_all, 0, i).start()
    own_dy.wait()

    @pl.loop(0, chips * two // 64)
    def _(r):
        q = r // (two // 64)
        o = pl.multiple_of(lax.rem(r, two // 64) * 64, 64)
        ypart[q, pl.ds(o, 64)] = jnp.zeros((64, width), F32)
        dxpart[q, pl.ds(o, 64)] = jnp.zeros((64, width), F32)

    for d in range(1, group):
        for cpy in meta_copies(d):
            cpy.wait_recv()

    upper = (lax.broadcasted_iota(jnp.int32, (tok, tok), 0) < lax.broadcasted_iota(jnp.int32, (tok, tok), 1)).astype(F32).astype(BF16)
    row_id = lax.broadcasted_iota(jnp.int32, (8, tok), 0)
    for s in range(group):
        q, core = s // 2, s % 2
        ids = ids_all[s]
        gates = gates_all[s]
        mask_m = jnp.zeros((8, tok), F32)
        gate_m = jnp.zeros((8, tok), F32)
        for le in range(n_loc):
            eq = ids == me * n_loc + le
            hit = jnp.sum(jnp.where(eq, 1.0, 0.0), axis=0, keepdims=True)
            gv = jnp.sum(jnp.where(eq, gates, 0.0), axis=0, keepdims=True)
            mask_m = jnp.where(row_id == le, hit, mask_m)
            gate_m = jnp.where(row_id == le, gv, gate_m)
        rank = dot_nn(mask_m.astype(BF16), upper)
        pos = jnp.where(mask_m > 0.0, rank + float(cap * core), -1.0)
        rt[q, :, core * tok:(core + 1) * tok] = pos
        gt[q, :, core * tok:(core + 1) * tok] = gate_m
        both = jnp.concatenate([pos, gate_m, jnp.zeros((tok - 16, tok), F32)], axis=0)
        mc[q, core * tok:(core + 1) * tok, :] = jnp.transpose(both)

    def pick(p, q, src, scaled):
        for e in range(n_loc):
            hit = rt[q, e:e + 1, :] == lax.broadcasted_iota(jnp.int32, (cp, two), 0).astype(F32)
            pbuf[e * cp:(e + 1) * cp, :] = jnp.where(hit, 1.0, 0.0).astype(BF16)
        gates = [None] * n_loc
        if scaled:
            for e in range(n_loc):
                hit = rt[q, e:e + 1, :] == lax.broadcasted_iota(jnp.int32, (cp, two), 0).astype(F32)
                gates[e] = jnp.sum(jnp.where(hit, gt[q, e:e + 1, :], 0.0), axis=1, keepdims=True)
        for j in range(width // 256):
            cs = slice(j * 256, (j + 1) * 256)
            got = dot_nn(pbuf[...], src[q, :, cs])
            for e in range(n_loc):
                part = got[e * cp:(e + 1) * cp]
                erows[e, pl.ds(p * cp, cp), cs] = (gates[e] * part if scaled else part).astype(BF16)

    def column(q, lane):
        return jnp.sum(jnp.where(lax.broadcasted_iota(jnp.int32, (two, 128), 1) == lane, mc[q], 0.0), axis=1, keepdims=True)

    def put_rows(q, e):
        hit = column(q, e) == lax.broadcasted_iota(jnp.int32, (two, cp), 1).astype(F32)
        return jnp.where(hit, 1.0, 0.0).astype(BF16)

    def forward(m, src, dst, s, aoff, on, emit):
        for j in range(hid // 256):
            cs = slice(j * 256, (j + 1) * 256)
            a = dot_nn(src[...], w1[s, :, cs])
            b = dot_nn(src[...], w3[s, :, cs])
            sg = jax.nn.sigmoid(a)
            ga = a * sg
            fa = b * (sg * (1.0 + a * (1.0 - sg)))
            u = ga * b
            if on is not None:
                fa, ga, u = jnp.where(on, fa, 0.0), jnp.where(on, ga, 0.0), jnp.where(on, u, 0.0)
            act1[pl.ds(aoff, m), cs] = fa
            act2[pl.ds(aoff, m), cs] = ga
            dst[:, cs] = u.astype(BF16)

        for j in range(width // 256):
            cs = slice(j * 256, (j + 1) * 256)
            emit(cs, dot_nn(dst[...], w2[s, :, cs]).astype(BF16))

    def backward(m, src, s, aoff, emit):
        for j in range(hid // 256):
            cs = slice(j * 256, (j + 1) * 256)
            du = dot_nt(src[...], w2[s, cs, :])
            darow[s, 0:m, cs] = (du * act1[pl.ds(aoff, m), cs]).astype(BF16)
            dbrow[s, 0:m, cs] = (du * act2[pl.ds(aoff, m), cs]).astype(BF16)
        for j in range(width // 256):
            cs = slice(j * 256, (j + 1) * 256)
            emit(cs, (dot_nt(darow[s, 0:m, :], w1[s, cs, :]) + dot_nt(dbrow[s, 0:m, :], w3[s, cs, :])).astype(BF16))

    def act_off(e):
        return pl.multiple_of(jnp.where(e == 0, 0, hot_rows + (e - 1) * n_rows), 64)

    def add_out(q, e, first):
        gate = column(q, e + 8)
        put = put_rows(q, e)
        for j in range(width // 256):
            cs = slice(j * 256, (j + 1) * 256)
            ypart[q, :, cs] += gate * dot_nn(put, orow[first:first + cp, cs])

    def add_dx_one(q, p, e):
        put = put_rows(q, e)
        for j in range(width // 256):
            cs = slice(j * 256, (j + 1) * 256)
            dxpart[q, :, cs] += dot_nn(put, orow[p * cp:(p + 1) * cp, cs])

    def add_dx_two(q, p, e):
        now, before = column(q, e), column(q, e - 1)
        now = jnp.where(now >= 0.0, now + float(cp), -1.0)
        lane = lax.broadcasted_iota(jnp.int32, (two, 2 * cp), 1).astype(F32)
        put = jnp.where(jnp.logical_or(before == lane, now == lane), 1.0, 0.0).astype(BF16)
        for j in range(width // 256):
            cs = slice(j * 256, (j + 1) * 256)
            both = jnp.concatenate([orow[2 * two + p * cp:2 * two + (p + 1) * cp, cs], orow[p * cp:(p + 1) * cp, cs]], axis=0)
            dxpart[q, :, cs] += dot_nn(put, both)

    def lane_of(q, r, n, lane):
        m = mc[q, pl.ds(r, n), :]
        return jnp.sum(jnp.where(lax.broadcasted_iota(jnp.int32, (n, 128), 1) == lane, m, 0.0), axis=1, keepdims=True)

    def hot_forward(p, q, s):
        o = pl.multiple_of(p * two, 64)
        gate = column(q, 8)

        def emit(cs, out):
            ypart[q, :, cs] += gate * out.astype(F32)

        forward(two, x_all.at[q], uhot.at[pl.ds(o, two)], s, o, column(q, 0) >= 0.0, emit)

    def cold_forward(e, s, r0, r1):
        def emit(cs, out):
            orow[0:r1 - r0, cs] = out

        forward(r1 - r0, erows.at[e, r0:r1], urow.at[e, r0:r1], s, pl.multiple_of(act_off(e) + r0, 16), None, emit)

    def turn(i, e, step, first):
        @pl.when(jnp.logical_and(i >= 1, i < last))
        def _():
            for cpy in w_copies(e + step):
                cpy.start()

        @pl.when(i >= (0 if first else 2))
        def _():
            for cpy in w_copies(e):
                cpy.wait()

    def rs(t, j):
        part = (ypart, dxpart)[t]
        o = k * tok
        if j < 4:
            q = (c_o, c_r, c_l, c)[j]
            src, dst, dev = part.at[q, pl.ds((1 - k) * tok, tok)], cbuf.at[q], partner
        else:
            src, dst, dev = (
                (part.at[c_o, pl.ds(o, half)], yra, right),
                (part.at[c_o, pl.ds(o + half, half)], yrb, left),
                (part.at[c_r, pl.ds(o + half, half)], yfl.at[half:tok], right),
                (part.at[c_l, pl.ds(o, half)], yfr.at[0:half], left),
                (part.at[c_r, pl.ds(o, half)], yfl.at[0:half], right),
                (part.at[c_l, pl.ds(o + half, half)], yfr.at[half:tok], left))[j - 4]
        return pltpu.make_async_remote_copy(
            src_ref=src, dst_ref=dst, send_sem=rs_send.at[t, j], recv_sem=rs_recv.at[t, j],
            device_id={"ep": dev}, device_id_type=MESH)

    def add_rows(part, q, off, src, n):
        @pl.loop(0, n // 32)
        def _(r):
            o = pl.multiple_of(r * 32, 32)
            part[q, pl.ds(pl.multiple_of(off + r * 32, 32), 32)] += src[pl.ds(o, 32)]

    ag(x_all, 0, 4).wait_recv()
    pick(0, c, x_all, False)

    @pl.loop(0, n_loc)
    def _(i):
        e = last - i
        s = lax.rem(e, 2)
        hot = jnp.logical_and(is_owner, e == 0)
        turn(i, e, -1, True)

        @pl.when(i == 3)
        def _():
            ag(x_all, 0, 0).wait_recv()
            ag(x_all, 0, 5).start()
            ag(x_all, 0, 2).wait_recv()
            ag(x_all, 0, 6).start()
            for n in (4, 0, 2, 1, 3):
                ag(dy_all, 1, n).start()

        @pl.when(jnp.logical_not(hot))
        def _():
            cold_forward(e, s, 0, cp)
            add_out(c, e, 0)

        @pl.when(hot)
        def _():
            hot_forward(0, c, s)

    ag(x_all, 0, 1).wait_recv()
    ag(x_all, 0, 7).start()
    ag(x_all, 0, 3).wait_recv()
    ag(x_all, 0, 8).start()
    rs(0, 3).start()
    ag(x_all, 0, 7).wait_recv()
    pick(1, c_l, x_all, False)
    ag(x_all, 0, 8).wait_recv()
    pick(2, c_r, x_all, False)

    @pl.loop(0, n_loc)
    def _(e):
        s = lax.rem(e, 2)
        hot = jnp.logical_and(is_owner, e == 0)
        turn(e, e, 1, False)

        @pl.when(e == 2)
        def _():
            ag(x_all, 0, 5).wait_recv()
            ag(x_all, 0, 9).start()
            ag(x_all, 0, 6).wait_recv()
            ag(x_all, 0, 10).start()

        @pl.when(e == last)
        def _():
            ag(dy_all, 1, 0).wait_recv()
            ag(dy_all, 1, 5).start()
            ag(dy_all, 1, 2).wait_recv()
            ag(dy_all, 1, 6).start()

        @pl.when(jnp.logical_not(hot))
        def _():
            cold_forward(e, s, cp, 3 * cp)
            for j, p in ((1, 2), (2, 1)):
                add_out(near[p], e, (p - 1) * cp)

                @pl.when(e == last)
                def _():
                    rs(0, j).start()

        @pl.when(hot)
        def _():
            @pl.loop(1, 3)
            def _(p):
                hot_forward(p, jnp.where(p == 1, c_l, c_r), s)

    rs(0, 3).wait_recv()
    add_rows(ypart, c, k * tok, cbuf.at[c], tok)
    ag(x_all, 0, 9).wait_recv()
    ag(x_all, 0, 10).wait_recv()
    pick(3, c_o, x_all, False)

    def st_fwd(e):
        return (pltpu.make_async_copy(erows.at[e], xr_hbm.at[e], st_sem.at[0, e]),
                pltpu.make_async_copy(urow.at[e], ur_hbm.at[e], st_sem.at[1, e]))

    def st_hot():
        return [pltpu.make_async_copy(uhot, uh_hbm, hst_sem.at[0])] + [
            pltpu.make_async_copy(x_all.at[q], xh_hbm.at[p * two:(p + 1) * two], hst_sem.at[1 + p]) for p, q in enumerate(near)]

    @pl.loop(0, n_loc)
    def _(i):
        e = last - i
        s = lax.rem(e, 2)
        hot = jnp.logical_and(is_owner, e == 0)
        turn(i, e, -1, False)

        @pl.when(i == 1)
        def _():
            for j, q in ((1, c_r), (2, c_l)):
                rs(0, j).wait_recv()
                add_rows(ypart, q, k * tok, cbuf.at[q], tok)
                rs(0, 5 + j).start()

        @pl.when(i == 3)
        def _():
            ag(dy_all, 1, 4).wait_recv()
            ag(dy_all, 1, 1).wait_recv()
            ag(dy_all, 1, 7).start()
            ag(dy_all, 1, 3).wait_recv()
            ag(dy_all, 1, 8).start()

        @pl.when(jnp.logical_not(hot))
        def _():
            cold_forward(e, s, 3 * cp, n_rows)
            add_out(c_o, e, 0)
            for cpy in st_fwd(e):
                cpy.start()

        @pl.when(hot)
        def _():
            hot_forward(3, c_o, s)
            for cpy in st_hot():
                cpy.start()

    rs(0, 0).start()

    @pl.loop(0, n_loc)
    def _(e):
        @pl.when(jnp.logical_not(jnp.logical_and(is_owner, e == 0)))
        def _():
            for cpy in st_fwd(e):
                cpy.wait()

    pick(0, c, dy_all, True)
    rs(0, 0).wait_recv()
    add_rows(ypart, c_o, k * tok, cbuf.at[c_o], tok)
    rs(0, 4).start()
    rs(0, 5).start()
    pl.semaphore_signal(free_sem, inc=1, device_id={"ep": partner}, device_id_type=MESH)
    ag(dy_all, 1, 7).wait_recv()
    pick(1, c_l, dy_all, True)
    ag(dy_all, 1, 5).wait_recv()
    ag(dy_all, 1, 9).start()
    ag(dy_all, 1, 6).wait_recv()
    ag(dy_all, 1, 10).start()
    ag(dy_all, 1, 8).wait_recv()
    pick(2, c_r, dy_all, True)
    ag(dy_all, 1, 9).wait_recv()
    ag(dy_all, 1, 10).wait_recv()
    pick(3, c_o, dy_all, True)

    @pl.when(is_owner)
    def _():
        for cpy in st_hot():
            cpy.wait()

    def st_d(e):
        return pltpu.make_async_copy(erows.at[e], dr_hbm.at[e], st_sem.at[0, e])

    def st_ab(e, s):
        return (pltpu.make_async_copy(darow.at[s, 0:n_rows], da_hbm.at[e], st_sem.at[1, s]),
                pltpu.make_async_copy(dbrow.at[s, 0:n_rows], db_hbm.at[e], st_sem.at[1, 2 + s]))

    for e in range(n_loc):
        st_d(e).start()

    def rs_relay_y():
        rs(0, 4).wait_recv()
        add_rows(ypart, c_r, k * tok, yra, half)
        rs(0, 8).start()
        rs(0, 5).wait_recv()
        add_rows(ypart, c_l, k * tok + half, yrb, half)
        rs(0, 9).start()

    @pl.loop(0, n_loc)
    def _(e):
        s = lax.rem(e, 2)
        hot = jnp.logical_and(is_owner, e == 0)

        turn(e, e, 1, False)

        @pl.when(jnp.logical_not(hot))
        def _():
            ooff = pl.multiple_of(s * 2 * two, 64)

            def emit(cs, out):
                orow[pl.ds(ooff, n_rows), cs] = out

            backward(n_rows, erows.at[e], s, act_off(e), emit)

            @pl.when(e == last - 1)
            def _():
                rs_relay_y()

            @pl.when(e == 0)
            def _():
                for p in range(chips):
                    add_dx_one(near[p], p, e)

            @pl.when(e == last)
            def _():
                pl.semaphore_wait(free_sem, 1)

            @pl.when(jnp.logical_and(e > 0, s == 0))
            def _():
                for j, p in enumerate((3, 2, 1, 0)):
                    add_dx_two(near[p], p, e)

                    @pl.when(e == last)
                    def _():
                        rs(1, j).start()

        @pl.when(hot)
        def _():
            @pl.loop(0, chips // 2)
            def _(h):
                pair = (jnp.where(h == 0, c, c_r), jnp.where(h == 0, c_l, c_o))
                for n, q in enumerate(pair):
                    @pl.loop(0, two // 64)
                    def _(r):
                        at = pl.multiple_of(r * 64, 64)
                        got = dy_all[q, pl.ds(at, 64), :].astype(F32)
                        hrows[pl.ds(pl.multiple_of(n * two + r * 64, 64), 64), :] = (lane_of(q, at, 64, 8) * got).astype(BF16)

                o = pl.multiple_of(h * 2 * two, 64)
                sd = pltpu.make_async_copy(hrows, dh_hbm.at[pl.ds(o, 2 * two)], hst_sem.at[0])
                sd.start()

                def emit(cs, out):
                    for n, q in enumerate(pair):
                        dxpart[q, :, cs] += out[n * two:(n + 1) * two].astype(F32)

                backward(2 * two, hrows, s, o, emit)
                sa = pltpu.make_async_copy(darow.at[s], dah_hbm.at[pl.ds(o, 2 * two)], hst_sem.at[1])
                sb = pltpu.make_async_copy(dbrow.at[s], dbh_hbm.at[pl.ds(o, 2 * two)], hst_sem.at[2])
                sa.start()
                sb.start()
                sd.wait()
                sa.wait()
                sb.wait()

        @pl.when(jnp.logical_and(e >= 1, jnp.logical_not(jnp.logical_and(is_owner, e == 1))))
        def _():
            for cpy in st_ab(e - 1, 1 - s):
                cpy.wait()

        @pl.when(jnp.logical_not(hot))
        def _():
            for cpy in st_ab(e, s):
                cpy.start()

    def rs_end_y():
        for j in (6, 7, 8, 9):
            rs(0, j).wait_recv()

        @pl.loop(0, tok // 32)
        def _(r):
            o = pl.multiple_of(r * 32, 32)
            total = ypart[c, pl.ds(pl.multiple_of(k * tok + r * 32, 32), 32)] + yfl[pl.ds(o, 32)] + yfr[pl.ds(o, 32)]
            outb[pl.ds(o, 32)] = total.astype(BF16)

        return pltpu.make_async_copy(outb, y_hbm, io_sem.at[0])

    def chip_sums_out(j):
        q = (c_o, c_r, c_l, c)[j]
        lo = dxpart.at[q, pl.ds(k * tok, half)]
        hi = dxpart.at[q, pl.ds(k * tok + half, half)]
        if j == 3:
            return (pltpu.make_async_copy(dxpart.at[q, pl.ds(k * tok, tok)], sc_hbm, so_sem.at[6]),)
        to_lo, to_hi = ((go_r.at[0:half], go_l.at[0:half]), (sr_hbm, go_r.at[half:tok]), (go_l.at[half:tok], sl_hbm))[j]
        return (pltpu.make_async_copy(lo, to_lo, so_sem.at[2 * j]), pltpu.make_async_copy(hi, to_hi, so_sem.at[2 * j + 1]))

    for j, q in enumerate((c_o, c_r, c_l, c)):
        rs(1, j).wait_recv()
        add_rows(dxpart, q, k * tok, cbuf.at[q], tok)
        for cpy in chip_sums_out(j):
            cpy.start()
    y_out = rs_end_y()
    y_out.start()

    for e in range(n_loc):
        st_d(e).wait()
    for cpy in st_ab(last, last % 2):
        cpy.wait()
    for d in range(1, group):
        for cpy in meta_copies(d):
            cpy.wait_send()
    for i in range(11):
        ag(x_all, 0, i).wait_send()
        ag(dy_all, 1, i).wait_send()
    for j in range(10):
        rs(0, j).wait_send()
    for j in range(4):
        rs(1, j).wait_send()
        for cpy in chip_sums_out(j):
            cpy.wait()
    y_out.wait()


def expert_grads(x_ref, d_ref, u_ref, da_ref, db_ref, g1, g3, g2):
    g1[0] = dot_tn(x_ref[0], da_ref[0]).astype(BF16)
    g3[0] = dot_tn(x_ref[0], db_ref[0]).astype(BF16)
    g2[0] = dot_tn(u_ref[0], d_ref[0]).astype(BF16)


def first_grads_kernel(owner, x_ref, d_ref, u_ref, da_ref, db_ref, xh, dh, uh, dah, dbh, y_ref, g1, g3, g2, y_out, xb, dbuf, ub, dab, dbb, sem):
    i = pl.program_id(0)
    y_out[...] = y_ref[...]
    is_owner = lax.axis_index("ep") == owner
    hot = jnp.logical_and(is_owner, i == pl.num_programs(0) - 1)

    def copies():
        return [pltpu.make_async_copy(src, dst, sem.at[j]) for j, (src, dst) in enumerate(((xh, xb), (dah, dab), (dbh, dbb), (uh, ub), (dh, dbuf)))]

    @pl.when(jnp.logical_and(is_owner, i == 0))
    def _():
        for cpy in copies():
            cpy.start()

    @pl.when(jnp.logical_not(hot))
    def _():
        expert_grads(x_ref, d_ref, u_ref, da_ref, db_ref, g1, g3, g2)

    @pl.when(hot)
    def _():
        for cpy in copies():
            cpy.wait()
        g1[0] = dot_tn(xb[...], dab[...]).astype(BF16)
        g3[0] = dot_tn(xb[...], dbb[...]).astype(BF16)
        g2[0] = dot_tn(ub[...], dbuf[...]).astype(BF16)


def later_grads_kernel(x_ref, d_ref, u_ref, da_ref, db_ref, g1_in, g3_in, g2_in, g1, g3, g2):
    del g1_in, g3_in, g2_in
    expert_grads(x_ref, d_ref, u_ref, da_ref, db_ref, g1, g3, g2)


def solution(mesh):
    group = mesh.shape["ep"]
    num_dev = mesh.shape["dp"] * group
    tok_spec = P(("dp", "ep"), None)
    w_spec = P("ep", None, None)
    grad_spec = P(("dp", "ep"), None, None)

    def layer_fn(tokens, expert_ids, gate_vals, w_gate, w_up, w_down, grad_out):
        n_exp, width, hid = w_gate.shape
        tok = tokens.shape[0] // num_dev
        top_k = expert_ids.shape[1]
        cap = ((2 * tok * top_k + 8 * n_exp - 1) // (8 * n_exp)) * 8
        n_loc = n_exp // group
        hot = n_exp // 2
        owner = hot // n_loc
        chips = group // 2
        n_rows = chips * 2 * cap
        hot_rows = group * tok
        cfg = (chips, tok, width, hid, n_loc, cap, owner)

        def device_fn(x, ids, gates, w1, w3, w2, dy):
            any_spec = pl.BlockSpec(memory_space=pl.ANY)
            vmem_spec = pl.BlockSpec(memory_space=pltpu.VMEM)
            sds = jax.ShapeDtypeStruct
            hb = hot_rows // 2
            half = tok // 2
            act_rows = hot_rows + (n_loc - 1) * n_rows
            outs = pl.pallas_call(
                functools.partial(layer_kernel, cfg),
                out_shape=(
                    sds((tok, width), BF16), *[sds((tok, width), F32)] * 2, *[sds((half, width), F32)] * 2, sds((tok, width), F32),
                    sds((n_loc, n_rows, width), BF16), sds((n_loc, n_rows, width), BF16),
                    sds((n_loc, n_rows, hid), BF16), sds((n_loc, n_rows, hid), BF16), sds((n_loc, n_rows, hid), BF16),
                    sds((hot_rows, width), BF16), sds((hot_rows, width), BF16),
                    sds((hot_rows, hid), BF16), sds((hot_rows, hid), BF16), sds((hot_rows, hid), BF16)),
                in_specs=[any_spec, any_spec, vmem_spec, vmem_spec, any_spec, any_spec, any_spec],
                out_specs=[any_spec] * 16,
                scratch_shapes=[
                    pltpu.VMEM((chips, 2 * tok, width), BF16), pltpu.VMEM((chips, 2 * tok, width), BF16),
                    pltpu.VMEM((group, top_k, tok), jnp.int32), pltpu.VMEM((group, top_k, tok), F32),
                    pltpu.VMEM((chips, 8, 2 * tok), F32), pltpu.VMEM((chips, 8, 2 * tok), F32),
                    pltpu.VMEM((chips, 2 * tok, 128), F32),
                    pltpu.VMEM((chips, 2 * tok, width), F32), pltpu.VMEM((chips, 2 * tok, width), F32),
                    pltpu.VMEM((chips, tok, width), F32),
                    pltpu.VMEM((half, width), F32), pltpu.VMEM((half, width), F32),
                    pltpu.VMEM((tok, width), F32), pltpu.VMEM((tok, width), F32),
                    pltpu.VMEM((n_loc, n_rows, width), BF16), pltpu.VMEM((hb, width), BF16),
                    pltpu.VMEM((n_loc, n_rows, hid), BF16), pltpu.VMEM((hot_rows, hid), BF16),
                    pltpu.VMEM((2, hb, hid), BF16), pltpu.VMEM((2, hb, hid), BF16),
                    pltpu.VMEM((act_rows, hid), F32), pltpu.VMEM((act_rows, hid), F32),
                    pltpu.VMEM((hb + n_rows, width), BF16), pltpu.VMEM((n_loc * 2 * cap, 2 * tok), BF16),
                    pltpu.VMEM((2, width, hid), BF16), pltpu.VMEM((2, width, hid), BF16), pltpu.VMEM((2, hid, width), BF16),
                    pltpu.VMEM((tok, width), BF16),
                    pltpu.SemaphoreType.DMA((2, group)), pltpu.SemaphoreType.DMA((2, group)),
                    pltpu.SemaphoreType.DMA((2, 11)), pltpu.SemaphoreType.DMA((2, 11)),
                    pltpu.SemaphoreType.DMA((2, 10)), pltpu.SemaphoreType.DMA((2, 10)),
                    pltpu.SemaphoreType.DMA((3, 2)), pltpu.SemaphoreType.DMA((2, n_loc)), pltpu.SemaphoreType.DMA((5,)),
                    pltpu.SemaphoreType.DMA((2,)), pltpu.SemaphoreType.DMA((7,)), pltpu.SemaphoreType.REGULAR,
                ],
                compiler_params=pltpu.CompilerParams(collective_id=0, has_side_effects=True, vmem_limit_bytes=67043328),
                name="moe_layer",
            )(x, dy, ids.T, gates.T, w1, w3, w2)
            y, go_r, go_l, sr, sl, sc, xr, dr, ur, dar, dbr, xh, dh, uh, dah, dbh = outs

            to_right = [(i, (i + 2) % group) for i in range(group)]
            to_left = [(i, (i + group - 2) % group) for i in range(group)]
            from_l = lax.ppermute(go_r, "ep", to_right)
            from_r = lax.ppermute(go_l, "ep", to_left)

            n_first = (n_loc + 1) // 2
            g_shapes = (sds((n_loc, width, hid), BF16), sds((n_loc, width, hid), BF16), sds((n_loc, hid, width), BF16))

            def blk(r, n, at):
                return pl.BlockSpec((1, r, n), lambda i: (at(i), 0, 0))

            def row_specs(at):
                return [blk(n_rows, width, at), blk(n_rows, width, at), blk(n_rows, hid, at), blk(n_rows, hid, at), blk(n_rows, hid, at)]

            def out_blks(at):
                return [blk(width, hid, at), blk(width, hid, at), blk(hid, width, at)]

            def cost(n):
                return pl.CostEstimate(flops=n * 6 * n_rows * width * hid, transcendentals=0,
                                       bytes_accessed=n * 2 * (2 * n_rows * width + 3 * n_rows * hid + 3 * width * hid))

            def first_at(i):
                return lax.rem(i + 1, n_first)

            def later_at(i):
                return i + n_first

            y_spec = pl.BlockSpec((tok, width), lambda i: (0, 0))
            *grads, y = pl.pallas_call(
                functools.partial(first_grads_kernel, owner),
                grid=(n_first,), out_shape=g_shapes + (sds((tok, width), BF16),),
                in_specs=row_specs(first_at) + [any_spec] * 5 + [y_spec], out_specs=out_blks(first_at) + [y_spec],
                scratch_shapes=[pltpu.VMEM((hot_rows, width), BF16), pltpu.VMEM((hot_rows, width), BF16), pltpu.VMEM((hot_rows, hid), BF16),
                                pltpu.VMEM((hot_rows, hid), BF16), pltpu.VMEM((hot_rows, hid), BF16), pltpu.SemaphoreType.DMA((5,))],
                compiler_params=pltpu.CompilerParams(vmem_limit_bytes=60 << 20),
                cost_estimate=cost(n_first), name="first_grads",
            )(xr, dr, ur, dar, dbr, xh, dh, uh, dah, dbh, y)

            fl_lo = lax.ppermute(sr + from_l[:half], "ep", to_right)
            fr_hi = lax.ppermute(sl + from_r[:half], "ep", to_left)
            g1, g3, g2 = pl.pallas_call(
                later_grads_kernel,
                grid=(n_loc - n_first,), out_shape=g_shapes,
                in_specs=row_specs(later_at) + [any_spec] * 3, out_specs=out_blks(later_at),
                input_output_aliases={5: 0, 6: 1, 7: 2},
                compiler_params=pltpu.CompilerParams(vmem_limit_bytes=60 << 20),
                cost_estimate=cost(n_loc - n_first), name="later_grads",
            )(xr, dr, ur, dar, dbr, *grads)
            fl = jnp.concatenate([fl_lo, from_l[half:]], axis=0)
            fr = jnp.concatenate([from_r[half:], fr_hi], axis=0)
            dx = (sc + fl + fr).astype(BF16)
            return y, dx, g1, g3, g2

        return jax.shard_map(device_fn, mesh=mesh, in_specs=(tok_spec, tok_spec, tok_spec, w_spec, w_spec, w_spec, tok_spec),
                             out_specs=(tok_spec, tok_spec, grad_spec, grad_spec, grad_spec), check_vma=False)(
            tokens, expert_ids, gate_vals, w_gate, w_up, w_down, grad_out)

    return layer_fn
```

```python
import functools

import jax
import jax.numpy as jnp
from jax import lax
from jax.experimental import pallas as pl
from jax.experimental.pallas import tpu as pltpu
from jax.sharding import PartitionSpec as P

MESH = pl.DeviceIdType.MESH
F32 = jnp.float32
BF16 = jnp.bfloat16


def dot_nn(a, b):
    return lax.dot_general(a, b, (((1,), (0,)), ((), ())), preferred_element_type=F32)


def dot_nt(a, b):
    return lax.dot_general(a, b, (((1,), (1,)), ((), ())), preferred_element_type=F32)


def dot_tn(a, b):
    return lax.dot_general(a, b, (((0,), (0,)), ((), ())), preferred_element_type=F32)


def layer_kernel(cfg, x_hbm, dy_hbm, ids_ref, gates_ref, w1_hbm, w3_hbm, w2_hbm,
                 y_hbm, go_r, go_l, sr_hbm, sl_hbm, sc_hbm, xr_hbm, dr_hbm, ur_hbm, da_hbm, db_hbm, xh_hbm, dh_hbm, uh_hbm, dah_hbm, dbh_hbm,
                 x_all, dy_all, ids_all, gates_all, rt, gt, mc, ypart, dxpart, cbuf, yra, yrb, yfl, yfr,
                 erows, hrows, urow, uhot, darow, dbrow, act1, act2, orow, pbuf, w1, w3, w2, outb,
                 m_send, m_recv, ag_send, ag_recv, rs_send, rs_recv, w_sem, st_sem, hst_sem, io_sem, so_sem, free_sem):
    chips, tok, width, hid, n_loc, cap, owner = cfg
    group = 2 * chips
    two = 2 * tok
    cp = 2 * cap
    n_rows = chips * cp
    hot_rows = chips * two
    half = tok // 2
    last = n_loc - 1
    me = lax.axis_index("ep")
    c = me // 2
    k = lax.rem(me, 2)
    c_r = lax.rem(c + 1, chips)
    c_l = lax.rem(c + chips - 1, chips)
    c_o = lax.rem(c + 2, chips)
    near = (c, c_l, c_r, c_o)
    right = 2 * c_r + k
    left = 2 * c_l + k
    partner = 2 * c + 1 - k
    is_owner = me == owner

    own_x = pltpu.make_async_copy(x_hbm, x_all.at[c, pl.ds(k * tok, tok)], io_sem.at[0])
    own_dy = pltpu.make_async_copy(dy_hbm, dy_all.at[c, pl.ds(k * tok, tok)], io_sem.at[1])
    own_x.start()
    own_dy.start()

    def w_copies(e):
        s = lax.rem(e, 2)
        return (pltpu.make_async_copy(w1_hbm.at[e], w1.at[s], w_sem.at[0, s]),
                pltpu.make_async_copy(w3_hbm.at[e], w3.at[s], w_sem.at[1, s]),
                pltpu.make_async_copy(w2_hbm.at[e], w2.at[s], w_sem.at[2, s]))

    for e in (last, last - 1):
        for cpy in w_copies(e):
            cpy.start()
    ids_all[me] = ids_ref[...]
    gates_all[me] = gates_ref[...]

    barrier = pltpu.get_barrier_semaphore()
    for d in range(1, group):
        pl.semaphore_signal(barrier, inc=1, device_id={"ep": lax.rem(me + d, group)}, device_id_type=MESH)
    pl.semaphore_wait(barrier, group - 1)

    def meta_copies(d):
        return tuple(pltpu.make_async_remote_copy(
            src_ref=src, dst_ref=dst.at[me], send_sem=m_send.at[i, d], recv_sem=m_recv.at[i, d],
            device_id={"ep": lax.rem(me + d, group)}, device_id_type=MESH)
            for i, (src, dst) in enumerate(((ids_ref, ids_all), (gates_ref, gates_all))))

    def ag(ref, t, i):
        chip, core, r0, n, dev = (
            (c, k, 0, half, right), (c, k, half, half, right), (c, k, half, half, left), (c, k, 0, half, left),
            (c, k, 0, tok, partner),
            (c_l, k, 0, half, right), (c_r, k, half, half, left),
            (c_l, k, 0, tok, partner), (c_r, k, 0, tok, partner),
            (c_o, k, 0, half, partner), (c_o, k, half, half, partner))[i]
        blk = ref.at[chip, pl.ds(core * tok + r0, n)]
        return pltpu.make_async_remote_copy(
            src_ref=blk, dst_ref=blk, send_sem=ag_send.at[t, i], recv_sem=ag_recv.at[t, i],
            device_id={"ep": dev}, device_id_type=MESH)

    own_x.wait()
    for d in range(1, group):
        for cpy in meta_copies(d):
            cpy.start()
    for i in (4, 0, 2, 1, 3):
        ag(x_all, 0, i).start()
    own_dy.wait()

    for d in range(1, group):
        for cpy in meta_copies(d):
            cpy.wait_recv()

    upper = (lax.broadcasted_iota(jnp.int32, (tok, tok), 0) < lax.broadcasted_iota(jnp.int32, (tok, tok), 1)).astype(F32).astype(BF16)
    row_id = lax.broadcasted_iota(jnp.int32, (8, tok), 0)
    for s in range(group):
        q, core = s // 2, s % 2
        ids = ids_all[s]
        gates = gates_all[s]
        mask_m = jnp.zeros((8, tok), F32)
        gate_m = jnp.zeros((8, tok), F32)
        for le in range(n_loc):
            eq = ids == me * n_loc + le
            hit = jnp.sum(jnp.where(eq, 1.0, 0.0), axis=0, keepdims=True)
            gv = jnp.sum(jnp.where(eq, gates, 0.0), axis=0, keepdims=True)
            mask_m = jnp.where(row_id == le, hit, mask_m)
            gate_m = jnp.where(row_id == le, gv, gate_m)
        rank = dot_nn(mask_m.astype(BF16), upper)
        pos = jnp.where(mask_m > 0.0, rank + float(cap * core), -1.0)
        rt[q, :, core * tok:(core + 1) * tok] = pos
        gt[q, :, core * tok:(core + 1) * tok] = gate_m
        both = jnp.concatenate([pos, gate_m, jnp.zeros((tok - 16, tok), F32)], axis=0)
        mc[q, core * tok:(core + 1) * tok, :] = jnp.transpose(both)

    def pick(p, q, src, scaled):
        for e in range(n_loc):
            hit = rt[q, e:e + 1, :] == lax.broadcasted_iota(jnp.int32, (cp, two), 0).astype(F32)
            pbuf[e * cp:(e + 1) * cp, :] = jnp.where(hit, 1.0, 0.0).astype(BF16)
        gates = [None] * n_loc
        if scaled:
            for e in range(n_loc):
                hit = rt[q, e:e + 1, :] == lax.broadcasted_iota(jnp.int32, (cp, two), 0).astype(F32)
                gates[e] = jnp.sum(jnp.where(hit, gt[q, e:e + 1, :], 0.0), axis=1, keepdims=True)
        for j in range(width // 256):
            cs = slice(j * 256, (j + 1) * 256)
            got = dot_nn(pbuf[...], src[q, :, cs])
            for e in range(n_loc):
                part = got[e * cp:(e + 1) * cp]
                erows[e, pl.ds(p * cp, cp), cs] = (gates[e] * part if scaled else part).astype(BF16)

    def column(q, lane):
        return jnp.sum(jnp.where(lax.broadcasted_iota(jnp.int32, (two, 128), 1) == lane, mc[q], 0.0), axis=1, keepdims=True)

    def put_rows(q, e):
        hit = column(q, e) == lax.broadcasted_iota(jnp.int32, (two, cp), 1).astype(F32)
        return jnp.where(hit, 1.0, 0.0).astype(BF16)

    def forward(m, src, dst, s, aoff, on, emit, used):
        for j in range(hid // 256):
            cs = slice(j * 256, (j + 1) * 256)
            a = dot_nn(src[...], w1[s, :, cs])
            b = dot_nn(src[...], w3[s, :, cs])
            sg = jax.nn.sigmoid(a)
            ga = a * sg
            fa = b * (sg * (1.0 + a * (1.0 - sg)))
            u = ga * b
            if on is not None:
                fa, ga, u = jnp.where(on, fa, 0.0), jnp.where(on, ga, 0.0), jnp.where(on, u, 0.0)
            act1[pl.ds(aoff, m), cs] = fa
            act2[pl.ds(aoff, m), cs] = ga
            dst[:, cs] = u.astype(BF16)

        used(0)
        for j in range(width // 256):
            cs = slice(j * 256, (j + 1) * 256)
            emit(cs, dot_nn(dst[...], w2[s, :, cs]).astype(BF16))

    def backward(m, src, s, aoff, emit):
        for j in range(hid // 256):
            cs = slice(j * 256, (j + 1) * 256)
            du = dot_nt(src[...], w2[s, cs, :])
            darow[s, 0:m, cs] = (du * act1[pl.ds(aoff, m), cs]).astype(BF16)
            dbrow[s, 0:m, cs] = (du * act2[pl.ds(aoff, m), cs]).astype(BF16)
        for j in range(width // 256):
            cs = slice(j * 256, (j + 1) * 256)
            emit(cs, (dot_nt(darow[s, 0:m, :], w1[s, cs, :]) + dot_nt(dbrow[s, 0:m, :], w3[s, cs, :])).astype(BF16))

    def act_off(e):
        return pl.multiple_of(jnp.where(e == 0, 0, hot_rows + (e - 1) * n_rows), 64)

    def add_out(q, e, first, fresh):
        gate = column(q, e + 8)
        put = put_rows(q, e)
        for j in range(width // 256):
            cs = slice(j * 256, (j + 1) * 256)
            ypart[q, :, cs] = jnp.where(fresh, 0.0, ypart[q, :, cs]) + gate * dot_nn(put, orow[first:first + cp, cs])

    def add_dx_one(q, p, e):
        put = put_rows(q, e)
        for j in range(width // 256):
            cs = slice(j * 256, (j + 1) * 256)
            dxpart[q, :, cs] = dot_nn(put, orow[p * cp:(p + 1) * cp, cs])

    def add_dx_two(q, p, e):
        now, before = column(q, e), column(q, e - 1)
        now = jnp.where(now >= 0.0, now + float(cp), -1.0)
        lane = lax.broadcasted_iota(jnp.int32, (two, 2 * cp), 1).astype(F32)
        put = jnp.where(jnp.logical_or(before == lane, now == lane), 1.0, 0.0).astype(BF16)
        for j in range(width // 256):
            cs = slice(j * 256, (j + 1) * 256)
            both = jnp.concatenate([orow[2 * two + p * cp:2 * two + (p + 1) * cp, cs], orow[p * cp:(p + 1) * cp, cs]], axis=0)
            dxpart[q, :, cs] += dot_nn(put, both)

    def lane_of(q, r, n, lane):
        m = mc[q, pl.ds(r, n), :]
        return jnp.sum(jnp.where(lax.broadcasted_iota(jnp.int32, (n, 128), 1) == lane, m, 0.0), axis=1, keepdims=True)

    def hot_forward(p, q, s, fresh):
        o = pl.multiple_of(p * two, 64)
        gate = column(q, 8)

        def emit(cs, out):
            ypart[q, :, cs] = jnp.where(fresh, 0.0, ypart[q, :, cs]) + gate * out.astype(F32)

        forward(two, x_all.at[q], uhot.at[pl.ds(o, two)], s, o, column(q, 0) >= 0.0, emit, lambda part: None)

    def load_next(i, e, step, parts):
        @pl.when(i < last - 1)
        def _():
            for n in parts:
                w_copies(e + 2 * step)[n].start()

    def cold_forward(i, e, step, s, r0, r1):
        def emit(cs, out):
            orow[0:r1 - r0, cs] = out

        forward(r1 - r0, erows.at[e, r0:r1], urow.at[e, r0:r1], s, pl.multiple_of(act_off(e) + r0, 16), None, emit,
                lambda part: load_next(i, e, step, (0, 1)))
        load_next(i, e, step, (2,))

    def weights_here(i, e, first):
        @pl.when(i >= (0 if first else 2))
        def _():
            for cpy in w_copies(e):
                cpy.wait()

    def rs(t, j):
        part = (ypart, dxpart)[t]
        o = k * tok
        if j < 4:
            q = (c_o, c_r, c_l, c)[j]
            src, dst, dev = part.at[q, pl.ds((1 - k) * tok, tok)], cbuf.at[q], partner
        else:
            src, dst, dev = (
                (part.at[c_o, pl.ds(o, half)], yra, right),
                (part.at[c_o, pl.ds(o + half, half)], yrb, left),
                (part.at[c_r, pl.ds(o + half, half)], yfl.at[half:tok], right),
                (part.at[c_l, pl.ds(o, half)], yfr.at[0:half], left),
                (part.at[c_r, pl.ds(o, half)], yfl.at[0:half], right),
                (part.at[c_l, pl.ds(o + half, half)], yfr.at[half:tok], left))[j - 4]
        return pltpu.make_async_remote_copy(
            src_ref=src, dst_ref=dst, send_sem=rs_send.at[t, j], recv_sem=rs_recv.at[t, j],
            device_id={"ep": dev}, device_id_type=MESH)

    def add_rows(part, q, off, src, n):
        @pl.loop(0, n // 32)
        def _(r):
            o = pl.multiple_of(r * 32, 32)
            part[q, pl.ds(pl.multiple_of(off + r * 32, 32), 32)] += src[pl.ds(o, 32)]

    ag(x_all, 0, 4).wait_recv()
    pick(0, c, x_all, False)

    @pl.loop(0, n_loc)
    def _(i):
        e = last - i
        s = lax.rem(e, 2)
        hot = jnp.logical_and(is_owner, e == 0)
        weights_here(i, e, True)

        @pl.when(i == 3)
        def _():
            ag(x_all, 0, 0).wait_recv()
            ag(x_all, 0, 5).start()
            ag(x_all, 0, 2).wait_recv()
            ag(x_all, 0, 6).start()
            for n in (4, 0, 2, 1, 3):
                ag(dy_all, 1, n).start()

        @pl.when(jnp.logical_not(hot))
        def _():
            cold_forward(i, e, -1, s, 0, cp)
            add_out(c, e, 0, i == 0)

        @pl.when(hot)
        def _():
            hot_forward(0, c, s, False)

    ag(x_all, 0, 1).wait_recv()
    ag(x_all, 0, 7).start()
    ag(x_all, 0, 3).wait_recv()
    ag(x_all, 0, 8).start()
    rs(0, 3).start()
    ag(x_all, 0, 7).wait_recv()
    pick(1, c_l, x_all, False)
    ag(x_all, 0, 8).wait_recv()
    pick(2, c_r, x_all, False)

    @pl.loop(0, n_loc)
    def _(e):
        s = lax.rem(e, 2)
        hot = jnp.logical_and(is_owner, e == 0)
        weights_here(e, e, False)

        @pl.when(e == 2)
        def _():
            ag(x_all, 0, 5).wait_recv()
            ag(x_all, 0, 9).start()
            ag(x_all, 0, 6).wait_recv()
            ag(x_all, 0, 10).start()

        @pl.when(e == last)
        def _():
            ag(dy_all, 1, 0).wait_recv()
            ag(dy_all, 1, 5).start()
            ag(dy_all, 1, 2).wait_recv()
            ag(dy_all, 1, 6).start()

        @pl.when(jnp.logical_not(hot))
        def _():
            cold_forward(e, e, 1, s, cp, 3 * cp)
            for j, p in ((1, 2), (2, 1)):
                add_out(near[p], e, (p - 1) * cp, e == 0)

                @pl.when(e == last)
                def _():
                    rs(0, j).start()

        @pl.when(hot)
        def _():
            @pl.loop(1, 3)
            def _(p):
                hot_forward(p, jnp.where(p == 1, c_l, c_r), s, True)

            load_next(e, e, 1, (0, 1, 2))

    rs(0, 3).wait_recv()
    add_rows(ypart, c, k * tok, cbuf.at[c], tok)
    ag(x_all, 0, 9).wait_recv()
    ag(x_all, 0, 10).wait_recv()
    pick(3, c_o, x_all, False)

    def st_fwd(e):
        return (pltpu.make_async_copy(erows.at[e], xr_hbm.at[e], st_sem.at[0, e]),
                pltpu.make_async_copy(urow.at[e], ur_hbm.at[e], st_sem.at[1, e]))

    for e in range(n_loc):
        st_fwd(e)[0].start()

    def st_hot():
        return [pltpu.make_async_copy(uhot, uh_hbm, hst_sem.at[0])] + [
            pltpu.make_async_copy(x_all.at[q], xh_hbm.at[p * two:(p + 1) * two], hst_sem.at[1 + p]) for p, q in enumerate(near)]

    @pl.loop(0, n_loc)
    def _(i):
        e = last - i
        s = lax.rem(e, 2)
        hot = jnp.logical_and(is_owner, e == 0)
        weights_here(i, e, False)

        @pl.when(i == 1)
        def _():
            for j, q in ((1, c_r), (2, c_l)):
                rs(0, j).wait_recv()
                add_rows(ypart, q, k * tok, cbuf.at[q], tok)
                rs(0, 5 + j).start()

        @pl.when(i == 3)
        def _():
            ag(dy_all, 1, 4).wait_recv()
            ag(dy_all, 1, 1).wait_recv()
            ag(dy_all, 1, 7).start()
            ag(dy_all, 1, 3).wait_recv()
            ag(dy_all, 1, 8).start()

        @pl.when(jnp.logical_not(hot))
        def _():
            cold_forward(i, e, -1, s, 3 * cp, n_rows)
            add_out(c_o, e, 0, i == 0)
            st_fwd(e)[1].start()

        @pl.when(hot)
        def _():
            hot_forward(3, c_o, s, False)
            for cpy in st_hot():
                cpy.start()

    rs(0, 0).start()

    for e in range(n_loc):
        st_fwd(e)[0].wait()
    pick(0, c, dy_all, True)
    rs(0, 0).wait_recv()
    add_rows(ypart, c_o, k * tok, cbuf.at[c_o], tok)
    rs(0, 4).start()
    rs(0, 5).start()
    pl.semaphore_signal(free_sem, inc=1, device_id={"ep": partner}, device_id_type=MESH)
    ag(dy_all, 1, 7).wait_recv()
    pick(1, c_l, dy_all, True)
    ag(dy_all, 1, 5).wait_recv()
    ag(dy_all, 1, 9).start()
    ag(dy_all, 1, 6).wait_recv()
    ag(dy_all, 1, 10).start()
    ag(dy_all, 1, 8).wait_recv()
    pick(2, c_r, dy_all, True)
    ag(dy_all, 1, 9).wait_recv()
    ag(dy_all, 1, 10).wait_recv()
    pick(3, c_o, dy_all, True)

    @pl.loop(0, n_loc)
    def _(e):
        @pl.when(jnp.logical_not(jnp.logical_and(is_owner, e == 0)))
        def _():
            st_fwd(e)[1].wait()

    @pl.when(is_owner)
    def _():
        for cpy in st_hot():
            cpy.wait()

    def st_d(e):
        return pltpu.make_async_copy(erows.at[e], dr_hbm.at[e], st_sem.at[0, e])

    def st_ab(e, s):
        return (pltpu.make_async_copy(darow.at[s, 0:n_rows], da_hbm.at[e], st_sem.at[1, s]),
                pltpu.make_async_copy(dbrow.at[s, 0:n_rows], db_hbm.at[e], st_sem.at[1, 2 + s]))

    for e in range(n_loc):
        st_d(e).start()

    def rs_relay_y():
        rs(0, 4).wait_recv()
        add_rows(ypart, c_r, k * tok, yra, half)
        rs(0, 8).start()
        rs(0, 5).wait_recv()
        add_rows(ypart, c_l, k * tok + half, yrb, half)
        rs(0, 9).start()

    @pl.loop(0, n_loc)
    def _(e):
        s = lax.rem(e, 2)
        hot = jnp.logical_and(is_owner, e == 0)

        weights_here(e, e, False)

        @pl.when(jnp.logical_not(hot))
        def _():
            ooff = pl.multiple_of(s * 2 * two, 64)

            def emit(cs, out):
                orow[pl.ds(ooff, n_rows), cs] = out

            backward(n_rows, erows.at[e], s, act_off(e), emit)
            load_next(e, e, 1, (0, 1, 2))

            @pl.when(e == last - 1)
            def _():
                rs_relay_y()

            @pl.when(e == 0)
            def _():
                for p in range(chips):
                    add_dx_one(near[p], p, e)

            @pl.when(e == last)
            def _():
                pl.semaphore_wait(free_sem, 1)

            @pl.when(jnp.logical_and(e > 0, s == 0))
            def _():
                for j, p in enumerate((3, 2, 1, 0)):
                    add_dx_two(near[p], p, e)

                    @pl.when(e == last)
                    def _():
                        rs(1, j).start()

        @pl.when(hot)
        def _():
            @pl.loop(0, chips // 2)
            def _(h):
                pair = (jnp.where(h == 0, c, c_r), jnp.where(h == 0, c_l, c_o))
                for n, q in enumerate(pair):
                    @pl.loop(0, two // 64)
                    def _(r):
                        at = pl.multiple_of(r * 64, 64)
                        got = dy_all[q, pl.ds(at, 64), :].astype(F32)
                        hrows[pl.ds(pl.multiple_of(n * two + r * 64, 64), 64), :] = (lane_of(q, at, 64, 8) * got).astype(BF16)

                o = pl.multiple_of(h * 2 * two, 64)
                sd = pltpu.make_async_copy(hrows, dh_hbm.at[pl.ds(o, 2 * two)], hst_sem.at[0])
                sd.start()

                def emit(cs, out):
                    for n, q in enumerate(pair):
                        dxpart[q, :, cs] = out[n * two:(n + 1) * two].astype(F32)

                backward(2 * two, hrows, s, o, emit)
                sa = pltpu.make_async_copy(darow.at[s], dah_hbm.at[pl.ds(o, 2 * two)], hst_sem.at[1])
                sb = pltpu.make_async_copy(dbrow.at[s], dbh_hbm.at[pl.ds(o, 2 * two)], hst_sem.at[2])
                sa.start()
                sb.start()
                sd.wait()
                sa.wait()
                sb.wait()

            load_next(e, e, 1, (0, 1, 2))

        @pl.when(jnp.logical_and(e >= 1, jnp.logical_not(jnp.logical_and(is_owner, e == 1))))
        def _():
            for cpy in st_ab(e - 1, 1 - s):
                cpy.wait()

        @pl.when(jnp.logical_not(hot))
        def _():
            for cpy in st_ab(e, s):
                cpy.start()

    def rs_end_y():
        for j in (6, 7, 8, 9):
            rs(0, j).wait_recv()

        @pl.loop(0, tok // 32)
        def _(r):
            o = pl.multiple_of(r * 32, 32)
            total = ypart[c, pl.ds(pl.multiple_of(k * tok + r * 32, 32), 32)] + yfl[pl.ds(o, 32)] + yfr[pl.ds(o, 32)]
            outb[pl.ds(o, 32)] = total.astype(BF16)

        return pltpu.make_async_copy(outb, y_hbm, io_sem.at[0])

    def chip_sums_out(j):
        q = (c_o, c_r, c_l, c)[j]
        lo = dxpart.at[q, pl.ds(k * tok, half)]
        hi = dxpart.at[q, pl.ds(k * tok + half, half)]
        if j == 3:
            return (pltpu.make_async_copy(dxpart.at[q, pl.ds(k * tok, tok)], sc_hbm, so_sem.at[6]),)
        to_lo, to_hi = ((go_r.at[0:half], go_l.at[0:half]), (sr_hbm, go_r.at[half:tok]), (go_l.at[half:tok], sl_hbm))[j]
        return (pltpu.make_async_copy(lo, to_lo, so_sem.at[2 * j]), pltpu.make_async_copy(hi, to_hi, so_sem.at[2 * j + 1]))

    for j, q in enumerate((c_o, c_r, c_l, c)):
        rs(1, j).wait_recv()
        add_rows(dxpart, q, k * tok, cbuf.at[q], tok)
        for cpy in chip_sums_out(j):
            cpy.start()
    y_out = rs_end_y()
    y_out.start()

    for e in range(n_loc):
        st_d(e).wait()
    for cpy in st_ab(last, last % 2):
        cpy.wait()
    for d in range(1, group):
        for cpy in meta_copies(d):
            cpy.wait_send()
    for i in range(11):
        ag(x_all, 0, i).wait_send()
        ag(dy_all, 1, i).wait_send()
    for j in range(10):
        rs(0, j).wait_send()
    for j in range(4):
        rs(1, j).wait_send()
        for cpy in chip_sums_out(j):
            cpy.wait()
    y_out.wait()


def expert_grads(x_ref, d_ref, u_ref, da_ref, db_ref, g1, g3, g2):
    g1[0] = dot_tn(x_ref[0], da_ref[0]).astype(BF16)
    g3[0] = dot_tn(x_ref[0], db_ref[0]).astype(BF16)
    g2[0] = dot_tn(u_ref[0], d_ref[0]).astype(BF16)


def first_grads_kernel(owner, x_ref, d_ref, u_ref, da_ref, db_ref, xh, dh, uh, dah, dbh, y_ref, g1, g3, g2, y_out, xb, dbuf, ub, dab, dbb, sem):
    i = pl.program_id(0)
    y_out[...] = y_ref[...]
    is_owner = lax.axis_index("ep") == owner
    hot = jnp.logical_and(is_owner, i == pl.num_programs(0) - 1)

    def copies():
        return [pltpu.make_async_copy(src, dst, sem.at[j]) for j, (src, dst) in enumerate(((xh, xb), (dah, dab), (dbh, dbb), (uh, ub), (dh, dbuf)))]

    @pl.when(jnp.logical_and(is_owner, i == 0))
    def _():
        for cpy in copies():
            cpy.start()

    @pl.when(jnp.logical_not(hot))
    def _():
        expert_grads(x_ref, d_ref, u_ref, da_ref, db_ref, g1, g3, g2)

    @pl.when(hot)
    def _():
        for cpy in copies():
            cpy.wait()
        g1[0] = dot_tn(xb[...], dab[...]).astype(BF16)
        g3[0] = dot_tn(xb[...], dbb[...]).astype(BF16)
        g2[0] = dot_tn(ub[...], dbuf[...]).astype(BF16)


def later_grads_kernel(x_ref, d_ref, u_ref, da_ref, db_ref, g1_in, g3_in, g2_in, g1, g3, g2):
    del g1_in, g3_in, g2_in
    expert_grads(x_ref, d_ref, u_ref, da_ref, db_ref, g1, g3, g2)


def solution(mesh):
    group = mesh.shape["ep"]
    num_dev = mesh.shape["dp"] * group
    tok_spec = P(("dp", "ep"), None)
    w_spec = P("ep", None, None)
    grad_spec = P(("dp", "ep"), None, None)

    def layer_fn(tokens, expert_ids, gate_vals, w_gate, w_up, w_down, grad_out):
        n_exp, width, hid = w_gate.shape
        tok = tokens.shape[0] // num_dev
        top_k = expert_ids.shape[1]
        cap = ((2 * tok * top_k + 8 * n_exp - 1) // (8 * n_exp)) * 8
        n_loc = n_exp // group
        hot = n_exp // 2
        owner = hot // n_loc
        chips = group // 2
        n_rows = chips * 2 * cap
        hot_rows = group * tok
        cfg = (chips, tok, width, hid, n_loc, cap, owner)

        def device_fn(x, ids, gates, w1, w3, w2, dy):
            any_spec = pl.BlockSpec(memory_space=pl.ANY)
            vmem_spec = pl.BlockSpec(memory_space=pltpu.VMEM)
            sds = jax.ShapeDtypeStruct
            hb = hot_rows // 2
            half = tok // 2
            act_rows = hot_rows + (n_loc - 1) * n_rows
            outs = pl.pallas_call(
                functools.partial(layer_kernel, cfg),
                out_shape=(
                    sds((tok, width), BF16), *[sds((tok, width), F32)] * 2, *[sds((half, width), F32)] * 2, sds((tok, width), F32),
                    sds((n_loc, n_rows, width), BF16), sds((n_loc, n_rows, width), BF16),
                    sds((n_loc, n_rows, hid), BF16), sds((n_loc, n_rows, hid), BF16), sds((n_loc, n_rows, hid), BF16),
                    sds((hot_rows, width), BF16), sds((hot_rows, width), BF16),
                    sds((hot_rows, hid), BF16), sds((hot_rows, hid), BF16), sds((hot_rows, hid), BF16)),
                in_specs=[any_spec, any_spec, vmem_spec, vmem_spec, any_spec, any_spec, any_spec],
                out_specs=[any_spec] * 16,
                scratch_shapes=[
                    pltpu.VMEM((chips, 2 * tok, width), BF16), pltpu.VMEM((chips, 2 * tok, width), BF16),
                    pltpu.VMEM((group, top_k, tok), jnp.int32), pltpu.VMEM((group, top_k, tok), F32),
                    pltpu.VMEM((chips, 8, 2 * tok), F32), pltpu.VMEM((chips, 8, 2 * tok), F32),
                    pltpu.VMEM((chips, 2 * tok, 128), F32),
                    pltpu.VMEM((chips, 2 * tok, width), F32), pltpu.VMEM((chips, 2 * tok, width), F32),
                    pltpu.VMEM((chips, tok, width), F32),
                    pltpu.VMEM((half, width), F32), pltpu.VMEM((half, width), F32),
                    pltpu.VMEM((tok, width), F32), pltpu.VMEM((tok, width), F32),
                    pltpu.VMEM((n_loc, n_rows, width), BF16), pltpu.VMEM((hb, width), BF16),
                    pltpu.VMEM((n_loc, n_rows, hid), BF16), pltpu.VMEM((hot_rows, hid), BF16),
                    pltpu.VMEM((2, hb, hid), BF16), pltpu.VMEM((2, hb, hid), BF16),
                    pltpu.VMEM((act_rows, hid), F32), pltpu.VMEM((act_rows, hid), F32),
                    pltpu.VMEM((hb + n_rows, width), BF16), pltpu.VMEM((n_loc * 2 * cap, 2 * tok), BF16),
                    pltpu.VMEM((2, width, hid), BF16), pltpu.VMEM((2, width, hid), BF16), pltpu.VMEM((2, hid, width), BF16),
                    pltpu.VMEM((tok, width), BF16),
                    pltpu.SemaphoreType.DMA((2, group)), pltpu.SemaphoreType.DMA((2, group)),
                    pltpu.SemaphoreType.DMA((2, 11)), pltpu.SemaphoreType.DMA((2, 11)),
                    pltpu.SemaphoreType.DMA((2, 10)), pltpu.SemaphoreType.DMA((2, 10)),
                    pltpu.SemaphoreType.DMA((3, 2)), pltpu.SemaphoreType.DMA((2, n_loc)), pltpu.SemaphoreType.DMA((5,)),
                    pltpu.SemaphoreType.DMA((2,)), pltpu.SemaphoreType.DMA((7,)), pltpu.SemaphoreType.REGULAR,
                ],
                compiler_params=pltpu.CompilerParams(collective_id=0, has_side_effects=True, vmem_limit_bytes=67043328),
                name="moe_layer",
            )(x, dy, ids.T, gates.T, w1, w3, w2)
            y, go_r, go_l, sr, sl, sc, xr, dr, ur, dar, dbr, xh, dh, uh, dah, dbh = outs

            to_right = [(i, (i + 2) % group) for i in range(group)]
            to_left = [(i, (i + group - 2) % group) for i in range(group)]
            from_l = lax.ppermute(go_r, "ep", to_right)
            from_r = lax.ppermute(go_l, "ep", to_left)

            n_first = (n_loc + 1) // 2
            g_shapes = (sds((n_loc, width, hid), BF16), sds((n_loc, width, hid), BF16), sds((n_loc, hid, width), BF16))

            def blk(r, n, at):
                return pl.BlockSpec((1, r, n), lambda i: (at(i), 0, 0))

            def row_specs(at):
                return [blk(n_rows, width, at), blk(n_rows, width, at), blk(n_rows, hid, at), blk(n_rows, hid, at), blk(n_rows, hid, at)]

            def out_blks(at):
                return [blk(width, hid, at), blk(width, hid, at), blk(hid, width, at)]

            def cost(n):
                return pl.CostEstimate(flops=n * 6 * n_rows * width * hid, transcendentals=0,
                                       bytes_accessed=n * 2 * (2 * n_rows * width + 3 * n_rows * hid + 3 * width * hid))

            def first_at(i):
                return lax.rem(i + 1, n_first)

            def later_at(i):
                return i + n_first

            y_spec = pl.BlockSpec((tok, width), lambda i: (0, 0))
            *grads, y = pl.pallas_call(
                functools.partial(first_grads_kernel, owner),
                grid=(n_first,), out_shape=g_shapes + (sds((tok, width), BF16),),
                in_specs=row_specs(first_at) + [any_spec] * 5 + [y_spec], out_specs=out_blks(first_at) + [y_spec],
                scratch_shapes=[pltpu.VMEM((hot_rows, width), BF16), pltpu.VMEM((hot_rows, width), BF16), pltpu.VMEM((hot_rows, hid), BF16),
                                pltpu.VMEM((hot_rows, hid), BF16), pltpu.VMEM((hot_rows, hid), BF16), pltpu.SemaphoreType.DMA((5,))],
                compiler_params=pltpu.CompilerParams(vmem_limit_bytes=60 << 20),
                cost_estimate=cost(n_first), name="first_grads",
            )(xr, dr, ur, dar, dbr, xh, dh, uh, dah, dbh, y)

            fl_lo = lax.ppermute(sr + from_l[:half], "ep", to_right)
            fr_hi = lax.ppermute(sl + from_r[:half], "ep", to_left)
            g1, g3, g2 = pl.pallas_call(
                later_grads_kernel,
                grid=(n_loc - n_first,), out_shape=g_shapes,
                in_specs=row_specs(later_at) + [any_spec] * 3, out_specs=out_blks(later_at),
                input_output_aliases={5: 0, 6: 1, 7: 2},
                compiler_params=pltpu.CompilerParams(vmem_limit_bytes=60 << 20),
                cost_estimate=cost(n_loc - n_first), name="later_grads",
            )(xr, dr, ur, dar, dbr, *grads)
            fl = jnp.concatenate([fl_lo, from_l[half:]], axis=0)
            fr = jnp.concatenate([from_r[half:], fr_hi], axis=0)
            dx = (sc + fl + fr).astype(BF16)
            return y, dx, g1, g3, g2

        return jax.shard_map(device_fn, mesh=mesh, in_specs=(tok_spec, tok_spec, tok_spec, w_spec, w_spec, w_spec, tok_spec),
                             out_specs=(tok_spec, tok_spec, grad_spec, grad_spec, grad_spec), check_vma=False)(
            tokens, expert_ids, gate_vals, w_gate, w_up, w_down, grad_out)

    return layer_fn
```

```python
import functools

import jax
import jax.numpy as jnp
from jax import lax
from jax.experimental import pallas as pl
from jax.experimental.pallas import tpu as pltpu
from jax.sharding import PartitionSpec as P

MESH = pl.DeviceIdType.MESH
F32 = jnp.float32
BF16 = jnp.bfloat16


def dot_nn(a, b):
    return lax.dot_general(a, b, (((1,), (0,)), ((), ())), preferred_element_type=F32)


def dot_nt(a, b):
    return lax.dot_general(a, b, (((1,), (1,)), ((), ())), preferred_element_type=F32)


def dot_tn(a, b):
    return lax.dot_general(a, b, (((0,), (0,)), ((), ())), preferred_element_type=F32)


def layer_kernel(cfg, x_hbm, dy_hbm, ids_ref, gates_ref, w1_hbm, w3_hbm, w2_hbm,
                 y_hbm, go_r, go_l, sr_hbm, sl_hbm, sc_hbm, xr_hbm, dr_hbm, ur_hbm, da_hbm, db_hbm, xh_hbm, dh_hbm, uh_hbm, dah_hbm, dbh_hbm,
                 x_all, dy_all, ids_all, gates_all, rt, gt, mc, ypart, dxpart, cbuf, yra, yrb, yfl, yfr,
                 erows, hrows, urow, uhot, darow, dbrow, act1, act2, orow, pbuf, w1, w3, w2, outb,
                 m_send, m_recv, ag_send, ag_recv, rs_send, rs_recv, w_sem, st_sem, hst_sem, io_sem, so_sem, free_sem):
    chips, tok, width, hid, n_loc, cap, owner = cfg
    group = 2 * chips
    two = 2 * tok
    cp = 2 * cap
    n_rows = chips * cp
    hot_rows = chips * two
    half = tok // 2
    last = n_loc - 1
    me = lax.axis_index("ep")
    c = me // 2
    k = lax.rem(me, 2)
    c_r = lax.rem(c + 1, chips)
    c_l = lax.rem(c + chips - 1, chips)
    c_o = lax.rem(c + 2, chips)
    near = (c, c_l, c_r, c_o)
    right = 2 * c_r + k
    left = 2 * c_l + k
    partner = 2 * c + 1 - k
    is_owner = me == owner

    own_x = pltpu.make_async_copy(x_hbm, x_all.at[c, pl.ds(k * tok, tok)], io_sem.at[0])
    own_dy = pltpu.make_async_copy(dy_hbm, dy_all.at[c, pl.ds(k * tok, tok)], io_sem.at[1])
    own_x.start()
    own_dy.start()

    def w_copies(e):
        s = lax.rem(e, 2)
        return (pltpu.make_async_copy(w1_hbm.at[e], w1.at[s], w_sem.at[0, s]),
                pltpu.make_async_copy(w3_hbm.at[e], w3.at[s], w_sem.at[1, s]),
                pltpu.make_async_copy(w2_hbm.at[e], w2.at[s], w_sem.at[2, s]))

    for e in (0, 1):
        for cpy in w_copies(e):
            cpy.start()
    ids_all[me] = ids_ref[...]
    gates_all[me] = gates_ref[...]

    barrier = pltpu.get_barrier_semaphore()
    for d in range(1, group):
        pl.semaphore_signal(barrier, inc=1, device_id={"ep": lax.rem(me + d, group)}, device_id_type=MESH)
    pl.semaphore_wait(barrier, group - 1)

    def meta_copies(d):
        return tuple(pltpu.make_async_remote_copy(
            src_ref=src, dst_ref=dst.at[me], send_sem=m_send.at[i, d], recv_sem=m_recv.at[i, d],
            device_id={"ep": lax.rem(me + d, group)}, device_id_type=MESH)
            for i, (src, dst) in enumerate(((ids_ref, ids_all), (gates_ref, gates_all))))

    def ag(ref, t, i):
        chip, core, r0, n, dev = (
            (c, k, 0, half, right), (c, k, half, half, right), (c, k, half, half, left), (c, k, 0, half, left),
            (c, k, 0, tok, partner),
            (c_l, k, 0, half, right), (c_r, k, half, half, left),
            (c_l, k, 0, tok, partner), (c_r, k, 0, tok, partner),
            (c_o, k, 0, half, partner), (c_o, k, half, half, partner))[i]
        blk = ref.at[chip, pl.ds(core * tok + r0, n)]
        return pltpu.make_async_remote_copy(
            src_ref=blk, dst_ref=blk, send_sem=ag_send.at[t, i], recv_sem=ag_recv.at[t, i],
            device_id={"ep": dev}, device_id_type=MESH)

    own_x.wait()
    for d in range(1, group):
        for cpy in meta_copies(d):
            cpy.start()
    for i in (4, 0, 2, 1, 3):
        ag(x_all, 0, i).start()
    own_dy.wait()

    for d in range(1, group):
        for cpy in meta_copies(d):
            cpy.wait_recv()

    upper = (lax.broadcasted_iota(jnp.int32, (tok, tok), 0) < lax.broadcasted_iota(jnp.int32, (tok, tok), 1)).astype(F32).astype(BF16)
    row_id = lax.broadcasted_iota(jnp.int32, (8, tok), 0)
    for s in range(group):
        q, core = s // 2, s % 2
        ids = ids_all[s]
        gates = gates_all[s]
        mask_m = jnp.zeros((8, tok), F32)
        gate_m = jnp.zeros((8, tok), F32)
        for le in range(n_loc):
            eq = ids == me * n_loc + le
            hit = jnp.sum(jnp.where(eq, 1.0, 0.0), axis=0, keepdims=True)
            gv = jnp.sum(jnp.where(eq, gates, 0.0), axis=0, keepdims=True)
            mask_m = jnp.where(row_id == le, hit, mask_m)
            gate_m = jnp.where(row_id == le, gv, gate_m)
        rank = dot_nn(mask_m.astype(BF16), upper)
        pos = jnp.where(mask_m > 0.0, rank + float(cap * core), -1.0)
        rt[q, :, core * tok:(core + 1) * tok] = pos
        gt[q, :, core * tok:(core + 1) * tok] = gate_m
        both = jnp.concatenate([pos, gate_m, jnp.zeros((tok - 16, tok), F32)], axis=0)
        mc[q, core * tok:(core + 1) * tok, :] = jnp.transpose(both)

    def pick(p, q, src, scaled):
        for e in range(n_loc):
            hit = rt[q, e:e + 1, :] == lax.broadcasted_iota(jnp.int32, (cp, two), 0).astype(F32)
            pbuf[e * cp:(e + 1) * cp, :] = jnp.where(hit, 1.0, 0.0).astype(BF16)
        gates = [None] * n_loc
        if scaled:
            for e in range(n_loc):
                hit = rt[q, e:e + 1, :] == lax.broadcasted_iota(jnp.int32, (cp, two), 0).astype(F32)
                gates[e] = jnp.sum(jnp.where(hit, gt[q, e:e + 1, :], 0.0), axis=1, keepdims=True)
        for j in range(width // 256):
            cs = slice(j * 256, (j + 1) * 256)
            got = dot_nn(pbuf[...], src[q, :, cs])
            for e in range(n_loc):
                part = got[e * cp:(e + 1) * cp]
                erows[e, pl.ds(p * cp, cp), cs] = (gates[e] * part if scaled else part).astype(BF16)

    def column(q, lane):
        return jnp.sum(jnp.where(lax.broadcasted_iota(jnp.int32, (two, 128), 1) == lane, mc[q], 0.0), axis=1, keepdims=True)

    def put_rows(q, e):
        hit = column(q, e) == lax.broadcasted_iota(jnp.int32, (two, cp), 1).astype(F32)
        return jnp.where(hit, 1.0, 0.0).astype(BF16)

    def forward(m, src, dst, s, aoff, on, emit, used):
        for j in range(hid // 256):
            cs = slice(j * 256, (j + 1) * 256)
            a = dot_nn(src[...], w1[s, :, cs])
            b = dot_nn(src[...], w3[s, :, cs])
            sg = jax.nn.sigmoid(a)
            ga = a * sg
            fa = b * (sg * (1.0 + a * (1.0 - sg)))
            u = ga * b
            if on is not None:
                fa, ga, u = jnp.where(on, fa, 0.0), jnp.where(on, ga, 0.0), jnp.where(on, u, 0.0)
            act1[pl.ds(aoff, m), cs] = fa
            act2[pl.ds(aoff, m), cs] = ga
            dst[:, cs] = u.astype(BF16)

        used(0)
        for j in range(width // 256):
            cs = slice(j * 256, (j + 1) * 256)
            emit(cs, dot_nn(dst[...], w2[s, :, cs]).astype(BF16))

    def backward(m, src, s, aoff, emit):
        for j in range(hid // 256):
            cs = slice(j * 256, (j + 1) * 256)
            du = dot_nt(src[...], w2[s, cs, :])
            darow[s, 0:m, cs] = (du * act1[pl.ds(aoff, m), cs]).astype(BF16)
            dbrow[s, 0:m, cs] = (du * act2[pl.ds(aoff, m), cs]).astype(BF16)
        for j in range(width // 256):
            cs = slice(j * 256, (j + 1) * 256)
            emit(cs, (dot_nt(darow[s, 0:m, :], w1[s, cs, :]) + dot_nt(dbrow[s, 0:m, :], w3[s, cs, :])).astype(BF16))

    def act_off(e):
        return pl.multiple_of(jnp.where(e == 0, 0, hot_rows + (e - 1) * n_rows), 64)

    def add_out(q, e, first, fresh):
        gate = column(q, e + 8)
        put = put_rows(q, e)
        for j in range(width // 256):
            cs = slice(j * 256, (j + 1) * 256)
            ypart[q, :, cs] = jnp.where(fresh, 0.0, ypart[q, :, cs]) + gate * dot_nn(put, orow[first:first + cp, cs])

    def add_dx_one(q, p, e):
        put = put_rows(q, e)
        for j in range(width // 256):
            cs = slice(j * 256, (j + 1) * 256)
            dxpart[q, :, cs] = dot_nn(put, orow[p * cp:(p + 1) * cp, cs])

    def add_dx_two(q, p, e):
        now, before = column(q, e), column(q, e - 1)
        now = jnp.where(now >= 0.0, now + float(cp), -1.0)
        lane = lax.broadcasted_iota(jnp.int32, (two, 2 * cp), 1).astype(F32)
        put = jnp.where(jnp.logical_or(before == lane, now == lane), 1.0, 0.0).astype(BF16)
        for j in range(width // 256):
            cs = slice(j * 256, (j + 1) * 256)
            both = jnp.concatenate([orow[2 * two + p * cp:2 * two + (p + 1) * cp, cs], orow[p * cp:(p + 1) * cp, cs]], axis=0)
            dxpart[q, :, cs] += dot_nn(put, both)

    def lane_of(q, r, n, lane):
        m = mc[q, pl.ds(r, n), :]
        return jnp.sum(jnp.where(lax.broadcasted_iota(jnp.int32, (n, 128), 1) == lane, m, 0.0), axis=1, keepdims=True)

    def hot_forward(p, q, s, fresh):
        o = pl.multiple_of(p * two, 64)
        gate = column(q, 8)

        def emit(cs, out):
            ypart[q, :, cs] = jnp.where(fresh, 0.0, ypart[q, :, cs]) + gate * out.astype(F32)

        forward(two, x_all.at[q], uhot.at[pl.ds(o, two)], s, o, column(q, 0) >= 0.0, emit, lambda part: None)

    def load_next(i, e, step, parts):
        @pl.when(i < last - 1)
        def _():
            for n in parts:
                w_copies(e + 2 * step)[n].start()

    def cold_forward(i, e, step, s, r0, r1):
        def emit(cs, out):
            orow[0:r1 - r0, cs] = out

        forward(r1 - r0, erows.at[e, r0:r1], urow.at[e, r0:r1], s, pl.multiple_of(act_off(e) + r0, 16), None, emit,
                lambda part: load_next(i, e, step, (0, 1)))
        load_next(i, e, step, (2,))

    def weights_here(i, e, first):
        @pl.when(i >= (0 if first else 2))
        def _():
            for cpy in w_copies(e):
                cpy.wait()

    def rs(t, j):
        part = (ypart, dxpart)[t]
        o = k * tok
        if j < 4:
            q = (c_o, c_r, c_l, c)[j]
            src, dst, dev = part.at[q, pl.ds((1 - k) * tok, tok)], cbuf.at[q], partner
        else:
            src, dst, dev = (
                (part.at[c_o, pl.ds(o, half)], yra, right),
                (part.at[c_o, pl.ds(o + half, half)], yrb, left),
                (part.at[c_r, pl.ds(o + half, half)], yfl.at[half:tok], right),
                (part.at[c_l, pl.ds(o, half)], yfr.at[0:half], left),
                (part.at[c_r, pl.ds(o, half)], yfl.at[0:half], right),
                (part.at[c_l, pl.ds(o + half, half)], yfr.at[half:tok], left))[j - 4]
        return pltpu.make_async_remote_copy(
            src_ref=src, dst_ref=dst, send_sem=rs_send.at[t, j], recv_sem=rs_recv.at[t, j],
            device_id={"ep": dev}, device_id_type=MESH)

    def add_rows(part, q, off, src, n):
        @pl.loop(0, n // 32)
        def _(r):
            o = pl.multiple_of(r * 32, 32)
            part[q, pl.ds(pl.multiple_of(off + r * 32, 32), 32)] += src[pl.ds(o, 32)]

    ag(x_all, 0, 4).wait_recv()
    pick(0, c, x_all, False)

    @pl.loop(0, n_loc)
    def _(e):
        s = lax.rem(e, 2)
        hot = jnp.logical_and(is_owner, e == 0)
        weights_here(e, e, True)

        @pl.when(e == 2)
        def _():
            ag(x_all, 0, 0).wait_recv()
            ag(x_all, 0, 5).start()
            ag(x_all, 0, 2).wait_recv()
            ag(x_all, 0, 6).start()
            for n in (4, 0, 2, 1, 3):
                ag(dy_all, 1, n).start()

        @pl.when(jnp.logical_not(hot))
        def _():
            cold_forward(e, e, 1, s, 0, cp)
            add_out(c, e, 0, e == 0)

        @pl.when(hot)
        def _():
            hot_forward(0, c, s, True)
            load_next(e, e, 1, (0, 1, 2))

    ag(x_all, 0, 1).wait_recv()
    ag(x_all, 0, 7).start()
    ag(x_all, 0, 3).wait_recv()
    ag(x_all, 0, 8).start()
    rs(0, 3).start()
    ag(x_all, 0, 7).wait_recv()
    pick(1, c_l, x_all, False)
    ag(x_all, 0, 5).wait_recv()
    ag(x_all, 0, 9).start()
    ag(x_all, 0, 6).wait_recv()
    ag(x_all, 0, 10).start()
    ag(x_all, 0, 8).wait_recv()
    pick(2, c_r, x_all, False)
    rs(0, 3).wait_recv()
    add_rows(ypart, c, k * tok, cbuf.at[c], tok)
    ag(x_all, 0, 9).wait_recv()
    ag(x_all, 0, 10).wait_recv()
    pick(3, c_o, x_all, False)

    def st_fwd(e):
        return (pltpu.make_async_copy(erows.at[e], xr_hbm.at[e], st_sem.at[0, e]),
                pltpu.make_async_copy(urow.at[e], ur_hbm.at[e], st_sem.at[1, e]))

    for e in range(n_loc):
        st_fwd(e)[0].start()

    def st_hot():
        return [pltpu.make_async_copy(uhot, uh_hbm, hst_sem.at[0])] + [
            pltpu.make_async_copy(x_all.at[q], xh_hbm.at[p * two:(p + 1) * two], hst_sem.at[1 + p]) for p, q in enumerate(near)]

    @pl.loop(0, n_loc)
    def _(i):
        e = last - i
        s = lax.rem(e, 2)
        hot = jnp.logical_and(is_owner, e == 0)
        weights_here(i, e, False)

        @pl.when(i == 1)
        def _():
            ag(dy_all, 1, 0).wait_recv()
            ag(dy_all, 1, 5).start()
            ag(dy_all, 1, 2).wait_recv()
            ag(dy_all, 1, 6).start()

        @pl.when(i == 3)
        def _():
            ag(dy_all, 1, 4).wait_recv()
            ag(dy_all, 1, 1).wait_recv()
            ag(dy_all, 1, 7).start()
            ag(dy_all, 1, 3).wait_recv()
            ag(dy_all, 1, 8).start()

        @pl.when(jnp.logical_not(hot))
        def _():
            cold_forward(i, e, -1, s, cp, n_rows)
            for j, p in enumerate((3, 2, 1)):
                add_out(near[p], e, (p - 1) * cp, i == 0)

                @pl.when(i == last)
                def _():
                    rs(0, j).start()

            st_fwd(e)[1].start()

        @pl.when(hot)
        def _():
            @pl.loop(0, 3)
            def _(n):
                p = 3 - n
                hot_forward(p, jnp.where(p == 1, c_l, jnp.where(p == 2, c_r, c_o)), s, False)
                for j in range(3):
                    @pl.when(n == j)
                    def _():
                        rs(0, j).start()

            for cpy in st_hot():
                cpy.start()

    for e in range(n_loc):
        st_fwd(e)[0].wait()
    rs(0, 0).wait_recv()
    add_rows(ypart, c_o, k * tok, cbuf.at[c_o], tok)
    rs(0, 4).start()
    rs(0, 5).start()
    ag(dy_all, 1, 5).wait_recv()
    ag(dy_all, 1, 9).start()
    ag(dy_all, 1, 6).wait_recv()
    ag(dy_all, 1, 10).start()
    pick(0, c, dy_all, True)
    for j, q in ((1, c_r), (2, c_l)):
        rs(0, j).wait_recv()
        add_rows(ypart, q, k * tok, cbuf.at[q], tok)
        rs(0, 5 + j).start()
    pl.semaphore_signal(free_sem, inc=1, device_id={"ep": partner}, device_id_type=MESH)
    ag(dy_all, 1, 7).wait_recv()
    pick(1, c_l, dy_all, True)
    ag(dy_all, 1, 8).wait_recv()
    pick(2, c_r, dy_all, True)
    ag(dy_all, 1, 9).wait_recv()
    ag(dy_all, 1, 10).wait_recv()
    pick(3, c_o, dy_all, True)

    @pl.loop(0, n_loc)
    def _(e):
        @pl.when(jnp.logical_not(jnp.logical_and(is_owner, e == 0)))
        def _():
            st_fwd(e)[1].wait()

    @pl.when(is_owner)
    def _():
        for cpy in st_hot():
            cpy.wait()

    def st_d(e):
        return pltpu.make_async_copy(erows.at[e], dr_hbm.at[e], st_sem.at[0, e])

    def st_ab(e, s):
        return (pltpu.make_async_copy(darow.at[s, 0:n_rows], da_hbm.at[e], st_sem.at[1, s]),
                pltpu.make_async_copy(dbrow.at[s, 0:n_rows], db_hbm.at[e], st_sem.at[1, 2 + s]))

    for e in range(n_loc):
        st_d(e).start()

    def rs_relay_y():
        rs(0, 4).wait_recv()
        add_rows(ypart, c_r, k * tok, yra, half)
        rs(0, 8).start()
        rs(0, 5).wait_recv()
        add_rows(ypart, c_l, k * tok + half, yrb, half)
        rs(0, 9).start()

    @pl.loop(0, n_loc)
    def _(e):
        s = lax.rem(e, 2)
        hot = jnp.logical_and(is_owner, e == 0)

        weights_here(e, e, False)

        @pl.when(jnp.logical_not(hot))
        def _():
            ooff = pl.multiple_of(s * 2 * two, 64)

            def emit(cs, out):
                orow[pl.ds(ooff, n_rows), cs] = out

            backward(n_rows, erows.at[e], s, act_off(e), emit)
            load_next(e, e, 1, (0, 1, 2))

            @pl.when(e == last - 2)
            def _():
                rs_relay_y()

            @pl.when(e == 0)
            def _():
                for p in range(chips):
                    add_dx_one(near[p], p, e)

            @pl.when(e == last)
            def _():
                pl.semaphore_wait(free_sem, 1)

            @pl.when(jnp.logical_and(e > 0, s == 0))
            def _():
                for j, p in enumerate((3, 2, 1, 0)):
                    add_dx_two(near[p], p, e)

                    @pl.when(e == last)
                    def _():
                        rs(1, j).start()

        @pl.when(hot)
        def _():
            @pl.loop(0, chips // 2)
            def _(h):
                pair = (jnp.where(h == 0, c, c_r), jnp.where(h == 0, c_l, c_o))
                for n, q in enumerate(pair):
                    @pl.loop(0, two // 64)
                    def _(r):
                        at = pl.multiple_of(r * 64, 64)
                        got = dy_all[q, pl.ds(at, 64), :].astype(F32)
                        hrows[pl.ds(pl.multiple_of(n * two + r * 64, 64), 64), :] = (lane_of(q, at, 64, 8) * got).astype(BF16)

                o = pl.multiple_of(h * 2 * two, 64)
                sd = pltpu.make_async_copy(hrows, dh_hbm.at[pl.ds(o, 2 * two)], hst_sem.at[0])
                sd.start()

                def emit(cs, out):
                    for n, q in enumerate(pair):
                        dxpart[q, :, cs] = out[n * two:(n + 1) * two].astype(F32)

                backward(2 * two, hrows, s, o, emit)
                sa = pltpu.make_async_copy(darow.at[s], dah_hbm.at[pl.ds(o, 2 * two)], hst_sem.at[1])
                sb = pltpu.make_async_copy(dbrow.at[s], dbh_hbm.at[pl.ds(o, 2 * two)], hst_sem.at[2])
                sa.start()
                sb.start()
                sd.wait()
                sa.wait()
                sb.wait()

            load_next(e, e, 1, (0, 1, 2))

        @pl.when(jnp.logical_and(e >= 1, jnp.logical_not(jnp.logical_and(is_owner, e == 1))))
        def _():
            for cpy in st_ab(e - 1, 1 - s):
                cpy.wait()

        @pl.when(jnp.logical_not(hot))
        def _():
            for cpy in st_ab(e, s):
                cpy.start()

    def rs_end_y():
        for j in (6, 7, 8, 9):
            rs(0, j).wait_recv()

        @pl.loop(0, tok // 32)
        def _(r):
            o = pl.multiple_of(r * 32, 32)
            total = ypart[c, pl.ds(pl.multiple_of(k * tok + r * 32, 32), 32)] + yfl[pl.ds(o, 32)] + yfr[pl.ds(o, 32)]
            outb[pl.ds(o, 32)] = total.astype(BF16)

        return pltpu.make_async_copy(outb, y_hbm, io_sem.at[0])

    def chip_sums_out(j):
        q = (c_o, c_r, c_l, c)[j]
        lo = dxpart.at[q, pl.ds(k * tok, half)]
        hi = dxpart.at[q, pl.ds(k * tok + half, half)]
        if j == 3:
            return (pltpu.make_async_copy(dxpart.at[q, pl.ds(k * tok, tok)], sc_hbm, so_sem.at[6]),)
        to_lo, to_hi = ((go_r.at[0:half], go_l.at[0:half]), (sr_hbm, go_r.at[half:tok]), (go_l.at[half:tok], sl_hbm))[j]
        return (pltpu.make_async_copy(lo, to_lo, so_sem.at[2 * j]), pltpu.make_async_copy(hi, to_hi, so_sem.at[2 * j + 1]))

    for j, q in enumerate((c_o, c_r, c_l, c)):
        rs(1, j).wait_recv()
        add_rows(dxpart, q, k * tok, cbuf.at[q], tok)
        for cpy in chip_sums_out(j):
            cpy.start()
    y_out = rs_end_y()
    y_out.start()

    for e in range(n_loc):
        st_d(e).wait()
    for cpy in st_ab(last, last % 2):
        cpy.wait()
    for d in range(1, group):
        for cpy in meta_copies(d):
            cpy.wait_send()
    for i in range(11):
        ag(x_all, 0, i).wait_send()
        ag(dy_all, 1, i).wait_send()
    for j in range(10):
        rs(0, j).wait_send()
    for j in range(4):
        rs(1, j).wait_send()
        for cpy in chip_sums_out(j):
            cpy.wait()
    y_out.wait()


def expert_grads(x_ref, d_ref, u_ref, da_ref, db_ref, g1, g3, g2):
    g1[0] = dot_tn(x_ref[0], da_ref[0]).astype(BF16)
    g3[0] = dot_tn(x_ref[0], db_ref[0]).astype(BF16)
    g2[0] = dot_tn(u_ref[0], d_ref[0]).astype(BF16)


def first_grads_kernel(owner, x_ref, d_ref, u_ref, da_ref, db_ref, xh, dh, uh, dah, dbh, y_ref, g1, g3, g2, y_out, xb, dbuf, ub, dab, dbb, sem):
    i = pl.program_id(0)
    y_out[...] = y_ref[...]
    is_owner = lax.axis_index("ep") == owner
    hot = jnp.logical_and(is_owner, i == pl.num_programs(0) - 1)

    def copies():
        return [pltpu.make_async_copy(src, dst, sem.at[j]) for j, (src, dst) in enumerate(((xh, xb), (dah, dab), (dbh, dbb), (uh, ub), (dh, dbuf)))]

    @pl.when(jnp.logical_and(is_owner, i == 0))
    def _():
        for cpy in copies():
            cpy.start()

    @pl.when(jnp.logical_not(hot))
    def _():
        expert_grads(x_ref, d_ref, u_ref, da_ref, db_ref, g1, g3, g2)

    @pl.when(hot)
    def _():
        for cpy in copies():
            cpy.wait()
        g1[0] = dot_tn(xb[...], dab[...]).astype(BF16)
        g3[0] = dot_tn(xb[...], dbb[...]).astype(BF16)
        g2[0] = dot_tn(ub[...], dbuf[...]).astype(BF16)


def later_grads_kernel(x_ref, d_ref, u_ref, da_ref, db_ref, g1_in, g3_in, g2_in, g1, g3, g2):
    del g1_in, g3_in, g2_in
    expert_grads(x_ref, d_ref, u_ref, da_ref, db_ref, g1, g3, g2)


def solution(mesh):
    group = mesh.shape["ep"]
    num_dev = mesh.shape["dp"] * group
    tok_spec = P(("dp", "ep"), None)
    w_spec = P("ep", None, None)
    grad_spec = P(("dp", "ep"), None, None)

    def layer_fn(tokens, expert_ids, gate_vals, w_gate, w_up, w_down, grad_out):
        n_exp, width, hid = w_gate.shape
        tok = tokens.shape[0] // num_dev
        top_k = expert_ids.shape[1]
        cap = ((2 * tok * top_k + 8 * n_exp - 1) // (8 * n_exp)) * 8
        n_loc = n_exp // group
        hot = n_exp // 2
        owner = hot // n_loc
        chips = group // 2
        n_rows = chips * 2 * cap
        hot_rows = group * tok
        cfg = (chips, tok, width, hid, n_loc, cap, owner)

        def device_fn(x, ids, gates, w1, w3, w2, dy):
            any_spec = pl.BlockSpec(memory_space=pl.ANY)
            vmem_spec = pl.BlockSpec(memory_space=pltpu.VMEM)
            sds = jax.ShapeDtypeStruct
            hb = hot_rows // 2
            half = tok // 2
            act_rows = hot_rows + (n_loc - 1) * n_rows
            outs = pl.pallas_call(
                functools.partial(layer_kernel, cfg),
                out_shape=(
                    sds((tok, width), BF16), *[sds((tok, width), F32)] * 2, *[sds((half, width), F32)] * 2, sds((tok, width), F32),
                    sds((n_loc, n_rows, width), BF16), sds((n_loc, n_rows, width), BF16),
                    sds((n_loc, n_rows, hid), BF16), sds((n_loc, n_rows, hid), BF16), sds((n_loc, n_rows, hid), BF16),
                    sds((hot_rows, width), BF16), sds((hot_rows, width), BF16),
                    sds((hot_rows, hid), BF16), sds((hot_rows, hid), BF16), sds((hot_rows, hid), BF16)),
                in_specs=[any_spec, any_spec, vmem_spec, vmem_spec, any_spec, any_spec, any_spec],
                out_specs=[any_spec] * 16,
                scratch_shapes=[
                    pltpu.VMEM((chips, 2 * tok, width), BF16), pltpu.VMEM((chips, 2 * tok, width), BF16),
                    pltpu.VMEM((group, top_k, tok), jnp.int32), pltpu.VMEM((group, top_k, tok), F32),
                    pltpu.VMEM((chips, 8, 2 * tok), F32), pltpu.VMEM((chips, 8, 2 * tok), F32),
                    pltpu.VMEM((chips, 2 * tok, 128), F32),
                    pltpu.VMEM((chips, 2 * tok, width), F32), pltpu.VMEM((chips, 2 * tok, width), F32),
                    pltpu.VMEM((chips, tok, width), F32),
                    pltpu.VMEM((half, width), F32), pltpu.VMEM((half, width), F32),
                    pltpu.VMEM((tok, width), F32), pltpu.VMEM((tok, width), F32),
                    pltpu.VMEM((n_loc, n_rows, width), BF16), pltpu.VMEM((hb, width), BF16),
                    pltpu.VMEM((n_loc, n_rows, hid), BF16), pltpu.VMEM((hot_rows, hid), BF16),
                    pltpu.VMEM((2, hb, hid), BF16), pltpu.VMEM((2, hb, hid), BF16),
                    pltpu.VMEM((act_rows, hid), F32), pltpu.VMEM((act_rows, hid), F32),
                    pltpu.VMEM((hb + n_rows, width), BF16), pltpu.VMEM((n_loc * 2 * cap, 2 * tok), BF16),
                    pltpu.VMEM((2, width, hid), BF16), pltpu.VMEM((2, width, hid), BF16), pltpu.VMEM((2, hid, width), BF16),
                    pltpu.VMEM((tok, width), BF16),
                    pltpu.SemaphoreType.DMA((2, group)), pltpu.SemaphoreType.DMA((2, group)),
                    pltpu.SemaphoreType.DMA((2, 11)), pltpu.SemaphoreType.DMA((2, 11)),
                    pltpu.SemaphoreType.DMA((2, 10)), pltpu.SemaphoreType.DMA((2, 10)),
                    pltpu.SemaphoreType.DMA((3, 2)), pltpu.SemaphoreType.DMA((2, n_loc)), pltpu.SemaphoreType.DMA((5,)),
                    pltpu.SemaphoreType.DMA((2,)), pltpu.SemaphoreType.DMA((7,)), pltpu.SemaphoreType.REGULAR,
                ],
                compiler_params=pltpu.CompilerParams(collective_id=0, has_side_effects=True, vmem_limit_bytes=67043328),
                name="moe_layer",
            )(x, dy, ids.T, gates.T, w1, w3, w2)
            y, go_r, go_l, sr, sl, sc, xr, dr, ur, dar, dbr, xh, dh, uh, dah, dbh = outs

            to_right = [(i, (i + 2) % group) for i in range(group)]
            to_left = [(i, (i + group - 2) % group) for i in range(group)]
            from_l = lax.ppermute(go_r, "ep", to_right)
            from_r = lax.ppermute(go_l, "ep", to_left)

            n_first = (n_loc + 1) // 2
            g_shapes = (sds((n_loc, width, hid), BF16), sds((n_loc, width, hid), BF16), sds((n_loc, hid, width), BF16))

            def blk(r, n, at):
                return pl.BlockSpec((1, r, n), lambda i: (at(i), 0, 0))

            def row_specs(at):
                return [blk(n_rows, width, at), blk(n_rows, width, at), blk(n_rows, hid, at), blk(n_rows, hid, at), blk(n_rows, hid, at)]

            def out_blks(at):
                return [blk(width, hid, at), blk(width, hid, at), blk(hid, width, at)]

            def cost(n):
                return pl.CostEstimate(flops=n * 6 * n_rows * width * hid, transcendentals=0,
                                       bytes_accessed=n * 2 * (2 * n_rows * width + 3 * n_rows * hid + 3 * width * hid))

            def first_at(i):
                return lax.rem(i + 1, n_first)

            def later_at(i):
                return i + n_first

            y_spec = pl.BlockSpec((tok, width), lambda i: (0, 0))
            *grads, y = pl.pallas_call(
                functools.partial(first_grads_kernel, owner),
                grid=(n_first,), out_shape=g_shapes + (sds((tok, width), BF16),),
                in_specs=row_specs(first_at) + [any_spec] * 5 + [y_spec], out_specs=out_blks(first_at) + [y_spec],
                scratch_shapes=[pltpu.VMEM((hot_rows, width), BF16), pltpu.VMEM((hot_rows, width), BF16), pltpu.VMEM((hot_rows, hid), BF16),
                                pltpu.VMEM((hot_rows, hid), BF16), pltpu.VMEM((hot_rows, hid), BF16), pltpu.SemaphoreType.DMA((5,))],
                compiler_params=pltpu.CompilerParams(vmem_limit_bytes=60 << 20),
                cost_estimate=cost(n_first), name="first_grads",
            )(xr, dr, ur, dar, dbr, xh, dh, uh, dah, dbh, y)

            fl_lo = lax.ppermute(sr + from_l[:half], "ep", to_right)
            fr_hi = lax.ppermute(sl + from_r[:half], "ep", to_left)
            g1, g3, g2 = pl.pallas_call(
                later_grads_kernel,
                grid=(n_loc - n_first,), out_shape=g_shapes,
                in_specs=row_specs(later_at) + [any_spec] * 3, out_specs=out_blks(later_at),
                input_output_aliases={5: 0, 6: 1, 7: 2},
                compiler_params=pltpu.CompilerParams(vmem_limit_bytes=60 << 20),
                cost_estimate=cost(n_loc - n_first), name="later_grads",
            )(xr, dr, ur, dar, dbr, *grads)
            fl = jnp.concatenate([fl_lo, from_l[half:]], axis=0)
            fr = jnp.concatenate([from_r[half:], fr_hi], axis=0)
            dx = (sc + fl + fr).astype(BF16)
            return y, dx, g1, g3, g2

        return jax.shard_map(device_fn, mesh=mesh, in_specs=(tok_spec, tok_spec, tok_spec, w_spec, w_spec, w_spec, tok_spec),
                             out_specs=(tok_spec, tok_spec, grad_spec, grad_spec, grad_spec), check_vma=False)(
            tokens, expert_ids, gate_vals, w_gate, w_up, w_down, grad_out)

    return layer_fn
```

```python
import functools

import jax
import jax.numpy as jnp
from jax import lax
from jax.experimental import pallas as pl
from jax.experimental.pallas import tpu as pltpu
from jax.sharding import PartitionSpec as P

MESH = pl.DeviceIdType.MESH
F32 = jnp.float32
BF16 = jnp.bfloat16


def dot_nn(a, b):
    return lax.dot_general(a, b, (((1,), (0,)), ((), ())), preferred_element_type=F32)


def dot_nt(a, b):
    return lax.dot_general(a, b, (((1,), (1,)), ((), ())), preferred_element_type=F32)


def dot_tn(a, b):
    return lax.dot_general(a, b, (((0,), (0,)), ((), ())), preferred_element_type=F32)


def layer_kernel(cfg, x_hbm, dy_hbm, ids_ref, gates_ref, w1_hbm, w3_hbm, w2_hbm,
                 y_hbm, go_r, go_l, sr_hbm, sl_hbm, sc_hbm, xr_hbm, dr_hbm, ur_hbm, da_hbm, db_hbm, xh_hbm, dh_hbm, uh_hbm, dah_hbm, dbh_hbm,
                 x_all, dy_all, ids_all, gates_all, rt, gt, mc, ypart, dxpart, cbuf, yra, yrb, yfl, yfr,
                 erows, hrows, urow, uhot, darow, dbrow, act1, act2, orow, pbuf, w1, w3, w2, outb,
                 m_send, m_recv, ag_send, ag_recv, rs_send, rs_recv, w_sem, st_sem, hst_sem, io_sem, so_sem, free_sem):
    chips, tok, width, hid, n_loc, cap, owner = cfg
    group = 2 * chips
    two = 2 * tok
    cp = 2 * cap
    n_rows = chips * cp
    hot_rows = chips * two
    half = tok // 2
    last = n_loc - 1
    me = lax.axis_index("ep")
    c = me // 2
    k = lax.rem(me, 2)
    c_r = lax.rem(c + 1, chips)
    c_l = lax.rem(c + chips - 1, chips)
    c_o = lax.rem(c + 2, chips)
    near = (c, c_l, c_r, c_o)
    right = 2 * c_r + k
    left = 2 * c_l + k
    partner = 2 * c + 1 - k
    is_owner = me == owner

    own_x = pltpu.make_async_copy(x_hbm, x_all.at[c, pl.ds(k * tok, tok)], io_sem.at[0])
    own_dy = pltpu.make_async_copy(dy_hbm, dy_all.at[c, pl.ds(k * tok, tok)], io_sem.at[1])
    own_x.start()
    own_dy.start()

    def w_copies(e):
        s = lax.rem(e, 2)
        return (pltpu.make_async_copy(w1_hbm.at[e], w1.at[s], w_sem.at[0, s]),
                pltpu.make_async_copy(w3_hbm.at[e], w3.at[s], w_sem.at[1, s]),
                pltpu.make_async_copy(w2_hbm.at[e], w2.at[s], w_sem.at[2, s]))

    for e in (0, 1):
        for cpy in w_copies(e):
            cpy.start()
    ids_all[me] = ids_ref[...]
    gates_all[me] = gates_ref[...]

    barrier = pltpu.get_barrier_semaphore()
    for d in range(1, group):
        pl.semaphore_signal(barrier, inc=1, device_id={"ep": lax.rem(me + d, group)}, device_id_type=MESH)
    pl.semaphore_wait(barrier, group - 1)

    def meta_copies(d):
        return tuple(pltpu.make_async_remote_copy(
            src_ref=src, dst_ref=dst.at[me], send_sem=m_send.at[i, d], recv_sem=m_recv.at[i, d],
            device_id={"ep": lax.rem(me + d, group)}, device_id_type=MESH)
            for i, (src, dst) in enumerate(((ids_ref, ids_all), (gates_ref, gates_all))))

    def ag(ref, t, i):
        chip, core, r0, n, dev = (
            (c, k, 0, half, right), (c, k, half, half, right), (c, k, half, half, left), (c, k, 0, half, left),
            (c, k, 0, tok, partner),
            (c_l, k, 0, half, right), (c_r, k, half, half, left),
            (c_l, k, 0, tok, partner), (c_r, k, 0, tok, partner),
            (c_o, k, 0, half, partner), (c_o, k, half, half, partner))[i]
        blk = ref.at[chip, pl.ds(core * tok + r0, n)]
        return pltpu.make_async_remote_copy(
            src_ref=blk, dst_ref=blk, send_sem=ag_send.at[t, i], recv_sem=ag_recv.at[t, i],
            device_id={"ep": dev}, device_id_type=MESH)

    own_x.wait()
    for d in range(1, group):
        for cpy in meta_copies(d):
            cpy.start()
    for i in (4, 0, 2, 1, 3):
        ag(x_all, 0, i).start()
    own_dy.wait()

    for d in range(1, group):
        for cpy in meta_copies(d):
            cpy.wait_recv()

    upper = (lax.broadcasted_iota(jnp.int32, (tok, tok), 0) < lax.broadcasted_iota(jnp.int32, (tok, tok), 1)).astype(F32).astype(BF16)
    row_id = lax.broadcasted_iota(jnp.int32, (8, tok), 0)
    for s in range(group):
        q, core = s // 2, s % 2
        ids = ids_all[s]
        gates = gates_all[s]
        mask_m = jnp.zeros((8, tok), F32)
        gate_m = jnp.zeros((8, tok), F32)
        for le in range(n_loc):
            eq = ids == me * n_loc + le
            hit = jnp.sum(jnp.where(eq, 1.0, 0.0), axis=0, keepdims=True)
            gv = jnp.sum(jnp.where(eq, gates, 0.0), axis=0, keepdims=True)
            mask_m = jnp.where(row_id == le, hit, mask_m)
            gate_m = jnp.where(row_id == le, gv, gate_m)
        rank = dot_nn(mask_m.astype(BF16), upper)
        pos = jnp.where(mask_m > 0.0, rank + float(cap * core), -1.0)
        rt[q, :, core * tok:(core + 1) * tok] = pos
        gt[q, :, core * tok:(core + 1) * tok] = gate_m
        both = jnp.concatenate([pos, gate_m, jnp.zeros((tok - 16, tok), F32)], axis=0)
        mc[q, core * tok:(core + 1) * tok, :] = jnp.transpose(both)

    def pick(p, q, src, scaled):
        for e in range(n_loc):
            hit = rt[q, e:e + 1, :] == lax.broadcasted_iota(jnp.int32, (cp, two), 0).astype(F32)
            pbuf[e * cp:(e + 1) * cp, :] = jnp.where(hit, 1.0, 0.0).astype(BF16)
        gates = [None] * n_loc
        if scaled:
            for e in range(n_loc):
                hit = rt[q, e:e + 1, :] == lax.broadcasted_iota(jnp.int32, (cp, two), 0).astype(F32)
                gates[e] = jnp.sum(jnp.where(hit, gt[q, e:e + 1, :], 0.0), axis=1, keepdims=True)
        for j in range(width // 256):
            cs = slice(j * 256, (j + 1) * 256)
            got = dot_nn(pbuf[...], src[q, :, cs])
            for e in range(n_loc):
                part = got[e * cp:(e + 1) * cp]
                erows[e, pl.ds(p * cp, cp), cs] = (gates[e] * part if scaled else part).astype(BF16)

    def column(q, lane):
        return jnp.sum(jnp.where(lax.broadcasted_iota(jnp.int32, (two, 128), 1) == lane, mc[q], 0.0), axis=1, keepdims=True)

    def put_rows(q, e):
        hit = column(q, e) == lax.broadcasted_iota(jnp.int32, (two, cp), 1).astype(F32)
        return jnp.where(hit, 1.0, 0.0).astype(BF16)

    def forward(m, src, dst, s, aoff, on, emit, used):
        for j in range(hid // 256):
            cs = slice(j * 256, (j + 1) * 256)
            a = dot_nn(src[...], w1[s, :, cs])
            b = dot_nn(src[...], w3[s, :, cs])
            sg = jax.nn.sigmoid(a)
            ga = a * sg
            fa = b * (sg * (1.0 + a * (1.0 - sg)))
            u = ga * b
            if on is not None:
                fa, ga, u = jnp.where(on, fa, 0.0), jnp.where(on, ga, 0.0), jnp.where(on, u, 0.0)
            act1[pl.ds(aoff, m), cs] = fa
            act2[pl.ds(aoff, m), cs] = ga
            dst[:, cs] = u.astype(BF16)

        used(0)
        for j in range(width // 256):
            cs = slice(j * 256, (j + 1) * 256)
            emit(cs, dot_nn(dst[...], w2[s, :, cs]).astype(BF16))

    all_tiles = range(width // 256)

    def backward_du(m, src, s, aoff, ab=None):
        ab = s if ab is None else ab
        for j in range(hid // 256):
            cs = slice(j * 256, (j + 1) * 256)
            du = dot_nt(src[...], w2[s, cs, :])
            darow[ab, 0:m, cs] = (du * act1[pl.ds(aoff, m), cs]).astype(BF16)
            dbrow[ab, 0:m, cs] = (du * act2[pl.ds(aoff, m), cs]).astype(BF16)
    def backward_dx(m, s, tiles, emit, ab=None):
        ab = s if ab is None else ab
        for j in tiles:
            cs = slice(j * 256, (j + 1) * 256)
            emit(cs, (dot_nt(darow[ab, 0:m, :], w1[s, cs, :]) + dot_nt(dbrow[ab, 0:m, :], w3[s, cs, :])).astype(BF16))

    def act_off(e):
        return pl.multiple_of(jnp.where(e == 0, 0, hot_rows + (e - 1) * n_rows), 64)

    def add_out(q, e, first, fresh):
        gate = column(q, e + 8)
        put = put_rows(q, e)
        for j in range(width // 256):
            cs = slice(j * 256, (j + 1) * 256)
            ypart[q, :, cs] = jnp.where(fresh, 0.0, ypart[q, :, cs]) + gate * dot_nn(put, orow[first:first + cp, cs])

    def add_dx_one(q, p, e):
        put = put_rows(q, e)
        for j in range(width // 256):
            cs = slice(j * 256, (j + 1) * 256)
            dxpart[q, :, cs] = dot_nn(put, orow[p * cp:(p + 1) * cp, cs])

    def add_dx_two(q, p, e, tiles):
        now, before = column(q, e), column(q, e - 1)
        now = jnp.where(now >= 0.0, now + float(cp), -1.0)
        lane = lax.broadcasted_iota(jnp.int32, (two, 2 * cp), 1).astype(F32)
        put = jnp.where(jnp.logical_or(before == lane, now == lane), 1.0, 0.0).astype(BF16)
        for j in tiles:
            cs = slice(j * 256, (j + 1) * 256)
            both = jnp.concatenate([orow[2 * two + p * cp:2 * two + (p + 1) * cp, cs], orow[p * cp:(p + 1) * cp, cs]], axis=0)
            dxpart[q, :, cs] += dot_nn(put, both)

    def lane_of(q, r, n, lane):
        m = mc[q, pl.ds(r, n), :]
        return jnp.sum(jnp.where(lax.broadcasted_iota(jnp.int32, (n, 128), 1) == lane, m, 0.0), axis=1, keepdims=True)

    def hot_forward(p, q, s, fresh):
        o = pl.multiple_of(p * two, 64)
        gate = column(q, 8)

        def emit(cs, out):
            ypart[q, :, cs] = jnp.where(fresh, 0.0, ypart[q, :, cs]) + gate * out.astype(F32)

        forward(two, x_all.at[q], uhot.at[pl.ds(o, two)], s, o, column(q, 0) >= 0.0, emit, lambda part: None)

    def load_next(i, e, step, parts):
        @pl.when(i < last - 1)
        def _():
            for n in parts:
                w_copies(e + 2 * step)[n].start()

    def cold_forward(i, e, step, s, r0, r1):
        def emit(cs, out):
            orow[0:r1 - r0, cs] = out

        forward(r1 - r0, erows.at[e, r0:r1], urow.at[e, r0:r1], s, pl.multiple_of(act_off(e) + r0, 16), None, emit,
                lambda part: load_next(i, e, step, (0, 1)))
        load_next(i, e, step, (2,))

    def weights_here(i, e, first):
        @pl.when(i >= (0 if first else 2))
        def _():
            for cpy in w_copies(e):
                cpy.wait()

    def rs(t, j):
        part = (ypart, dxpart)[t]
        o = k * tok
        if j < 4:
            q = (c_o, c_r, c_l, c)[j]
            src, dst, dev = part.at[q, pl.ds((1 - k) * tok, tok)], cbuf.at[q], partner
            if t == 1:
                src, dst = part.at[q, pl.ds((1 - k) * tok, tok), 0:width // 2], cbuf.at[q, :, 0:width // 2]
        elif j >= 10:
            q = (c_o, c_r, c_l, c)[j - 10]
            src, dst, dev = part.at[q, pl.ds((1 - k) * tok, tok), width // 2:width], cbuf.at[q, :, width // 2:width], partner
        else:
            src, dst, dev = (
                (part.at[c_o, pl.ds(o, half)], yra, right),
                (part.at[c_o, pl.ds(o + half, half)], yrb, left),
                (part.at[c_r, pl.ds(o + half, half)], yfl.at[half:tok], right),
                (part.at[c_l, pl.ds(o, half)], yfr.at[0:half], left),
                (part.at[c_r, pl.ds(o, half)], yfl.at[0:half], right),
                (part.at[c_l, pl.ds(o + half, half)], yfr.at[half:tok], left))[j - 4]
        return pltpu.make_async_remote_copy(
            src_ref=src, dst_ref=dst, send_sem=rs_send.at[t, j], recv_sem=rs_recv.at[t, j],
            device_id={"ep": dev}, device_id_type=MESH)

    def add_rows(part, q, off, src, n):
        @pl.loop(0, n // 32)
        def _(r):
            o = pl.multiple_of(r * 32, 32)
            part[q, pl.ds(pl.multiple_of(off + r * 32, 32), 32)] += src[pl.ds(o, 32)]

    ag(x_all, 0, 4).wait_recv()
    pick(0, c, x_all, False)

    @pl.loop(0, n_loc)
    def _(e):
        s = lax.rem(e, 2)
        hot = jnp.logical_and(is_owner, e == 0)
        weights_here(e, e, True)

        @pl.when(e == 2)
        def _():
            ag(x_all, 0, 0).wait_recv()
            ag(x_all, 0, 5).start()
            ag(x_all, 0, 2).wait_recv()
            ag(x_all, 0, 6).start()
            for n in (4, 0, 2, 1, 3):
                ag(dy_all, 1, n).start()

        @pl.when(jnp.logical_not(hot))
        def _():
            cold_forward(e, e, 1, s, 0, cp)
            add_out(c, e, 0, e == 0)

        @pl.when(hot)
        def _():
            hot_forward(0, c, s, True)
            load_next(e, e, 1, (0, 1, 2))

    ag(x_all, 0, 1).wait_recv()
    ag(x_all, 0, 7).start()
    ag(x_all, 0, 3).wait_recv()
    ag(x_all, 0, 8).start()
    rs(0, 3).start()
    ag(x_all, 0, 7).wait_recv()
    pick(1, c_l, x_all, False)
    ag(x_all, 0, 5).wait_recv()
    ag(x_all, 0, 9).start()
    ag(x_all, 0, 6).wait_recv()
    ag(x_all, 0, 10).start()
    ag(x_all, 0, 8).wait_recv()
    pick(2, c_r, x_all, False)
    rs(0, 3).wait_recv()
    add_rows(ypart, c, k * tok, cbuf.at[c], tok)
    ag(x_all, 0, 9).wait_recv()
    ag(x_all, 0, 10).wait_recv()
    pick(3, c_o, x_all, False)

    def st_fwd(e):
        return (pltpu.make_async_copy(erows.at[e], xr_hbm.at[e], st_sem.at[0, e]),
                pltpu.make_async_copy(urow.at[e], ur_hbm.at[e], st_sem.at[1, e]))

    for e in range(n_loc):
        st_fwd(e)[0].start()

    def st_hot():
        return [pltpu.make_async_copy(uhot, uh_hbm, hst_sem.at[0])] + [
            pltpu.make_async_copy(x_all.at[q], xh_hbm.at[p * two:(p + 1) * two], hst_sem.at[1 + p]) for p, q in enumerate(near)]

    @pl.loop(0, n_loc)
    def _(i):
        e = last - i
        s = lax.rem(e, 2)
        hot = jnp.logical_and(is_owner, e == 0)
        weights_here(i, e, False)

        @pl.when(i == 1)
        def _():
            ag(dy_all, 1, 0).wait_recv()
            ag(dy_all, 1, 5).start()
            ag(dy_all, 1, 2).wait_recv()
            ag(dy_all, 1, 6).start()

        @pl.when(i == 3)
        def _():
            ag(dy_all, 1, 4).wait_recv()
            ag(dy_all, 1, 1).wait_recv()
            ag(dy_all, 1, 7).start()
            ag(dy_all, 1, 3).wait_recv()
            ag(dy_all, 1, 8).start()

        @pl.when(jnp.logical_not(hot))
        def _():
            cold_forward(i, e, -1, s, cp, n_rows)
            for j, p in enumerate((3, 2, 1)):
                add_out(near[p], e, (p - 1) * cp, i == 0)

                @pl.when(i == last)
                def _():
                    rs(0, j).start()

            st_fwd(e)[1].start()

        @pl.when(hot)
        def _():
            @pl.loop(0, 3)
            def _(n):
                p = 3 - n
                hot_forward(p, jnp.where(p == 1, c_l, jnp.where(p == 2, c_r, c_o)), s, False)
                for j in range(3):
                    @pl.when(n == j)
                    def _():
                        rs(0, j).start()

            for cpy in st_hot():
                cpy.start()

    for e in range(n_loc):
        st_fwd(e)[0].wait()
    rs(0, 0).wait_recv()
    add_rows(ypart, c_o, k * tok, cbuf.at[c_o], tok)
    rs(0, 4).start()
    rs(0, 5).start()
    ag(dy_all, 1, 5).wait_recv()
    ag(dy_all, 1, 9).start()
    ag(dy_all, 1, 6).wait_recv()
    ag(dy_all, 1, 10).start()
    pick(0, c, dy_all, True)
    for j, q in ((1, c_r), (2, c_l)):
        rs(0, j).wait_recv()
        add_rows(ypart, q, k * tok, cbuf.at[q], tok)
        rs(0, 5 + j).start()
    pl.semaphore_signal(free_sem, inc=1, device_id={"ep": partner}, device_id_type=MESH)
    ag(dy_all, 1, 7).wait_recv()
    pick(1, c_l, dy_all, True)
    ag(dy_all, 1, 8).wait_recv()
    pick(2, c_r, dy_all, True)
    ag(dy_all, 1, 9).wait_recv()
    ag(dy_all, 1, 10).wait_recv()
    pick(3, c_o, dy_all, True)

    @pl.loop(0, n_loc)
    def _(e):
        @pl.when(jnp.logical_not(jnp.logical_and(is_owner, e == 0)))
        def _():
            st_fwd(e)[1].wait()

    @pl.when(is_owner)
    def _():
        for cpy in st_hot():
            cpy.wait()

    def st_d(e):
        return pltpu.make_async_copy(erows.at[e], dr_hbm.at[e], st_sem.at[0, e])

    def st_ab(e, s):
        return (pltpu.make_async_copy(darow.at[s, 0:n_rows], da_hbm.at[e], st_sem.at[1, s]),
                pltpu.make_async_copy(dbrow.at[s, 0:n_rows], db_hbm.at[e], st_sem.at[1, 2 + s]))

    for e in range(n_loc):
        st_d(e).start()

    def st_hot_ab(h):
        at = pl.multiple_of(h * 2 * two, 64)
        return (pltpu.make_async_copy(darow.at[h], dah_hbm.at[pl.ds(at, 2 * two)], hst_sem.at[1 + h]),
                pltpu.make_async_copy(dbrow.at[h], dbh_hbm.at[pl.ds(at, 2 * two)], hst_sem.at[3 + h]))

    def rs_relay_y():
        rs(0, 4).wait_recv()
        add_rows(ypart, c_r, k * tok, yra, half)
        rs(0, 8).start()
        rs(0, 5).wait_recv()
        add_rows(ypart, c_l, k * tok + half, yrb, half)
        rs(0, 9).start()

    @pl.loop(0, n_loc)
    def _(e):
        s = lax.rem(e, 2)
        hot = jnp.logical_and(is_owner, e == 0)

        weights_here(e, e, False)

        @pl.when(jnp.logical_and(is_owner, e == 1))
        def _():
            for h in range(2):
                for cpy in st_hot_ab(h):
                    cpy.wait()

        @pl.when(jnp.logical_not(hot))
        def _():
            ooff = pl.multiple_of(s * 2 * two, 64)

            def emit(cs, out):
                orow[pl.ds(ooff, n_rows), cs] = out

            backward_du(n_rows, erows.at[e], s, act_off(e))

            @pl.when(e < last)
            def _():
                backward_dx(n_rows, s, all_tiles, emit)
                load_next(e, e, 1, (0, 1, 2))

                @pl.when(e == last - 2)
                def _():
                    rs_relay_y()

                @pl.when(e == 0)
                def _():
                    for p in range(chips):
                        add_dx_one(near[p], p, e)

                @pl.when(jnp.logical_and(e > 0, s == 0))
                def _():
                    for p in (3, 2, 1, 0):
                        add_dx_two(near[p], p, e, all_tiles)

            @pl.when(e == last)
            def _():
                for h in range(2):
                    tiles = all_tiles[h * len(all_tiles) // 2:(h + 1) * len(all_tiles) // 2]
                    backward_dx(n_rows, s, tiles, emit)
                    if h == 0:
                        pl.semaphore_wait(free_sem, 1)
                    for j, p in enumerate((3, 2, 1, 0)):
                        add_dx_two(near[p], p, e, tiles)
                        rs(1, j + 10 * h).start()

        @pl.when(hot)
        def _():
            @pl.loop(0, chips // 2)
            def _(h):
                pair = (jnp.where(h == 0, c, c_r), jnp.where(h == 0, c_l, c_o))
                for n, q in enumerate(pair):
                    @pl.loop(0, two // 64)
                    def _(r):
                        at = pl.multiple_of(r * 64, 64)
                        got = dy_all[q, pl.ds(at, 64), :].astype(F32)
                        hrows[pl.ds(pl.multiple_of(n * two + r * 64, 64), 64), :] = (lane_of(q, at, 64, 8) * got).astype(BF16)

                o = pl.multiple_of(h * 2 * two, 64)
                sd = pltpu.make_async_copy(hrows, dh_hbm.at[pl.ds(o, 2 * two)], hst_sem.at[0])
                sd.start()

                def emit(cs, out):
                    for n, q in enumerate(pair):
                        dxpart[q, :, cs] = out[n * two:(n + 1) * two].astype(F32)

                backward_du(2 * two, hrows, s, o, h)
                backward_dx(2 * two, s, all_tiles, emit, h)
                for cpy in st_hot_ab(h):
                    cpy.start()
                sd.wait()

            load_next(e, e, 1, (0, 1, 2))

        @pl.when(jnp.logical_and(e >= 1, jnp.logical_not(jnp.logical_and(is_owner, e == 1))))
        def _():
            for cpy in st_ab(e - 1, 1 - s):
                cpy.wait()

        @pl.when(jnp.logical_not(hot))
        def _():
            for cpy in st_ab(e, s):
                cpy.start()

    def rs_end_y():
        for j in (6, 7, 8, 9):
            rs(0, j).wait_recv()

        @pl.loop(0, tok // 32)
        def _(r):
            o = pl.multiple_of(r * 32, 32)
            total = ypart[c, pl.ds(pl.multiple_of(k * tok + r * 32, 32), 32)] + yfl[pl.ds(o, 32)] + yfr[pl.ds(o, 32)]
            outb[pl.ds(o, 32)] = total.astype(BF16)

        return pltpu.make_async_copy(outb, y_hbm, io_sem.at[0])

    def chip_sums_out(j):
        q = (c_o, c_r, c_l, c)[j]
        lo = dxpart.at[q, pl.ds(k * tok, half)]
        hi = dxpart.at[q, pl.ds(k * tok + half, half)]
        if j == 3:
            return (pltpu.make_async_copy(dxpart.at[q, pl.ds(k * tok, tok)], sc_hbm, so_sem.at[6]),)
        to_lo, to_hi = ((go_r.at[0:half], go_l.at[0:half]), (sr_hbm, go_r.at[half:tok]), (go_l.at[half:tok], sl_hbm))[j]
        return (pltpu.make_async_copy(lo, to_lo, so_sem.at[2 * j]), pltpu.make_async_copy(hi, to_hi, so_sem.at[2 * j + 1]))

    for j, q in enumerate((c_o, c_r, c_l, c)):
        rs(1, j).wait_recv()
        rs(1, j + 10).wait_recv()
        add_rows(dxpart, q, k * tok, cbuf.at[q], tok)
        for cpy in chip_sums_out(j):
            cpy.start()
    y_out = rs_end_y()
    y_out.start()

    for e in range(n_loc):
        st_d(e).wait()
    for cpy in st_ab(last, last % 2):
        cpy.wait()
    for d in range(1, group):
        for cpy in meta_copies(d):
            cpy.wait_send()
    for i in range(11):
        ag(x_all, 0, i).wait_send()
        ag(dy_all, 1, i).wait_send()
    for j in range(10):
        rs(0, j).wait_send()
    for j in range(4):
        rs(1, j).wait_send()
        rs(1, j + 10).wait_send()
        for cpy in chip_sums_out(j):
            cpy.wait()
    y_out.wait()


def expert_grads(x_ref, d_ref, u_ref, da_ref, db_ref, g1, g3, g2):
    g1[0] = dot_tn(x_ref[0], da_ref[0]).astype(BF16)
    g3[0] = dot_tn(x_ref[0], db_ref[0]).astype(BF16)
    g2[0] = dot_tn(u_ref[0], d_ref[0]).astype(BF16)


def first_grads_kernel(owner, x_ref, d_ref, u_ref, da_ref, db_ref, xh, dh, uh, dah, dbh, y_ref, g1, g3, g2, y_out, xb, dbuf, ub, dab, dbb, sem):
    i = pl.program_id(0)
    y_out[...] = y_ref[...]
    is_owner = lax.axis_index("ep") == owner
    hot = jnp.logical_and(is_owner, i == pl.num_programs(0) - 1)

    def copies():
        return [pltpu.make_async_copy(src, dst, sem.at[j]) for j, (src, dst) in enumerate(((xh, xb), (dah, dab), (dbh, dbb), (uh, ub), (dh, dbuf)))]

    @pl.when(jnp.logical_and(is_owner, i == 0))
    def _():
        for cpy in copies():
            cpy.start()

    @pl.when(jnp.logical_not(hot))
    def _():
        expert_grads(x_ref, d_ref, u_ref, da_ref, db_ref, g1, g3, g2)

    @pl.when(hot)
    def _():
        for cpy in copies():
            cpy.wait()
        g1[0] = dot_tn(xb[...], dab[...]).astype(BF16)
        g3[0] = dot_tn(xb[...], dbb[...]).astype(BF16)
        g2[0] = dot_tn(ub[...], dbuf[...]).astype(BF16)


def later_grads_kernel(x_ref, d_ref, u_ref, da_ref, db_ref, g1_in, g3_in, g2_in, g1, g3, g2):
    del g1_in, g3_in, g2_in
    expert_grads(x_ref, d_ref, u_ref, da_ref, db_ref, g1, g3, g2)


def solution(mesh):
    group = mesh.shape["ep"]
    num_dev = mesh.shape["dp"] * group
    tok_spec = P(("dp", "ep"), None)
    w_spec = P("ep", None, None)
    grad_spec = P(("dp", "ep"), None, None)

    def layer_fn(tokens, expert_ids, gate_vals, w_gate, w_up, w_down, grad_out):
        n_exp, width, hid = w_gate.shape
        tok = tokens.shape[0] // num_dev
        top_k = expert_ids.shape[1]
        cap = ((2 * tok * top_k + 8 * n_exp - 1) // (8 * n_exp)) * 8
        n_loc = n_exp // group
        hot = n_exp // 2
        owner = hot // n_loc
        chips = group // 2
        n_rows = chips * 2 * cap
        hot_rows = group * tok
        cfg = (chips, tok, width, hid, n_loc, cap, owner)

        def device_fn(x, ids, gates, w1, w3, w2, dy):
            any_spec = pl.BlockSpec(memory_space=pl.ANY)
            vmem_spec = pl.BlockSpec(memory_space=pltpu.VMEM)
            sds = jax.ShapeDtypeStruct
            hb = hot_rows // 2
            half = tok // 2
            act_rows = hot_rows + (n_loc - 1) * n_rows
            outs = pl.pallas_call(
                functools.partial(layer_kernel, cfg),
                out_shape=(
                    sds((tok, width), BF16), *[sds((tok, width), F32)] * 2, *[sds((half, width), F32)] * 2, sds((tok, width), F32),
                    sds((n_loc, n_rows, width), BF16), sds((n_loc, n_rows, width), BF16),
                    sds((n_loc, n_rows, hid), BF16), sds((n_loc, n_rows, hid), BF16), sds((n_loc, n_rows, hid), BF16),
                    sds((hot_rows, width), BF16), sds((hot_rows, width), BF16),
                    sds((hot_rows, hid), BF16), sds((hot_rows, hid), BF16), sds((hot_rows, hid), BF16)),
                in_specs=[any_spec, any_spec, vmem_spec, vmem_spec, any_spec, any_spec, any_spec],
                out_specs=[any_spec] * 16,
                scratch_shapes=[
                    pltpu.VMEM((chips, 2 * tok, width), BF16), pltpu.VMEM((chips, 2 * tok, width), BF16),
                    pltpu.VMEM((group, top_k, tok), jnp.int32), pltpu.VMEM((group, top_k, tok), F32),
                    pltpu.VMEM((chips, 8, 2 * tok), F32), pltpu.VMEM((chips, 8, 2 * tok), F32),
                    pltpu.VMEM((chips, 2 * tok, 128), F32),
                    pltpu.VMEM((chips, 2 * tok, width), F32), pltpu.VMEM((chips, 2 * tok, width), F32),
                    pltpu.VMEM((chips, tok, width), F32),
                    pltpu.VMEM((half, width), F32), pltpu.VMEM((half, width), F32),
                    pltpu.VMEM((tok, width), F32), pltpu.VMEM((tok, width), F32),
                    pltpu.VMEM((n_loc, n_rows, width), BF16), pltpu.VMEM((hb, width), BF16),
                    pltpu.VMEM((n_loc, n_rows, hid), BF16), pltpu.VMEM((hot_rows, hid), BF16),
                    pltpu.VMEM((2, hb, hid), BF16), pltpu.VMEM((2, hb, hid), BF16),
                    pltpu.VMEM((act_rows, hid), F32), pltpu.VMEM((act_rows, hid), F32),
                    pltpu.VMEM((hb + n_rows, width), BF16), pltpu.VMEM((n_loc * 2 * cap, 2 * tok), BF16),
                    pltpu.VMEM((2, width, hid), BF16), pltpu.VMEM((2, width, hid), BF16), pltpu.VMEM((2, hid, width), BF16),
                    pltpu.VMEM((tok, width), BF16),
                    pltpu.SemaphoreType.DMA((2, group)), pltpu.SemaphoreType.DMA((2, group)),
                    pltpu.SemaphoreType.DMA((2, 11)), pltpu.SemaphoreType.DMA((2, 11)),
                    pltpu.SemaphoreType.DMA((2, 14)), pltpu.SemaphoreType.DMA((2, 14)),
                    pltpu.SemaphoreType.DMA((3, 2)), pltpu.SemaphoreType.DMA((2, n_loc)), pltpu.SemaphoreType.DMA((5,)),
                    pltpu.SemaphoreType.DMA((2,)), pltpu.SemaphoreType.DMA((7,)), pltpu.SemaphoreType.REGULAR,
                ],
                compiler_params=pltpu.CompilerParams(collective_id=0, has_side_effects=True, vmem_limit_bytes=67043328),
                name="moe_layer",
            )(x, dy, ids.T, gates.T, w1, w3, w2)
            y, go_r, go_l, sr, sl, sc, xr, dr, ur, dar, dbr, xh, dh, uh, dah, dbh = outs

            to_right = [(i, (i + 2) % group) for i in range(group)]
            to_left = [(i, (i + group - 2) % group) for i in range(group)]
            from_l = lax.ppermute(go_r, "ep", to_right)
            from_r = lax.ppermute(go_l, "ep", to_left)

            n_first = (n_loc + 1) // 2
            g_shapes = (sds((n_loc, width, hid), BF16), sds((n_loc, width, hid), BF16), sds((n_loc, hid, width), BF16))

            def blk(r, n, at):
                return pl.BlockSpec((1, r, n), lambda i: (at(i), 0, 0))

            def row_specs(at):
                return [blk(n_rows, width, at), blk(n_rows, width, at), blk(n_rows, hid, at), blk(n_rows, hid, at), blk(n_rows, hid, at)]

            def out_blks(at):
                return [blk(width, hid, at), blk(width, hid, at), blk(hid, width, at)]

            def cost(n):
                return pl.CostEstimate(flops=n * 6 * n_rows * width * hid, transcendentals=0,
                                       bytes_accessed=n * 2 * (2 * n_rows * width + 3 * n_rows * hid + 3 * width * hid))

            def first_at(i):
                return lax.rem(i + 1, n_first)

            def later_at(i):
                return i + n_first

            y_spec = pl.BlockSpec((tok, width), lambda i: (0, 0))
            *grads, y = pl.pallas_call(
                functools.partial(first_grads_kernel, owner),
                grid=(n_first,), out_shape=g_shapes + (sds((tok, width), BF16),),
                in_specs=row_specs(first_at) + [any_spec] * 5 + [y_spec], out_specs=out_blks(first_at) + [y_spec],
                scratch_shapes=[pltpu.VMEM((hot_rows, width), BF16), pltpu.VMEM((hot_rows, width), BF16), pltpu.VMEM((hot_rows, hid), BF16),
                                pltpu.VMEM((hot_rows, hid), BF16), pltpu.VMEM((hot_rows, hid), BF16), pltpu.SemaphoreType.DMA((5,))],
                compiler_params=pltpu.CompilerParams(vmem_limit_bytes=60 << 20),
                cost_estimate=cost(n_first), name="first_grads",
            )(xr, dr, ur, dar, dbr, xh, dh, uh, dah, dbh, y)

            fl_lo = lax.ppermute(sr + from_l[:half], "ep", to_right)
            fr_hi = lax.ppermute(sl + from_r[:half], "ep", to_left)
            g1, g3, g2 = pl.pallas_call(
                later_grads_kernel,
                grid=(n_loc - n_first,), out_shape=g_shapes,
                in_specs=row_specs(later_at) + [any_spec] * 3, out_specs=out_blks(later_at),
                input_output_aliases={5: 0, 6: 1, 7: 2},
                compiler_params=pltpu.CompilerParams(vmem_limit_bytes=60 << 20),
                cost_estimate=cost(n_loc - n_first), name="later_grads",
            )(xr, dr, ur, dar, dbr, *grads)
            fl = jnp.concatenate([fl_lo, from_l[half:]], axis=0)
            fr = jnp.concatenate([from_r[half:], fr_hi], axis=0)
            dx = (sc + fl + fr).astype(BF16)
            return y, dx, g1, g3, g2

        return jax.shard_map(device_fn, mesh=mesh, in_specs=(tok_spec, tok_spec, tok_spec, w_spec, w_spec, w_spec, tok_spec),
                             out_specs=(tok_spec, tok_spec, grad_spec, grad_spec, grad_spec), check_vma=False)(
            tokens, expert_ids, gate_vals, w_gate, w_up, w_down, grad_out)

    return layer_fn
```

```python
import functools

import jax
import jax.numpy as jnp
from jax import lax
from jax.experimental import pallas as pl
from jax.experimental.pallas import tpu as pltpu
from jax.sharding import PartitionSpec as P

MESH = pl.DeviceIdType.MESH
F32 = jnp.float32
BF16 = jnp.bfloat16


def dot_nn(a, b):
    return lax.dot_general(a, b, (((1,), (0,)), ((), ())), preferred_element_type=F32)


def dot_nt(a, b):
    return lax.dot_general(a, b, (((1,), (1,)), ((), ())), preferred_element_type=F32)


def dot_tn(a, b):
    return lax.dot_general(a, b, (((0,), (0,)), ((), ())), preferred_element_type=F32)


def layer_kernel(cfg, x_hbm, dy_hbm, ids_ref, gates_ref, w1_hbm, w3_hbm, w2_hbm,
                 yown, yfl, yfr, go_r, go_l, sr_hbm, sl_hbm, sc_hbm, xr_hbm, dr_hbm, ur_hbm, da_hbm, db_hbm, xh_hbm, dh_hbm, uh_hbm, dah_hbm, dbh_hbm,
                 x_all, dy_all, ids_all, gates_all, rt, gt, mc, ypart, dxpart, cbuf, yra, yrb,
                 erows, hrows, urow, uhot, darow, dbrow, act1, act2, orow, pbuf, w1, w3, w2,
                 m_send, m_recv, ag_send, ag_recv, rs_send, rs_recv, w_sem, st_sem, hst_sem, io_sem, so_sem, free_sem):
    chips, tok, width, hid, n_loc, cap, owner = cfg
    group = 2 * chips
    two = 2 * tok
    cp = 2 * cap
    n_rows = chips * cp
    hot_rows = chips * two
    half = tok // 2
    last = n_loc - 1
    me = lax.axis_index("ep")
    c = me // 2
    k = lax.rem(me, 2)
    c_r = lax.rem(c + 1, chips)
    c_l = lax.rem(c + chips - 1, chips)
    c_o = lax.rem(c + 2, chips)
    near = (c, c_l, c_r, c_o)
    right = 2 * c_r + k
    left = 2 * c_l + k
    partner = 2 * c + 1 - k
    is_owner = me == owner

    own_x = pltpu.make_async_copy(x_hbm, x_all.at[c, pl.ds(k * tok, tok)], io_sem.at[0])
    own_dy = pltpu.make_async_copy(dy_hbm, dy_all.at[c, pl.ds(k * tok, tok)], io_sem.at[1])
    own_x.start()
    own_dy.start()

    def w_copies(e):
        s = lax.rem(e, 2)
        return (pltpu.make_async_copy(w1_hbm.at[e], w1.at[s], w_sem.at[0, s]),
                pltpu.make_async_copy(w3_hbm.at[e], w3.at[s], w_sem.at[1, s]),
                pltpu.make_async_copy(w2_hbm.at[e], w2.at[s], w_sem.at[2, s]))

    for e in (0, 1):
        for cpy in w_copies(e):
            cpy.start()
    ids_all[me] = ids_ref[...]
    gates_all[me] = gates_ref[...]

    barrier = pltpu.get_barrier_semaphore()
    for d in range(1, group):
        pl.semaphore_signal(barrier, inc=1, device_id={"ep": lax.rem(me + d, group)}, device_id_type=MESH)
    pl.semaphore_wait(barrier, group - 1)

    def meta_copies(d):
        return tuple(pltpu.make_async_remote_copy(
            src_ref=src, dst_ref=dst.at[me], send_sem=m_send.at[i, d], recv_sem=m_recv.at[i, d],
            device_id={"ep": lax.rem(me + d, group)}, device_id_type=MESH)
            for i, (src, dst) in enumerate(((ids_ref, ids_all), (gates_ref, gates_all))))

    def ag(ref, t, i):
        chip, core, r0, n, dev = (
            (c, k, 0, half, right), (c, k, half, half, right), (c, k, half, half, left), (c, k, 0, half, left),
            (c, k, 0, tok, partner),
            (c_l, k, 0, half, right), (c_r, k, half, half, left),
            (c_l, k, 0, tok, partner), (c_r, k, 0, tok, partner),
            (c_o, k, 0, half, partner), (c_o, k, half, half, partner))[i]
        blk = ref.at[chip, pl.ds(core * tok + r0, n)]
        return pltpu.make_async_remote_copy(
            src_ref=blk, dst_ref=blk, send_sem=ag_send.at[t, i], recv_sem=ag_recv.at[t, i],
            device_id={"ep": dev}, device_id_type=MESH)

    own_x.wait()
    for d in range(1, group):
        for cpy in meta_copies(d):
            cpy.start()
    for i in (4, 0, 2, 1, 3):
        ag(x_all, 0, i).start()
    own_dy.wait()

    for d in range(1, group):
        for cpy in meta_copies(d):
            cpy.wait_recv()

    upper = (lax.broadcasted_iota(jnp.int32, (tok, tok), 0) < lax.broadcasted_iota(jnp.int32, (tok, tok), 1)).astype(F32).astype(BF16)
    row_id = lax.broadcasted_iota(jnp.int32, (8, tok), 0)
    for s in range(group):
        q, core = s // 2, s % 2
        ids = ids_all[s]
        gates = gates_all[s]
        mask_m = jnp.zeros((8, tok), F32)
        gate_m = jnp.zeros((8, tok), F32)
        for le in range(n_loc):
            eq = ids == me * n_loc + le
            hit = jnp.sum(jnp.where(eq, 1.0, 0.0), axis=0, keepdims=True)
            gv = jnp.sum(jnp.where(eq, gates, 0.0), axis=0, keepdims=True)
            mask_m = jnp.where(row_id == le, hit, mask_m)
            gate_m = jnp.where(row_id == le, gv, gate_m)
        rank = dot_nn(mask_m.astype(BF16), upper)
        pos = jnp.where(mask_m > 0.0, rank + float(cap * core), -1.0)
        rt[q, :, core * tok:(core + 1) * tok] = pos
        gt[q, :, core * tok:(core + 1) * tok] = gate_m
        both = jnp.concatenate([pos, gate_m, jnp.zeros((tok - 16, tok), F32)], axis=0)
        mc[q, core * tok:(core + 1) * tok, :] = jnp.transpose(both)

    def pick(p, q, src, scaled):
        for e in range(n_loc):
            hit = rt[q, e:e + 1, :] == lax.broadcasted_iota(jnp.int32, (cp, two), 0).astype(F32)
            pbuf[e * cp:(e + 1) * cp, :] = jnp.where(hit, 1.0, 0.0).astype(BF16)
        gates = [None] * n_loc
        if scaled:
            for e in range(n_loc):
                hit = rt[q, e:e + 1, :] == lax.broadcasted_iota(jnp.int32, (cp, two), 0).astype(F32)
                gates[e] = jnp.sum(jnp.where(hit, gt[q, e:e + 1, :], 0.0), axis=1, keepdims=True)
        for j in range(width // 256):
            cs = slice(j * 256, (j + 1) * 256)
            got = dot_nn(pbuf[...], src[q, :, cs])
            for e in range(n_loc):
                part = got[e * cp:(e + 1) * cp]
                erows[e, pl.ds(p * cp, cp), cs] = (gates[e] * part if scaled else part).astype(BF16)

    def column(q, lane):
        return jnp.sum(jnp.where(lax.broadcasted_iota(jnp.int32, (two, 128), 1) == lane, mc[q], 0.0), axis=1, keepdims=True)

    def put_rows(q, e):
        hit = column(q, e) == lax.broadcasted_iota(jnp.int32, (two, cp), 1).astype(F32)
        return jnp.where(hit, 1.0, 0.0).astype(BF16)

    def forward(m, src, dst, s, aoff, on, emit, used):
        for j in range(hid // 256):
            cs = slice(j * 256, (j + 1) * 256)
            a = dot_nn(src[...], w1[s, :, cs])
            b = dot_nn(src[...], w3[s, :, cs])
            sg = jax.nn.sigmoid(a)
            ga = a * sg
            fa = b * (sg * (1.0 + a * (1.0 - sg)))
            u = ga * b
            if on is not None:
                fa, ga, u = jnp.where(on, fa, 0.0), jnp.where(on, ga, 0.0), jnp.where(on, u, 0.0)
            act1[pl.ds(aoff, m), cs] = fa
            act2[pl.ds(aoff, m), cs] = ga
            dst[:, cs] = u.astype(BF16)

        used(0)
        for j in range(width // 256):
            cs = slice(j * 256, (j + 1) * 256)
            emit(cs, dot_nn(dst[...], w2[s, :, cs]).astype(BF16))

    all_tiles = range(width // 256)

    def backward_du(m, src, s, aoff, ab=None):
        ab = s if ab is None else ab
        for j in range(hid // 256):
            cs = slice(j * 256, (j + 1) * 256)
            du = dot_nt(src[...], w2[s, cs, :])
            darow[ab, 0:m, cs] = (du * act1[pl.ds(aoff, m), cs]).astype(BF16)
            dbrow[ab, 0:m, cs] = (du * act2[pl.ds(aoff, m), cs]).astype(BF16)
    def backward_dx(m, s, tiles, emit, ab=None):
        ab = s if ab is None else ab
        for j in tiles:
            cs = slice(j * 256, (j + 1) * 256)
            emit(cs, (dot_nt(darow[ab, 0:m, :], w1[s, cs, :]) + dot_nt(dbrow[ab, 0:m, :], w3[s, cs, :])).astype(BF16))

    def act_off(e):
        return pl.multiple_of(jnp.where(e == 0, 0, hot_rows + (e - 1) * n_rows), 64)

    def add_out(q, e, first, fresh):
        gate = column(q, e + 8)
        put = put_rows(q, e)
        for j in range(width // 256):
            cs = slice(j * 256, (j + 1) * 256)
            ypart[q, :, cs] = jnp.where(fresh, 0.0, ypart[q, :, cs]) + gate * dot_nn(put, orow[first:first + cp, cs])

    def add_dx_one(q, p, e):
        put = put_rows(q, e)
        for j in range(width // 256):
            cs = slice(j * 256, (j + 1) * 256)
            dxpart[q, :, cs] = dot_nn(put, orow[p * cp:(p + 1) * cp, cs])

    def add_dx_two(q, p, e, tiles):
        now, before = column(q, e), column(q, e - 1)
        now = jnp.where(now >= 0.0, now + float(cp), -1.0)
        lane = lax.broadcasted_iota(jnp.int32, (two, 2 * cp), 1).astype(F32)
        put = jnp.where(jnp.logical_or(before == lane, now == lane), 1.0, 0.0).astype(BF16)
        for j in tiles:
            cs = slice(j * 256, (j + 1) * 256)
            both = jnp.concatenate([orow[2 * two + p * cp:2 * two + (p + 1) * cp, cs], orow[p * cp:(p + 1) * cp, cs]], axis=0)
            dxpart[q, :, cs] += dot_nn(put, both)

    def lane_of(q, r, n, lane):
        m = mc[q, pl.ds(r, n), :]
        return jnp.sum(jnp.where(lax.broadcasted_iota(jnp.int32, (n, 128), 1) == lane, m, 0.0), axis=1, keepdims=True)

    def hot_forward(p, q, s, fresh):
        o = pl.multiple_of(p * two, 64)
        gate = column(q, 8)

        def emit(cs, out):
            ypart[q, :, cs] = jnp.where(fresh, 0.0, ypart[q, :, cs]) + gate * out.astype(F32)

        forward(two, x_all.at[q], uhot.at[pl.ds(o, two)], s, o, column(q, 0) >= 0.0, emit, lambda part: None)

    def load_next(i, e, step, parts):
        @pl.when(i < last - 1)
        def _():
            for n in parts:
                w_copies(e + 2 * step)[n].start()

    def cold_forward(i, e, step, s, r0, r1):
        def emit(cs, out):
            orow[0:r1 - r0, cs] = out

        forward(r1 - r0, erows.at[e, r0:r1], urow.at[e, r0:r1], s, pl.multiple_of(act_off(e) + r0, 16), None, emit,
                lambda part: load_next(i, e, step, (0, 1)))
        load_next(i, e, step, (2,))

    def weights_here(i, e, first):
        @pl.when(i >= (0 if first else 2))
        def _():
            for cpy in w_copies(e):
                cpy.wait()

    def rs(t, j):
        part = (ypart, dxpart)[t]
        o = k * tok
        if j < 4:
            q = (c_o, c_r, c_l, c)[j]
            src, dst, dev = part.at[q, pl.ds((1 - k) * tok, tok)], cbuf.at[q], partner
            if t == 1:
                src, dst = part.at[q, pl.ds((1 - k) * tok, tok), 0:width // 2], cbuf.at[q, :, 0:width // 2]
        elif j >= 10:
            q = (c_o, c_r, c_l, c)[j - 10]
            src, dst, dev = part.at[q, pl.ds((1 - k) * tok, tok), width // 2:width], cbuf.at[q, :, width // 2:width], partner
        else:
            src, dst, dev = (
                (part.at[c_o, pl.ds(o, half)], yra, right),
                (part.at[c_o, pl.ds(o + half, half)], yrb, left),
                (part.at[c_r, pl.ds(o + half, half)], yfl.at[half:tok], right),
                (part.at[c_l, pl.ds(o, half)], yfr.at[0:half], left),
                (part.at[c_r, pl.ds(o, half)], yfl.at[0:half], right),
                (part.at[c_l, pl.ds(o + half, half)], yfr.at[half:tok], left))[j - 4]
        return pltpu.make_async_remote_copy(
            src_ref=src, dst_ref=dst, send_sem=rs_send.at[t, j], recv_sem=rs_recv.at[t, j],
            device_id={"ep": dev}, device_id_type=MESH)

    def add_rows(part, q, off, src, n):
        @pl.loop(0, n // 32)
        def _(r):
            o = pl.multiple_of(r * 32, 32)
            part[q, pl.ds(pl.multiple_of(off + r * 32, 32), 32)] += src[pl.ds(o, 32)]

    ag(x_all, 0, 4).wait_recv()
    pick(0, c, x_all, False)

    @pl.loop(0, n_loc)
    def _(e):
        s = lax.rem(e, 2)
        hot = jnp.logical_and(is_owner, e == 0)
        weights_here(e, e, True)

        @pl.when(e == 2)
        def _():
            ag(x_all, 0, 0).wait_recv()
            ag(x_all, 0, 5).start()
            ag(x_all, 0, 2).wait_recv()
            ag(x_all, 0, 6).start()
            for n in (4, 0, 2, 1, 3):
                ag(dy_all, 1, n).start()

        @pl.when(jnp.logical_not(hot))
        def _():
            cold_forward(e, e, 1, s, 0, cp)
            add_out(c, e, 0, e == 0)

        @pl.when(hot)
        def _():
            hot_forward(0, c, s, True)
            load_next(e, e, 1, (0, 1, 2))

    ag(x_all, 0, 1).wait_recv()
    ag(x_all, 0, 7).start()
    ag(x_all, 0, 3).wait_recv()
    ag(x_all, 0, 8).start()
    rs(0, 3).start()
    ag(x_all, 0, 7).wait_recv()
    pick(1, c_l, x_all, False)
    ag(x_all, 0, 5).wait_recv()
    ag(x_all, 0, 9).start()
    ag(x_all, 0, 6).wait_recv()
    ag(x_all, 0, 10).start()
    ag(x_all, 0, 8).wait_recv()
    pick(2, c_r, x_all, False)
    rs(0, 3).wait_recv()
    add_rows(ypart, c, k * tok, cbuf.at[c], tok)
    own_out = pltpu.make_async_copy(ypart.at[c, pl.ds(k * tok, tok)], yown, io_sem.at[0])
    own_out.start()
    ag(x_all, 0, 9).wait_recv()
    ag(x_all, 0, 10).wait_recv()
    pick(3, c_o, x_all, False)

    def st_fwd(e):
        return (pltpu.make_async_copy(erows.at[e], xr_hbm.at[e], st_sem.at[0, e]),
                pltpu.make_async_copy(urow.at[e], ur_hbm.at[e], st_sem.at[1, e]))

    for e in range(n_loc):
        st_fwd(e)[0].start()

    def st_hot():
        return [pltpu.make_async_copy(uhot, uh_hbm, hst_sem.at[0])] + [
            pltpu.make_async_copy(x_all.at[q], xh_hbm.at[p * two:(p + 1) * two], hst_sem.at[1 + p]) for p, q in enumerate(near)]

    @pl.loop(0, n_loc)
    def _(i):
        e = last - i
        s = lax.rem(e, 2)
        hot = jnp.logical_and(is_owner, e == 0)
        weights_here(i, e, False)

        @pl.when(i == 1)
        def _():
            ag(dy_all, 1, 0).wait_recv()
            ag(dy_all, 1, 5).start()
            ag(dy_all, 1, 2).wait_recv()
            ag(dy_all, 1, 6).start()

        @pl.when(i == 3)
        def _():
            ag(dy_all, 1, 4).wait_recv()
            ag(dy_all, 1, 1).wait_recv()
            ag(dy_all, 1, 7).start()
            ag(dy_all, 1, 3).wait_recv()
            ag(dy_all, 1, 8).start()

        @pl.when(jnp.logical_not(hot))
        def _():
            cold_forward(i, e, -1, s, cp, n_rows)
            for j, p in enumerate((3, 2, 1)):
                add_out(near[p], e, (p - 1) * cp, i == 0)

                @pl.when(i == last)
                def _():
                    rs(0, j).start()

            st_fwd(e)[1].start()

        @pl.when(hot)
        def _():
            @pl.loop(0, 3)
            def _(n):
                p = 3 - n
                hot_forward(p, jnp.where(p == 1, c_l, jnp.where(p == 2, c_r, c_o)), s, False)
                for j in range(3):
                    @pl.when(n == j)
                    def _():
                        rs(0, j).start()

            for cpy in st_hot():
                cpy.start()

    for e in range(n_loc):
        st_fwd(e)[0].wait()
    rs(0, 0).wait_recv()
    add_rows(ypart, c_o, k * tok, cbuf.at[c_o], tok)
    rs(0, 4).start()
    rs(0, 5).start()
    ag(dy_all, 1, 5).wait_recv()
    ag(dy_all, 1, 9).start()
    ag(dy_all, 1, 6).wait_recv()
    ag(dy_all, 1, 10).start()
    pick(0, c, dy_all, True)
    for j, q in ((1, c_r), (2, c_l)):
        rs(0, j).wait_recv()
        add_rows(ypart, q, k * tok, cbuf.at[q], tok)
        rs(0, 5 + j).start()
    pl.semaphore_signal(free_sem, inc=1, device_id={"ep": partner}, device_id_type=MESH)
    ag(dy_all, 1, 7).wait_recv()
    pick(1, c_l, dy_all, True)
    ag(dy_all, 1, 8).wait_recv()
    pick(2, c_r, dy_all, True)
    ag(dy_all, 1, 9).wait_recv()
    ag(dy_all, 1, 10).wait_recv()
    pick(3, c_o, dy_all, True)

    @pl.loop(0, n_loc)
    def _(e):
        @pl.when(jnp.logical_not(jnp.logical_and(is_owner, e == 0)))
        def _():
            st_fwd(e)[1].wait()

    @pl.when(is_owner)
    def _():
        for cpy in st_hot():
            cpy.wait()

    def st_d(e):
        return pltpu.make_async_copy(erows.at[e], dr_hbm.at[e], st_sem.at[0, e])

    def st_ab(e, s):
        return (pltpu.make_async_copy(darow.at[s, 0:n_rows], da_hbm.at[e], st_sem.at[1, s]),
                pltpu.make_async_copy(dbrow.at[s, 0:n_rows], db_hbm.at[e], st_sem.at[1, 2 + s]))

    for e in range(n_loc):
        st_d(e).start()

    def st_hot_ab(h):
        at = pl.multiple_of(h * 2 * two, 64)
        return (pltpu.make_async_copy(darow.at[h], dah_hbm.at[pl.ds(at, 2 * two)], hst_sem.at[1 + h]),
                pltpu.make_async_copy(dbrow.at[h], dbh_hbm.at[pl.ds(at, 2 * two)], hst_sem.at[3 + h]))

    def rs_relay_y():
        rs(0, 4).wait_recv()
        add_rows(ypart, c_r, k * tok, yra, half)
        rs(0, 8).start()
        rs(0, 5).wait_recv()
        add_rows(ypart, c_l, k * tok + half, yrb, half)
        rs(0, 9).start()

    @pl.loop(0, n_loc)
    def _(e):
        s = lax.rem(e, 2)
        hot = jnp.logical_and(is_owner, e == 0)

        weights_here(e, e, False)

        @pl.when(jnp.logical_and(is_owner, e == 1))
        def _():
            for h in range(2):
                for cpy in st_hot_ab(h):
                    cpy.wait()

        @pl.when(jnp.logical_not(hot))
        def _():
            ooff = pl.multiple_of(s * 2 * two, 64)

            def emit(cs, out):
                orow[pl.ds(ooff, n_rows), cs] = out

            backward_du(n_rows, erows.at[e], s, act_off(e))

            @pl.when(e < last)
            def _():
                backward_dx(n_rows, s, all_tiles, emit)
                load_next(e, e, 1, (0, 1, 2))

                @pl.when(e == last - 2)
                def _():
                    rs_relay_y()

                @pl.when(e == 0)
                def _():
                    for p in range(chips):
                        add_dx_one(near[p], p, e)

                @pl.when(jnp.logical_and(e > 0, s == 0))
                def _():
                    for p in (3, 2, 1, 0):
                        add_dx_two(near[p], p, e, all_tiles)

            @pl.when(e == last)
            def _():
                for h in range(2):
                    tiles = all_tiles[h * len(all_tiles) // 2:(h + 1) * len(all_tiles) // 2]
                    backward_dx(n_rows, s, tiles, emit)
                    if h == 0:
                        pl.semaphore_wait(free_sem, 1)
                    for j, p in enumerate((3, 2, 1, 0)):
                        add_dx_two(near[p], p, e, tiles)
                        rs(1, j + 10 * h).start()

        @pl.when(hot)
        def _():
            @pl.loop(0, chips // 2)
            def _(h):
                pair = (jnp.where(h == 0, c, c_r), jnp.where(h == 0, c_l, c_o))
                for n, q in enumerate(pair):
                    @pl.loop(0, two // 64)
                    def _(r):
                        at = pl.multiple_of(r * 64, 64)
                        got = dy_all[q, pl.ds(at, 64), :].astype(F32)
                        hrows[pl.ds(pl.multiple_of(n * two + r * 64, 64), 64), :] = (lane_of(q, at, 64, 8) * got).astype(BF16)

                o = pl.multiple_of(h * 2 * two, 64)
                sd = pltpu.make_async_copy(hrows, dh_hbm.at[pl.ds(o, 2 * two)], hst_sem.at[0])
                sd.start()

                def emit(cs, out):
                    for n, q in enumerate(pair):
                        dxpart[q, :, cs] = out[n * two:(n + 1) * two].astype(F32)

                backward_du(2 * two, hrows, s, o, h)
                backward_dx(2 * two, s, all_tiles, emit, h)
                for cpy in st_hot_ab(h):
                    cpy.start()
                sd.wait()

            load_next(e, e, 1, (0, 1, 2))

        @pl.when(jnp.logical_and(e >= 1, jnp.logical_not(jnp.logical_and(is_owner, e == 1))))
        def _():
            for cpy in st_ab(e - 1, 1 - s):
                cpy.wait()

        @pl.when(jnp.logical_not(hot))
        def _():
            for cpy in st_ab(e, s):
                cpy.start()

    def chip_sums_out(j):
        q = (c_o, c_r, c_l, c)[j]
        lo = dxpart.at[q, pl.ds(k * tok, half)]
        hi = dxpart.at[q, pl.ds(k * tok + half, half)]
        if j == 3:
            return (pltpu.make_async_copy(dxpart.at[q, pl.ds(k * tok, tok)], sc_hbm, so_sem.at[6]),)
        to_lo, to_hi = ((go_r.at[0:half], go_l.at[0:half]), (sr_hbm, go_r.at[half:tok]), (go_l.at[half:tok], sl_hbm))[j]
        return (pltpu.make_async_copy(lo, to_lo, so_sem.at[2 * j]), pltpu.make_async_copy(hi, to_hi, so_sem.at[2 * j + 1]))

    for j, q in enumerate((c_o, c_r, c_l, c)):
        rs(1, j).wait_recv()
        rs(1, j + 10).wait_recv()
        add_rows(dxpart, q, k * tok, cbuf.at[q], tok)
        for cpy in chip_sums_out(j):
            cpy.start()
    for j in (6, 7, 8, 9):
        rs(0, j).wait_recv()

    for e in range(n_loc):
        st_d(e).wait()
    for cpy in st_ab(last, last % 2):
        cpy.wait()
    for d in range(1, group):
        for cpy in meta_copies(d):
            cpy.wait_send()
    for i in range(11):
        ag(x_all, 0, i).wait_send()
        ag(dy_all, 1, i).wait_send()
    for j in range(10):
        rs(0, j).wait_send()
    for j in range(4):
        rs(1, j).wait_send()
        rs(1, j + 10).wait_send()
        for cpy in chip_sums_out(j):
            cpy.wait()
    own_out.wait()


def expert_grads(x_ref, d_ref, u_ref, da_ref, db_ref, g1, g3, g2):
    g1[0] = dot_tn(x_ref[0], da_ref[0]).astype(BF16)
    g3[0] = dot_tn(x_ref[0], db_ref[0]).astype(BF16)
    g2[0] = dot_tn(u_ref[0], d_ref[0]).astype(BF16)


def first_grads_kernel(owner, x_ref, d_ref, u_ref, da_ref, db_ref, xh, dh, uh, dah, dbh, own_ref, fl_ref, fr_ref, g1, g3, g2, y_out, xb, dbuf, ub, dab, dbb, sem):
    i = pl.program_id(0)
    is_owner = lax.axis_index("ep") == owner
    hot = jnp.logical_and(is_owner, i == pl.num_programs(0) - 1)

    def copies():
        return [pltpu.make_async_copy(src, dst, sem.at[j]) for j, (src, dst) in enumerate(((xh, xb), (dah, dab), (dbh, dbb), (uh, ub), (dh, dbuf)))]

    @pl.when(i == 0)
    def _():
        y_out[...] = (own_ref[...] + fl_ref[...] + fr_ref[...]).astype(BF16)

    @pl.when(jnp.logical_and(is_owner, i == 0))
    def _():
        for cpy in copies():
            cpy.start()

    @pl.when(jnp.logical_not(hot))
    def _():
        expert_grads(x_ref, d_ref, u_ref, da_ref, db_ref, g1, g3, g2)

    @pl.when(hot)
    def _():
        for cpy in copies():
            cpy.wait()
        g1[0] = dot_tn(xb[...], dab[...]).astype(BF16)
        g3[0] = dot_tn(xb[...], dbb[...]).astype(BF16)
        g2[0] = dot_tn(ub[...], dbuf[...]).astype(BF16)


def later_grads_kernel(x_ref, d_ref, u_ref, da_ref, db_ref, g1_in, g3_in, g2_in, g1, g3, g2):
    del g1_in, g3_in, g2_in
    expert_grads(x_ref, d_ref, u_ref, da_ref, db_ref, g1, g3, g2)


def solution(mesh):
    group = mesh.shape["ep"]
    num_dev = mesh.shape["dp"] * group
    tok_spec = P(("dp", "ep"), None)
    w_spec = P("ep", None, None)
    grad_spec = P(("dp", "ep"), None, None)

    def layer_fn(tokens, expert_ids, gate_vals, w_gate, w_up, w_down, grad_out):
        n_exp, width, hid = w_gate.shape
        tok = tokens.shape[0] // num_dev
        top_k = expert_ids.shape[1]
        cap = ((2 * tok * top_k + 8 * n_exp - 1) // (8 * n_exp)) * 8
        n_loc = n_exp // group
        hot = n_exp // 2
        owner = hot // n_loc
        chips = group // 2
        n_rows = chips * 2 * cap
        hot_rows = group * tok
        cfg = (chips, tok, width, hid, n_loc, cap, owner)

        def device_fn(x, ids, gates, w1, w3, w2, dy):
            any_spec = pl.BlockSpec(memory_space=pl.ANY)
            vmem_spec = pl.BlockSpec(memory_space=pltpu.VMEM)
            sds = jax.ShapeDtypeStruct
            hb = hot_rows // 2
            half = tok // 2
            act_rows = hot_rows + (n_loc - 1) * n_rows
            outs = pl.pallas_call(
                functools.partial(layer_kernel, cfg),
                out_shape=(
                    *[sds((tok, width), F32)] * 5, *[sds((half, width), F32)] * 2, sds((tok, width), F32),
                    sds((n_loc, n_rows, width), BF16), sds((n_loc, n_rows, width), BF16),
                    sds((n_loc, n_rows, hid), BF16), sds((n_loc, n_rows, hid), BF16), sds((n_loc, n_rows, hid), BF16),
                    sds((hot_rows, width), BF16), sds((hot_rows, width), BF16),
                    sds((hot_rows, hid), BF16), sds((hot_rows, hid), BF16), sds((hot_rows, hid), BF16)),
                in_specs=[any_spec, any_spec, vmem_spec, vmem_spec, any_spec, any_spec, any_spec],
                out_specs=[any_spec] * 18,
                scratch_shapes=[
                    pltpu.VMEM((chips, 2 * tok, width), BF16), pltpu.VMEM((chips, 2 * tok, width), BF16),
                    pltpu.VMEM((group, top_k, tok), jnp.int32), pltpu.VMEM((group, top_k, tok), F32),
                    pltpu.VMEM((chips, 8, 2 * tok), F32), pltpu.VMEM((chips, 8, 2 * tok), F32),
                    pltpu.VMEM((chips, 2 * tok, 128), F32),
                    pltpu.VMEM((chips, 2 * tok, width), F32), pltpu.VMEM((chips, 2 * tok, width), F32),
                    pltpu.VMEM((chips, tok, width), F32),
                    pltpu.VMEM((half, width), F32), pltpu.VMEM((half, width), F32),
                    pltpu.VMEM((n_loc, n_rows, width), BF16), pltpu.VMEM((hb, width), BF16),
                    pltpu.VMEM((n_loc, n_rows, hid), BF16), pltpu.VMEM((hot_rows, hid), BF16),
                    pltpu.VMEM((2, hb, hid), BF16), pltpu.VMEM((2, hb, hid), BF16),
                    pltpu.VMEM((act_rows, hid), F32), pltpu.VMEM((act_rows, hid), F32),
                    pltpu.VMEM((hb + n_rows, width), BF16), pltpu.VMEM((n_loc * 2 * cap, 2 * tok), BF16),
                    pltpu.VMEM((2, width, hid), BF16), pltpu.VMEM((2, width, hid), BF16), pltpu.VMEM((2, hid, width), BF16),
                    pltpu.SemaphoreType.DMA((2, group)), pltpu.SemaphoreType.DMA((2, group)),
                    pltpu.SemaphoreType.DMA((2, 11)), pltpu.SemaphoreType.DMA((2, 11)),
                    pltpu.SemaphoreType.DMA((2, 14)), pltpu.SemaphoreType.DMA((2, 14)),
                    pltpu.SemaphoreType.DMA((3, 2)), pltpu.SemaphoreType.DMA((2, n_loc)), pltpu.SemaphoreType.DMA((5,)),
                    pltpu.SemaphoreType.DMA((2,)), pltpu.SemaphoreType.DMA((7,)), pltpu.SemaphoreType.REGULAR,
                ],
                compiler_params=pltpu.CompilerParams(collective_id=0, has_side_effects=True, vmem_limit_bytes=67043328),
                name="moe_layer",
            )(x, dy, ids.T, gates.T, w1, w3, w2)
            yown, yfl, yfr, go_r, go_l, sr, sl, sc, xr, dr, ur, dar, dbr, xh, dh, uh, dah, dbh = outs

            to_right = [(i, (i + 2) % group) for i in range(group)]
            to_left = [(i, (i + group - 2) % group) for i in range(group)]
            from_l = lax.ppermute(go_r, "ep", to_right)
            from_r = lax.ppermute(go_l, "ep", to_left)

            n_first = (n_loc + 1) // 2
            g_shapes = (sds((n_loc, width, hid), BF16), sds((n_loc, width, hid), BF16), sds((n_loc, hid, width), BF16))

            def blk(r, n, at):
                return pl.BlockSpec((1, r, n), lambda i: (at(i), 0, 0))

            def row_specs(at):
                return [blk(n_rows, width, at), blk(n_rows, width, at), blk(n_rows, hid, at), blk(n_rows, hid, at), blk(n_rows, hid, at)]

            def out_blks(at):
                return [blk(width, hid, at), blk(width, hid, at), blk(hid, width, at)]

            def cost(n):
                return pl.CostEstimate(flops=n * 6 * n_rows * width * hid, transcendentals=0,
                                       bytes_accessed=n * 2 * (2 * n_rows * width + 3 * n_rows * hid + 3 * width * hid))

            def first_at(i):
                return lax.rem(i + 1, n_first)

            def later_at(i):
                return i + n_first

            y_spec = pl.BlockSpec((tok, width), lambda i: (0, 0))
            *grads, y = pl.pallas_call(
                functools.partial(first_grads_kernel, owner),
                grid=(n_first,), out_shape=g_shapes + (sds((tok, width), BF16),),
                in_specs=row_specs(first_at) + [any_spec] * 5 + [y_spec] * 3, out_specs=out_blks(first_at) + [y_spec],
                scratch_shapes=[pltpu.VMEM((hot_rows, width), BF16), pltpu.VMEM((hot_rows, width), BF16), pltpu.VMEM((hot_rows, hid), BF16),
                                pltpu.VMEM((hot_rows, hid), BF16), pltpu.VMEM((hot_rows, hid), BF16), pltpu.SemaphoreType.DMA((5,))],
                compiler_params=pltpu.CompilerParams(vmem_limit_bytes=60 << 20),
                cost_estimate=cost(n_first), name="first_grads",
            )(xr, dr, ur, dar, dbr, xh, dh, uh, dah, dbh, yown, yfl, yfr)

            fl_lo = lax.ppermute(sr + from_l[:half], "ep", to_right)
            fr_hi = lax.ppermute(sl + from_r[:half], "ep", to_left)
            g1, g3, g2 = pl.pallas_call(
                later_grads_kernel,
                grid=(n_loc - n_first,), out_shape=g_shapes,
                in_specs=row_specs(later_at) + [any_spec] * 3, out_specs=out_blks(later_at),
                input_output_aliases={5: 0, 6: 1, 7: 2},
                compiler_params=pltpu.CompilerParams(vmem_limit_bytes=60 << 20),
                cost_estimate=cost(n_loc - n_first), name="later_grads",
            )(xr, dr, ur, dar, dbr, *grads)
            fl = jnp.concatenate([fl_lo, from_l[half:]], axis=0)
            fr = jnp.concatenate([from_r[half:], fr_hi], axis=0)
            dx = (sc + fl + fr).astype(BF16)
            return y, dx, g1, g3, g2

        return jax.shard_map(device_fn, mesh=mesh, in_specs=(tok_spec, tok_spec, tok_spec, w_spec, w_spec, w_spec, tok_spec),
                             out_specs=(tok_spec, tok_spec, grad_spec, grad_spec, grad_spec), check_vma=False)(
            tokens, expert_ids, gate_vals, w_gate, w_up, w_down, grad_out)

    return layer_fn
```

```python
import functools

import jax
import jax.numpy as jnp
from jax import lax
from jax.experimental import pallas as pl
from jax.experimental.pallas import tpu as pltpu
from jax.sharding import PartitionSpec as P

MESH = pl.DeviceIdType.MESH
F32 = jnp.float32
BF16 = jnp.bfloat16


def dot_nn(a, b):
    return lax.dot_general(a, b, (((1,), (0,)), ((), ())), preferred_element_type=F32)


def dot_nt(a, b):
    return lax.dot_general(a, b, (((1,), (1,)), ((), ())), preferred_element_type=F32)


def dot_tn(a, b):
    return lax.dot_general(a, b, (((0,), (0,)), ((), ())), preferred_element_type=F32)


def layer_kernel(cfg, x_hbm, dy_hbm, ids_ref, gates_ref, w1_hbm, w3_hbm, w2_hbm,
                 yown, yfl, yfr, go_r, go_l, sr_hbm, sl_hbm, sc_hbm, xr_hbm, dr_hbm, ur_hbm, da_hbm, db_hbm, xh_hbm, dh_hbm, uh_hbm, dah_hbm, dbh_hbm,
                 x_all, dy_all, ids_all, gates_all, rt, gt, mc, ypart, dxpart, cbuf, yra, yrb,
                 erows, hrows, urow, uhot, darow, dbrow, act1, act2, orow, pbuf, w1, w3, w2,
                 m_send, m_recv, ag_send, ag_recv, rs_send, rs_recv, w_sem, st_sem, hst_sem, io_sem, so_sem, free_sem):
    chips, tok, width, hid, n_loc, cap, owner = cfg
    group = 2 * chips
    two = 2 * tok
    cp = 2 * cap
    n_rows = chips * cp
    hot_rows = chips * two
    half = tok // 2
    last = n_loc - 1
    me = lax.axis_index("ep")
    c = me // 2
    k = lax.rem(me, 2)
    c_r = lax.rem(c + 1, chips)
    c_l = lax.rem(c + chips - 1, chips)
    c_o = lax.rem(c + 2, chips)
    near = (c, c_l, c_r, c_o)
    right = 2 * c_r + k
    left = 2 * c_l + k
    partner = 2 * c + 1 - k
    is_owner = me == owner

    own_x = pltpu.make_async_copy(x_hbm, x_all.at[c, pl.ds(k * tok, tok)], io_sem.at[0])
    own_dy = pltpu.make_async_copy(dy_hbm, dy_all.at[c, pl.ds(k * tok, tok)], io_sem.at[1])
    own_x.start()
    own_dy.start()

    def w_copies(e):
        s = lax.rem(e, 2)
        return (pltpu.make_async_copy(w1_hbm.at[e], w1.at[s], w_sem.at[0, s]),
                pltpu.make_async_copy(w3_hbm.at[e], w3.at[s], w_sem.at[1, s]),
                pltpu.make_async_copy(w2_hbm.at[e], w2.at[s], w_sem.at[2, s]))

    for e in (0, 1):
        for cpy in w_copies(e):
            cpy.start()
    ids_all[me] = ids_ref[...]
    gates_all[me] = gates_ref[...]

    barrier = pltpu.get_barrier_semaphore()
    for d in range(1, group):
        pl.semaphore_signal(barrier, inc=1, device_id={"ep": lax.rem(me + d, group)}, device_id_type=MESH)
    pl.semaphore_wait(barrier, group - 1)

    def meta_copies(d):
        return tuple(pltpu.make_async_remote_copy(
            src_ref=src, dst_ref=dst.at[me], send_sem=m_send.at[i, d], recv_sem=m_recv.at[i, d],
            device_id={"ep": lax.rem(me + d, group)}, device_id_type=MESH)
            for i, (src, dst) in enumerate(((ids_ref, ids_all), (gates_ref, gates_all))))

    def ag(ref, t, i):
        chip, core, r0, n, dev = (
            (c, k, 0, half, right), (c, k, half, half, right), (c, k, half, half, left), (c, k, 0, half, left),
            (c, k, 0, tok, partner),
            (c_l, k, 0, half, right), (c_r, k, half, half, left),
            (c_l, k, 0, tok, partner), (c_r, k, 0, tok, partner),
            (c_o, k, 0, half, partner), (c_o, k, half, half, partner))[i]
        blk = ref.at[chip, pl.ds(core * tok + r0, n)]
        return pltpu.make_async_remote_copy(
            src_ref=blk, dst_ref=blk, send_sem=ag_send.at[t, i], recv_sem=ag_recv.at[t, i],
            device_id={"ep": dev}, device_id_type=MESH)

    own_x.wait()
    for d in range(1, group):
        for cpy in meta_copies(d):
            cpy.start()
    for i in (4, 0, 2, 1, 3):
        ag(x_all, 0, i).start()
    own_dy.wait()

    for d in range(1, group):
        for cpy in meta_copies(d):
            cpy.wait_recv()

    upper = (lax.broadcasted_iota(jnp.int32, (tok, tok), 0) < lax.broadcasted_iota(jnp.int32, (tok, tok), 1)).astype(F32).astype(BF16)
    row_id = lax.broadcasted_iota(jnp.int32, (8, tok), 0)
    for s in range(group):
        q, core = s // 2, s % 2
        ids = ids_all[s]
        gates = gates_all[s]
        mask_m = jnp.zeros((8, tok), F32)
        gate_m = jnp.zeros((8, tok), F32)
        for le in range(n_loc):
            eq = ids == me * n_loc + le
            hit = jnp.sum(jnp.where(eq, 1.0, 0.0), axis=0, keepdims=True)
            gv = jnp.sum(jnp.where(eq, gates, 0.0), axis=0, keepdims=True)
            mask_m = jnp.where(row_id == le, hit, mask_m)
            gate_m = jnp.where(row_id == le, gv, gate_m)
        rank = dot_nn(mask_m.astype(BF16), upper)
        pos = jnp.where(mask_m > 0.0, rank + float(cap * core), -1.0)
        rt[q, :, core * tok:(core + 1) * tok] = pos
        gt[q, :, core * tok:(core + 1) * tok] = gate_m
        both = jnp.concatenate([pos, gate_m, jnp.zeros((tok - 16, tok), F32)], axis=0)
        mc[q, core * tok:(core + 1) * tok, :] = jnp.transpose(both)

    def pick(p, q, src, scaled):
        for e in range(n_loc):
            hit = rt[q, e:e + 1, :] == lax.broadcasted_iota(jnp.int32, (cp, two), 0).astype(F32)
            pbuf[e * cp:(e + 1) * cp, :] = jnp.where(hit, 1.0, 0.0).astype(BF16)
        gates = [None] * n_loc
        if scaled:
            for e in range(n_loc):
                hit = rt[q, e:e + 1, :] == lax.broadcasted_iota(jnp.int32, (cp, two), 0).astype(F32)
                gates[e] = jnp.sum(jnp.where(hit, gt[q, e:e + 1, :], 0.0), axis=1, keepdims=True)
        for j in range(width // 256):
            cs = slice(j * 256, (j + 1) * 256)
            got = dot_nn(pbuf[...], src[q, :, cs])
            for e in range(n_loc):
                part = got[e * cp:(e + 1) * cp]
                erows[e, pl.ds(p * cp, cp), cs] = (gates[e] * part if scaled else part).astype(BF16)

    def column(q, lane):
        return jnp.sum(jnp.where(lax.broadcasted_iota(jnp.int32, (two, 128), 1) == lane, mc[q], 0.0), axis=1, keepdims=True)

    def put_rows(q, e):
        hit = column(q, e) == lax.broadcasted_iota(jnp.int32, (two, cp), 1).astype(F32)
        return jnp.where(hit, 1.0, 0.0).astype(BF16)

    def forward(m, src, dst, s, aoff, on, emit, used):
        for j in range(hid // 256):
            cs = slice(j * 256, (j + 1) * 256)
            a = dot_nn(src[...], w1[s, :, cs])
            b = dot_nn(src[...], w3[s, :, cs])
            sg = jax.nn.sigmoid(a)
            ga = a * sg
            fa = b * (sg * (1.0 + a * (1.0 - sg)))
            u = ga * b
            if on is not None:
                fa, ga, u = jnp.where(on, fa, 0.0), jnp.where(on, ga, 0.0), jnp.where(on, u, 0.0)
            act1[pl.ds(aoff, m), cs] = fa
            act2[pl.ds(aoff, m), cs] = ga
            dst[:, cs] = u.astype(BF16)

        used(0)
        for j in range(width // 256):
            cs = slice(j * 256, (j + 1) * 256)
            emit(cs, dot_nn(dst[...], w2[s, :, cs]).astype(BF16))

    all_tiles = range(width // 256)

    def backward_du(m, src, s, aoff, ab=None):
        ab = s if ab is None else ab
        for j in range(hid // 256):
            cs = slice(j * 256, (j + 1) * 256)
            du = dot_nt(src[...], w2[s, cs, :])
            darow[ab, 0:m, cs] = (du * act1[pl.ds(aoff, m), cs]).astype(BF16)
            dbrow[ab, 0:m, cs] = (du * act2[pl.ds(aoff, m), cs]).astype(BF16)
    def backward_dx(m, s, tiles, emit, ab=None):
        ab = s if ab is None else ab
        for j in tiles:
            cs = slice(j * 256, (j + 1) * 256)
            emit(cs, (dot_nt(darow[ab, 0:m, :], w1[s, cs, :]) + dot_nt(dbrow[ab, 0:m, :], w3[s, cs, :])).astype(BF16))

    def act_off(e):
        return pl.multiple_of(jnp.where(e == 0, 0, hot_rows + (e - 1) * n_rows), 64)

    def add_out(q, e, first, fresh):
        gate = column(q, e + 8)
        put = put_rows(q, e)
        for j in range(width // 256):
            cs = slice(j * 256, (j + 1) * 256)
            ypart[q, :, cs] = jnp.where(fresh, 0.0, ypart[q, :, cs]) + gate * dot_nn(put, orow[first:first + cp, cs])

    def add_dx_one(q, p, e):
        put = put_rows(q, e)
        for j in range(width // 256):
            cs = slice(j * 256, (j + 1) * 256)
            dxpart[q, :, cs] = dot_nn(put, orow[p * cp:(p + 1) * cp, cs])

    def add_dx_two(q, p, e, tiles):
        now, before = column(q, e), column(q, e - 1)
        now = jnp.where(now >= 0.0, now + float(cp), -1.0)
        lane = lax.broadcasted_iota(jnp.int32, (two, 2 * cp), 1).astype(F32)
        put = jnp.where(jnp.logical_or(before == lane, now == lane), 1.0, 0.0).astype(BF16)
        for j in tiles:
            cs = slice(j * 256, (j + 1) * 256)
            both = jnp.concatenate([orow[2 * two + p * cp:2 * two + (p + 1) * cp, cs], orow[p * cp:(p + 1) * cp, cs]], axis=0)
            dxpart[q, :, cs] += dot_nn(put, both)

    def lane_of(q, r, n, lane):
        m = mc[q, pl.ds(r, n), :]
        return jnp.sum(jnp.where(lax.broadcasted_iota(jnp.int32, (n, 128), 1) == lane, m, 0.0), axis=1, keepdims=True)

    def hot_forward(p, q, s, fresh):
        o = pl.multiple_of(p * two, 64)
        gate = column(q, 8)

        def emit(cs, out):
            ypart[q, :, cs] = jnp.where(fresh, 0.0, ypart[q, :, cs]) + gate * out.astype(F32)

        forward(two, x_all.at[q], uhot.at[pl.ds(o, two)], s, o, column(q, 0) >= 0.0, emit, lambda part: None)

    def load_next(i, e, step, parts):
        @pl.when(i < last - 1)
        def _():
            for n in parts:
                w_copies(e + 2 * step)[n].start()

    def cold_forward(i, e, step, s, r0, r1):
        def emit(cs, out):
            orow[0:r1 - r0, cs] = out

        forward(r1 - r0, erows.at[e, r0:r1], urow.at[e, r0:r1], s, pl.multiple_of(act_off(e) + r0, 16), None, emit,
                lambda part: load_next(i, e, step, (0, 1)))
        load_next(i, e, step, (2,))

    def weights_here(i, e, first):
        @pl.when(i >= (0 if first else 2))
        def _():
            for cpy in w_copies(e):
                cpy.wait()

    def rs(t, j):
        part = (ypart, dxpart)[t]
        o = k * tok
        if j < 4:
            q = (c_o, c_r, c_l, c)[j]
            src, dst, dev = part.at[q, pl.ds((1 - k) * tok, tok)], cbuf.at[q], partner
            if t == 1:
                src, dst = part.at[q, pl.ds((1 - k) * tok, tok), 0:width // 2], cbuf.at[q, :, 0:width // 2]
        elif j >= 10:
            q = (c_o, c_r, c_l, c)[j - 10]
            src, dst, dev = part.at[q, pl.ds((1 - k) * tok, tok), width // 2:width], cbuf.at[q, :, width // 2:width], partner
        else:
            src, dst, dev = (
                (part.at[c_o, pl.ds(o, half)], yra, right),
                (part.at[c_o, pl.ds(o + half, half)], yrb, left),
                (part.at[c_r, pl.ds(o + half, half)], yfl.at[half:tok], right),
                (part.at[c_l, pl.ds(o, half)], yfr.at[0:half], left),
                (part.at[c_r, pl.ds(o, half)], yfl.at[0:half], right),
                (part.at[c_l, pl.ds(o + half, half)], yfr.at[half:tok], left))[j - 4]
        return pltpu.make_async_remote_copy(
            src_ref=src, dst_ref=dst, send_sem=rs_send.at[t, j], recv_sem=rs_recv.at[t, j],
            device_id={"ep": dev}, device_id_type=MESH)

    def add_rows(part, q, off, src, n):
        @pl.loop(0, n // 32)
        def _(r):
            o = pl.multiple_of(r * 32, 32)
            part[q, pl.ds(pl.multiple_of(off + r * 32, 32), 32)] += src[pl.ds(o, 32)]

    ag(x_all, 0, 4).wait_recv()
    pick(0, c, x_all, False)

    @pl.loop(0, n_loc)
    def _(e):
        s = lax.rem(e, 2)
        hot = jnp.logical_and(is_owner, e == 0)
        weights_here(e, e, True)

        @pl.when(e == 2)
        def _():
            ag(x_all, 0, 0).wait_recv()
            ag(x_all, 0, 5).start()
            ag(x_all, 0, 2).wait_recv()
            ag(x_all, 0, 6).start()
            for n in (4, 0, 2, 1, 3):
                ag(dy_all, 1, n).start()

        @pl.when(jnp.logical_not(hot))
        def _():
            cold_forward(e, e, 1, s, 0, cp)
            add_out(c, e, 0, e == 0)

        @pl.when(hot)
        def _():
            hot_forward(0, c, s, True)
            load_next(e, e, 1, (0, 1, 2))

    ag(x_all, 0, 1).wait_recv()
    ag(x_all, 0, 7).start()
    ag(x_all, 0, 3).wait_recv()
    ag(x_all, 0, 8).start()
    rs(0, 3).start()
    ag(x_all, 0, 7).wait_recv()
    pick(1, c_l, x_all, False)
    ag(x_all, 0, 5).wait_recv()
    ag(x_all, 0, 9).start()
    ag(x_all, 0, 6).wait_recv()
    ag(x_all, 0, 10).start()
    ag(x_all, 0, 8).wait_recv()
    pick(2, c_r, x_all, False)
    rs(0, 3).wait_recv()
    add_rows(ypart, c, k * tok, cbuf.at[c], tok)
    own_out = pltpu.make_async_copy(ypart.at[c, pl.ds(k * tok, tok)], yown, io_sem.at[0])
    own_out.start()
    ag(x_all, 0, 9).wait_recv()
    ag(x_all, 0, 10).wait_recv()
    pick(3, c_o, x_all, False)

    def st_fwd(e):
        return (pltpu.make_async_copy(erows.at[e], xr_hbm.at[e], st_sem.at[0, e]),
                pltpu.make_async_copy(urow.at[e], ur_hbm.at[e], st_sem.at[1, e]))

    for e in range(n_loc):
        st_fwd(e)[0].start()

    def st_hot():
        return [pltpu.make_async_copy(uhot, uh_hbm, hst_sem.at[0])] + [
            pltpu.make_async_copy(x_all.at[q], xh_hbm.at[p * two:(p + 1) * two], hst_sem.at[1 + p]) for p, q in enumerate(near)]

    @pl.loop(0, n_loc)
    def _(i):
        e = last - i
        s = lax.rem(e, 2)
        hot = jnp.logical_and(is_owner, e == 0)
        weights_here(i, e, False)

        @pl.when(i == 1)
        def _():
            ag(dy_all, 1, 0).wait_recv()
            ag(dy_all, 1, 5).start()
            ag(dy_all, 1, 2).wait_recv()
            ag(dy_all, 1, 6).start()

        @pl.when(i == 3)
        def _():
            ag(dy_all, 1, 4).wait_recv()
            ag(dy_all, 1, 1).wait_recv()
            ag(dy_all, 1, 7).start()
            ag(dy_all, 1, 3).wait_recv()
            ag(dy_all, 1, 8).start()

        @pl.when(jnp.logical_not(hot))
        def _():
            cold_forward(i, e, -1, s, cp, n_rows)
            for j, p in enumerate((3, 2, 1)):
                add_out(near[p], e, (p - 1) * cp, i == 0)

                @pl.when(i == last)
                def _():
                    rs(0, j).start()

            st_fwd(e)[1].start()

        @pl.when(hot)
        def _():
            @pl.loop(0, 3)
            def _(n):
                p = 3 - n
                hot_forward(p, jnp.where(p == 1, c_l, jnp.where(p == 2, c_r, c_o)), s, False)
                for j in range(3):
                    @pl.when(n == j)
                    def _():
                        rs(0, j).start()

            for cpy in st_hot():
                cpy.start()

    for e in range(n_loc):
        st_fwd(e)[0].wait()
    rs(0, 0).wait_recv()
    add_rows(ypart, c_o, k * tok, cbuf.at[c_o], tok)
    rs(0, 4).start()
    rs(0, 5).start()
    ag(dy_all, 1, 5).wait_recv()
    ag(dy_all, 1, 9).start()
    ag(dy_all, 1, 6).wait_recv()
    ag(dy_all, 1, 10).start()
    pick(0, c, dy_all, True)
    for j, q in ((1, c_r), (2, c_l)):
        rs(0, j).wait_recv()
        add_rows(ypart, q, k * tok, cbuf.at[q], tok)
        rs(0, 5 + j).start()
    pl.semaphore_signal(free_sem, inc=1, device_id={"ep": partner}, device_id_type=MESH)
    ag(dy_all, 1, 7).wait_recv()
    pick(1, c_l, dy_all, True)
    ag(dy_all, 1, 8).wait_recv()
    pick(2, c_r, dy_all, True)
    ag(dy_all, 1, 9).wait_recv()
    ag(dy_all, 1, 10).wait_recv()
    pick(3, c_o, dy_all, True)

    @pl.loop(0, n_loc)
    def _(e):
        @pl.when(jnp.logical_not(jnp.logical_and(is_owner, e == 0)))
        def _():
            st_fwd(e)[1].wait()

    @pl.when(is_owner)
    def _():
        for cpy in st_hot():
            cpy.wait()

    def st_d(e):
        return pltpu.make_async_copy(erows.at[e], dr_hbm.at[e], st_sem.at[0, e])

    def st_ab(e, s):
        return (pltpu.make_async_copy(darow.at[s, 0:n_rows], da_hbm.at[e], st_sem.at[1, s]),
                pltpu.make_async_copy(dbrow.at[s, 0:n_rows], db_hbm.at[e], st_sem.at[1, 2 + s]))

    for e in range(n_loc):
        st_d(e).start()

    def st_hot_ab(h):
        at = pl.multiple_of(h * 2 * two, 64)
        return (pltpu.make_async_copy(darow.at[h], dah_hbm.at[pl.ds(at, 2 * two)], hst_sem.at[1 + h]),
                pltpu.make_async_copy(dbrow.at[h], dbh_hbm.at[pl.ds(at, 2 * two)], hst_sem.at[3 + h]))

    def rs_relay_y():
        rs(0, 4).wait_recv()
        add_rows(ypart, c_r, k * tok, yra, half)
        rs(0, 8).start()
        rs(0, 5).wait_recv()
        add_rows(ypart, c_l, k * tok + half, yrb, half)
        rs(0, 9).start()

    @pl.loop(0, n_loc)
    def _(e):
        s = lax.rem(e, 2)
        hot = jnp.logical_and(is_owner, e == 0)

        weights_here(e, e, False)

        @pl.when(jnp.logical_and(is_owner, e == 1))
        def _():
            for h in range(2):
                for cpy in st_hot_ab(h):
                    cpy.wait()

        @pl.when(jnp.logical_not(hot))
        def _():
            ooff = pl.multiple_of(s * 2 * two, 64)

            def emit(cs, out):
                orow[pl.ds(ooff, n_rows), cs] = out

            backward_du(n_rows, erows.at[e], s, act_off(e))

            @pl.when(e < last)
            def _():
                backward_dx(n_rows, s, all_tiles, emit)
                load_next(e, e, 1, (0, 1, 2))

                @pl.when(e == last - 2)
                def _():
                    rs_relay_y()

                @pl.when(e == 0)
                def _():
                    for p in range(chips):
                        add_dx_one(near[p], p, e)

                @pl.when(jnp.logical_and(e > 0, s == 0))
                def _():
                    for p in (3, 2, 1, 0):
                        add_dx_two(near[p], p, e, all_tiles)

            @pl.when(e == last)
            def _():
                for h in range(2):
                    tiles = all_tiles[h * len(all_tiles) // 2:(h + 1) * len(all_tiles) // 2]
                    backward_dx(n_rows, s, tiles, emit)
                    if h == 0:
                        pl.semaphore_wait(free_sem, 1)
                    for j, p in enumerate((3, 2, 1, 0)):
                        add_dx_two(near[p], p, e, tiles)
                        rs(1, j + 10 * h).start()

        @pl.when(hot)
        def _():
            @pl.loop(0, chips // 2)
            def _(h):
                pair = (jnp.where(h == 0, c, c_r), jnp.where(h == 0, c_l, c_o))
                for n, q in enumerate(pair):
                    @pl.loop(0, two // 64)
                    def _(r):
                        at = pl.multiple_of(r * 64, 64)
                        got = dy_all[q, pl.ds(at, 64), :].astype(F32)
                        hrows[pl.ds(pl.multiple_of(n * two + r * 64, 64), 64), :] = (lane_of(q, at, 64, 8) * got).astype(BF16)

                o = pl.multiple_of(h * 2 * two, 64)
                sd = pltpu.make_async_copy(hrows, dh_hbm.at[pl.ds(o, 2 * two)], hst_sem.at[0])
                sd.start()

                def emit(cs, out):
                    for n, q in enumerate(pair):
                        dxpart[q, :, cs] = out[n * two:(n + 1) * two].astype(F32)

                backward_du(2 * two, hrows, s, o, h)
                backward_dx(2 * two, s, all_tiles, emit, h)
                for cpy in st_hot_ab(h):
                    cpy.start()
                sd.wait()

            load_next(e, e, 1, (0, 1, 2))

        @pl.when(jnp.logical_and(e >= 1, jnp.logical_not(jnp.logical_and(is_owner, e == 1))))
        def _():
            for cpy in st_ab(e - 1, 1 - s):
                cpy.wait()

        @pl.when(jnp.logical_not(hot))
        def _():
            for cpy in st_ab(e, s):
                cpy.start()

    def chip_sums_out(j):
        q = (c_o, c_r, c_l, c)[j]
        lo = dxpart.at[q, pl.ds(k * tok, half)]
        hi = dxpart.at[q, pl.ds(k * tok + half, half)]
        if j == 3:
            return (pltpu.make_async_copy(dxpart.at[q, pl.ds(k * tok, tok)], sc_hbm, so_sem.at[6]),)
        to_lo, to_hi = ((go_r.at[0:half], go_l.at[0:half]), (sr_hbm, go_r.at[half:tok]), (go_l.at[half:tok], sl_hbm))[j]
        return (pltpu.make_async_copy(lo, to_lo, so_sem.at[2 * j]), pltpu.make_async_copy(hi, to_hi, so_sem.at[2 * j + 1]))

    for j, q in enumerate((c_o, c_r, c_l, c)):
        rs(1, j).wait_recv()
        rs(1, j + 10).wait_recv()
        add_rows(dxpart, q, k * tok, cbuf.at[q], tok)
        for cpy in chip_sums_out(j):
            cpy.start()
    for j in (6, 7, 8, 9):
        rs(0, j).wait_recv()

    for e in range(n_loc):
        st_d(e).wait()
    for cpy in st_ab(last, last % 2):
        cpy.wait()
    for d in range(1, group):
        for cpy in meta_copies(d):
            cpy.wait_send()
    for i in range(11):
        ag(x_all, 0, i).wait_send()
        ag(dy_all, 1, i).wait_send()
    for j in range(10):
        rs(0, j).wait_send()
    for j in range(4):
        rs(1, j).wait_send()
        rs(1, j + 10).wait_send()
        for cpy in chip_sums_out(j):
            cpy.wait()
    own_out.wait()


def expert_grads(x_ref, d_ref, u_ref, da_ref, db_ref, g1, g3, g2):
    g1[0] = dot_tn(x_ref[0], da_ref[0]).astype(BF16)
    g3[0] = dot_tn(x_ref[0], db_ref[0]).astype(BF16)
    g2[0] = dot_tn(u_ref[0], d_ref[0]).astype(BF16)


def first_grads_kernel(owner, x_ref, d_ref, u_ref, da_ref, db_ref, xh, dh, uh, dah, dbh, own_hbm, fl_hbm, fr_hbm, g1, g3, g2, y_out, xb, dbuf, ub, dab, dbb, parts, sem, y_sem):
    i = pl.program_id(0)
    is_owner = lax.axis_index("ep") == owner
    hot = jnp.logical_and(is_owner, i == pl.num_programs(0) - 1)

    def copies():
        return [pltpu.make_async_copy(src, dst, sem.at[j]) for j, (src, dst) in enumerate(((xh, xb), (dah, dab), (dbh, dbb), (uh, ub), (dh, dbuf)))]

    def y_copies():
        return [pltpu.make_async_copy(src, parts.at[j], y_sem.at[j]) for j, src in enumerate((own_hbm, fl_hbm, fr_hbm))]

    @pl.when(i == 0)
    def _():
        for cpy in y_copies():
            cpy.start()

    @pl.when(i == pl.num_programs(0) - 1)
    def _():
        for cpy in y_copies():
            cpy.wait()
        y_out[...] = (parts[0] + parts[1] + parts[2]).astype(BF16)

    @pl.when(jnp.logical_and(is_owner, i == 0))
    def _():
        for cpy in copies():
            cpy.start()

    @pl.when(jnp.logical_not(hot))
    def _():
        expert_grads(x_ref, d_ref, u_ref, da_ref, db_ref, g1, g3, g2)

    @pl.when(hot)
    def _():
        for cpy in copies():
            cpy.wait()
        g1[0] = dot_tn(xb[...], dab[...]).astype(BF16)
        g3[0] = dot_tn(xb[...], dbb[...]).astype(BF16)
        g2[0] = dot_tn(ub[...], dbuf[...]).astype(BF16)


def later_grads_kernel(x_ref, d_ref, u_ref, da_ref, db_ref, g1_in, g3_in, g2_in, g1, g3, g2):
    del g1_in, g3_in, g2_in
    expert_grads(x_ref, d_ref, u_ref, da_ref, db_ref, g1, g3, g2)


def solution(mesh):
    group = mesh.shape["ep"]
    num_dev = mesh.shape["dp"] * group
    tok_spec = P(("dp", "ep"), None)
    w_spec = P("ep", None, None)
    grad_spec = P(("dp", "ep"), None, None)

    def layer_fn(tokens, expert_ids, gate_vals, w_gate, w_up, w_down, grad_out):
        n_exp, width, hid = w_gate.shape
        tok = tokens.shape[0] // num_dev
        top_k = expert_ids.shape[1]
        cap = ((2 * tok * top_k + 8 * n_exp - 1) // (8 * n_exp)) * 8
        n_loc = n_exp // group
        hot = n_exp // 2
        owner = hot // n_loc
        chips = group // 2
        n_rows = chips * 2 * cap
        hot_rows = group * tok
        cfg = (chips, tok, width, hid, n_loc, cap, owner)

        def device_fn(x, ids, gates, w1, w3, w2, dy):
            any_spec = pl.BlockSpec(memory_space=pl.ANY)
            vmem_spec = pl.BlockSpec(memory_space=pltpu.VMEM)
            sds = jax.ShapeDtypeStruct
            hb = hot_rows // 2
            half = tok // 2
            act_rows = hot_rows + (n_loc - 1) * n_rows
            outs = pl.pallas_call(
                functools.partial(layer_kernel, cfg),
                out_shape=(
                    *[sds((tok, width), F32)] * 5, *[sds((half, width), F32)] * 2, sds((tok, width), F32),
                    sds((n_loc, n_rows, width), BF16), sds((n_loc, n_rows, width), BF16),
                    sds((n_loc, n_rows, hid), BF16), sds((n_loc, n_rows, hid), BF16), sds((n_loc, n_rows, hid), BF16),
                    sds((hot_rows, width), BF16), sds((hot_rows, width), BF16),
                    sds((hot_rows, hid), BF16), sds((hot_rows, hid), BF16), sds((hot_rows, hid), BF16)),
                in_specs=[any_spec, any_spec, vmem_spec, vmem_spec, any_spec, any_spec, any_spec],
                out_specs=[any_spec] * 18,
                scratch_shapes=[
                    pltpu.VMEM((chips, 2 * tok, width), BF16), pltpu.VMEM((chips, 2 * tok, width), BF16),
                    pltpu.VMEM((group, top_k, tok), jnp.int32), pltpu.VMEM((group, top_k, tok), F32),
                    pltpu.VMEM((chips, 8, 2 * tok), F32), pltpu.VMEM((chips, 8, 2 * tok), F32),
                    pltpu.VMEM((chips, 2 * tok, 128), F32),
                    pltpu.VMEM((chips, 2 * tok, width), F32), pltpu.VMEM((chips, 2 * tok, width), F32),
                    pltpu.VMEM((chips, tok, width), F32),
                    pltpu.VMEM((half, width), F32), pltpu.VMEM((half, width), F32),
                    pltpu.VMEM((n_loc, n_rows, width), BF16), pltpu.VMEM((hb, width), BF16),
                    pltpu.VMEM((n_loc, n_rows, hid), BF16), pltpu.VMEM((hot_rows, hid), BF16),
                    pltpu.VMEM((2, hb, hid), BF16), pltpu.VMEM((2, hb, hid), BF16),
                    pltpu.VMEM((act_rows, hid), F32), pltpu.VMEM((act_rows, hid), F32),
                    pltpu.VMEM((hb + n_rows, width), BF16), pltpu.VMEM((n_loc * 2 * cap, 2 * tok), BF16),
                    pltpu.VMEM((2, width, hid), BF16), pltpu.VMEM((2, width, hid), BF16), pltpu.VMEM((2, hid, width), BF16),
                    pltpu.SemaphoreType.DMA((2, group)), pltpu.SemaphoreType.DMA((2, group)),
                    pltpu.SemaphoreType.DMA((2, 11)), pltpu.SemaphoreType.DMA((2, 11)),
                    pltpu.SemaphoreType.DMA((2, 14)), pltpu.SemaphoreType.DMA((2, 14)),
                    pltpu.SemaphoreType.DMA((3, 2)), pltpu.SemaphoreType.DMA((2, n_loc)), pltpu.SemaphoreType.DMA((5,)),
                    pltpu.SemaphoreType.DMA((2,)), pltpu.SemaphoreType.DMA((7,)), pltpu.SemaphoreType.REGULAR,
                ],
                compiler_params=pltpu.CompilerParams(collective_id=0, has_side_effects=True, vmem_limit_bytes=67043328),
                name="moe_layer",
            )(x, dy, ids.T, gates.T, w1, w3, w2)
            yown, yfl, yfr, go_r, go_l, sr, sl, sc, xr, dr, ur, dar, dbr, xh, dh, uh, dah, dbh = outs

            to_right = [(i, (i + 2) % group) for i in range(group)]
            to_left = [(i, (i + group - 2) % group) for i in range(group)]
            from_l = lax.ppermute(go_r, "ep", to_right)
            from_r = lax.ppermute(go_l, "ep", to_left)

            n_first = (n_loc + 1) // 2
            g_shapes = (sds((n_loc, width, hid), BF16), sds((n_loc, width, hid), BF16), sds((n_loc, hid, width), BF16))

            def blk(r, n, at):
                return pl.BlockSpec((1, r, n), lambda i: (at(i), 0, 0))

            def row_specs(at):
                return [blk(n_rows, width, at), blk(n_rows, width, at), blk(n_rows, hid, at), blk(n_rows, hid, at), blk(n_rows, hid, at)]

            def out_blks(at):
                return [blk(width, hid, at), blk(width, hid, at), blk(hid, width, at)]

            def cost(n):
                return pl.CostEstimate(flops=n * 6 * n_rows * width * hid, transcendentals=0,
                                       bytes_accessed=n * 2 * (2 * n_rows * width + 3 * n_rows * hid + 3 * width * hid))

            def first_at(i):
                return lax.rem(i + 1, n_first)

            def later_at(i):
                return i + n_first

            y_spec = pl.BlockSpec((tok, width), lambda i: (0, 0))
            *grads, y = pl.pallas_call(
                functools.partial(first_grads_kernel, owner),
                grid=(n_first,), out_shape=g_shapes + (sds((tok, width), BF16),),
                in_specs=row_specs(first_at) + [any_spec] * 8, out_specs=out_blks(first_at) + [y_spec],
                scratch_shapes=[pltpu.VMEM((hot_rows, width), BF16), pltpu.VMEM((hot_rows, width), BF16), pltpu.VMEM((hot_rows, hid), BF16),
                                pltpu.VMEM((hot_rows, hid), BF16), pltpu.VMEM((hot_rows, hid), BF16), pltpu.VMEM((3, tok, width), F32),
                                pltpu.SemaphoreType.DMA((5,)), pltpu.SemaphoreType.DMA((3,))],
                compiler_params=pltpu.CompilerParams(vmem_limit_bytes=60 << 20),
                cost_estimate=cost(n_first), name="first_grads",
            )(xr, dr, ur, dar, dbr, xh, dh, uh, dah, dbh, yown, yfl, yfr)

            fl_lo = lax.ppermute(sr + from_l[:half], "ep", to_right)
            fr_hi = lax.ppermute(sl + from_r[:half], "ep", to_left)
            g1, g3, g2 = pl.pallas_call(
                later_grads_kernel,
                grid=(n_loc - n_first,), out_shape=g_shapes,
                in_specs=row_specs(later_at) + [any_spec] * 3, out_specs=out_blks(later_at),
                input_output_aliases={5: 0, 6: 1, 7: 2},
                compiler_params=pltpu.CompilerParams(vmem_limit_bytes=60 << 20),
                cost_estimate=cost(n_loc - n_first), name="later_grads",
            )(xr, dr, ur, dar, dbr, *grads)
            fl = jnp.concatenate([fl_lo, from_l[half:]], axis=0)
            fr = jnp.concatenate([from_r[half:], fr_hi], axis=0)
            dx = (sc + fl + fr).astype(BF16)
            return y, dx, g1, g3, g2

        return jax.shard_map(device_fn, mesh=mesh, in_specs=(tok_spec, tok_spec, tok_spec, w_spec, w_spec, w_spec, tok_spec),
                             out_specs=(tok_spec, tok_spec, grad_spec, grad_spec, grad_spec), check_vma=False)(
            tokens, expert_ids, gate_vals, w_gate, w_up, w_down, grad_out)

    return layer_fn
```
